32 devices in a mesh: gx: 8 (over y, x, core), gy: 4 (over z).
Axes of the slice: x: 2, y: 2, z: 4, core: 2. Of those that a mesh axis runs over, the one named last changes fastest.
Arguments:
- products: bfloat16 [1536, 3, 2048], P('gy', None, 'gx'), may hold values from -6 to 6
- operator: bfloat16 [1536, 1536], P(None, 'gy'), may hold values from -0.21875 to 0.21875
Outputs:
- derivative: bfloat16 [1536, 3, 2048], P(('gy', 'gx'))
The draws below stay inside these ranges and needn't reach their ends.
All inputs are finite; a program needn't handle non-finite values.
Results may differ from the reference program's by a relative error of at most 0.002.
Values may be sent and summed in bfloat16 or wider, within the bound.
A program may use at most 64 MiB of HBM per device.

```python
import jax
import jax.numpy as jnp

NY = 1536
MODES = 2048


def strengthened(array, own_key, source, target, blocks, factor):
    owner, partner = [(jnp.arange(array.shape[position]) // (array.shape[position] // blocks)).reshape([-1 if axis == position else 1 for axis in range(array.ndim)]) for position in (source, target)]
    chosen = jax.random.permutation(own_key, blocks)[partner]
    strong = (owner == chosen) | (owner == (partner + blocks // 2) % blocks)
    return jnp.where(strong, factor * array, array)


def block_scale(rng, shape, pieces, smallest, largest):
    loudness = 1.0
    for axis_at, shards_of in pieces:
        heights = jax.random.uniform(jax.random.fold_in(jax.random.fold_in(rng, 6), axis_at), (shards_of,), jnp.float32, smallest / len(pieces), largest / len(pieces))
        loudness = loudness * jnp.repeat(jnp.exp(heights), shape[axis_at] // shards_of).reshape((-1,) + (1,) * (len(shape) - 1 - axis_at))
    return loudness


def gaussian(own_key, extent, scale, limit, split=(), kind=jnp.bfloat16):
    entries = scale * jax.random.normal(own_key, extent, jnp.float32)
    if split:
        entries = entries * block_scale(own_key, extent, split, -0.22, 0.18)
    return jnp.clip(entries, -limit, limit).astype(kind)


def heavy_noise(key, shape, width, limit, pieces, heavy, kind=jnp.bfloat16):
    entries = width * jax.random.normal(key, shape, jnp.float32)
    if pieces:
        entries = entries * block_scale(key, shape, pieces, -0.22, 0.18)
    return jnp.clip(strengthened(entries, jax.random.fold_in(key, 3), *heavy), -limit, limit).astype(kind)


def setup_inputs(seed: int = 0) -> dict:
    streams_of = jax.random.split(jax.random.key(seed), 3)
    products = gaussian(streams_of[0], (NY, 3, MODES), 1.0, 6.0, ((0, 4), (2, 8)))
    operator = heavy_noise(streams_of[1], (NY, NY), NY ** -0.5, 0.21875, ((1, 4),), (1, 0, 4, 2.0))
    return dict(products=products, operator=operator)


def reference(products, operator):
    flat = products.reshape(NY, 3 * MODES)
    summed = jnp.dot(operator, flat, preferred_element_type=jnp.float32)
    return summed.astype(jnp.bfloat16).reshape(NY, 3, MODES)
```

```python
import functools

import jax
import jax.numpy as jnp
from jax import lax
from jax.experimental import pallas as pl
from jax.experimental.pallas import tpu as pltpu
from jax.sharding import PartitionSpec as P

MESH = pl.DeviceIdType.MESH
LANES = 128
SUBLANES = 16
VMEM_BYTES = 60 * 1024 * 1024
GRANT = 54500 * 1024


def kernel(n, g, parts, p_ref, op_ref, out_ref, blocks, ops, res,
           own_send, fwd_send, op_send, spread_send, res_send, blk_recv, op_recv, out_recv, own_copy, ready, ahead_of,
           op_far, tail, part, part_in, far_terms, near_terms, terms, last,
           part_send, part_recv, far_send, near_send, terms_recv, last_copy):
    j, k = lax.axis_index("gx"), lax.axis_index("gy")
    half = n // 2
    side = lax.div(k, half)
    step = 1 - 2 * side
    centre = jnp.where(side == 0, half - 1, half)
    other = n - 1 - centre
    is_centre = k == centre
    planes, rows, cols = p_ref.shape
    width = cols // parts
    chunks = planes * parts
    piece = half * rows // g
    outrows = rows // g
    raw = chunks - 1
    ahead, lead = 2, min(3, raw)

    def flip(mask):
        to = j
        for bit in (1 << b for b in range(mask.bit_length())):
            if mask & bit:
                to = to + bit * (1 - 2 * lax.rem(lax.div(j, bit), 2))
        return to

    def near(d):
        return centre - step * d

    def far(d):
        return other + step * d

    rounds = g.bit_length() - 1
    barrier = pltpu.get_barrier_semaphore()

    def signal(sem, gx, gy):
        pl.semaphore_signal(sem, inc=1, device_id=(gx, gy), device_id_type=MESH)

    for b in range(rounds):
        signal(barrier, flip(1 << b), k)

    @pl.when(is_centre)
    def _():
        signal(barrier, j, other)
        for d in range(1, half):
            signal(barrier, j, near(d))
        pl.semaphore_wait(barrier, rounds + half)

    @pl.when(jnp.logical_not(is_centre))
    def _():
        signal(barrier, j, centre)
        pl.semaphore_wait(barrier, rounds + 1)

    def hops(owner):
        d, to = owner
        return bin(to >> 1).count("1") - d, to

    owners = sorted(((d, to) for d in range(half) for to in range(g)), key=hops)

    def far_rows(d, to):
        rel = far(d) - (1 - side) * half
        return pl.ds(pl.multiple_of(rel * rows + to * outrows, outrows), outrows)

    def near_rows(d, to):
        rel = near(d) - side * half
        return pl.ds(pl.multiple_of(rel * rows + to * outrows, outrows), outrows)

    far_op = pltpu.make_async_copy(
        op_ref.at[pl.ds(pl.multiple_of((1 - side) * (half * rows), half * rows), half * rows), :], op_far,
        own_copy.at[2])
    tail_in = pltpu.make_async_copy(p_ref.at[planes - 1, :, pl.ds((parts - 1) * width, width)], tail, own_copy.at[3])

    def own_part():
        far_op.wait()
        tail_in.wait()
        part[...] = jnp.dot(op_far[...], tail[...], preferred_element_type=jnp.float32)

    def plane_entered():
        for b in range(rounds):
            signal(ready.at[b], flip(1 << b), k)
            pl.semaphore_wait(ready.at[b], 1)

    def remote(src, dst, send, recv, gx, gy):
        return pltpu.make_async_remote_copy(
            src_ref=src, dst_ref=dst, send_sem=send, recv_sem=recv,
            device_id=(gx, gy), device_id_type=MESH)

    def wait_bytes(ref, sem):
        pltpu.make_async_copy(ref, ref, sem).wait()

    def chunk_of(ref, i):
        c, h = lax.div(i, parts), lax.rem(i, parts)
        return ref.at[c, :, pl.ds(pl.multiple_of(h * width, width), width)]

    def piece_rows(at):
        return pl.ds(pl.multiple_of(at * piece, piece), piece)

    def from_source(s):
        return pl.ds(pl.multiple_of(s * rows, rows), rows)

    def op_part(s, at):
        return ops.at[piece_rows(at), from_source(s)]

    def block_part(s, i):
        c, h = lax.div(i, parts), lax.rem(i, parts)
        return blocks.at[c, from_source(s), pl.ds(pl.multiple_of(h * width, width), width)]

    def op_out(slot, to_side, to):
        at = pl.multiple_of(to_side * (half * rows) + j * piece, piece)
        remote(op_ref.at[pl.ds(at, piece), :], op_part(k, j),
               op_send.at[slot], op_recv.at[k, j], j, to).start()

    def block_out(i, to):
        remote(chunk_of(p_ref, i), block_part(k, i), own_send.at[i], blk_recv.at[k, i], j, to).start()

    @pl.when(is_centre)
    def _():
        op_out(0, 1 - side, other)
        for i in range(ahead):
            block_out(i, other)
        for d in range(1, half):
            signal(ready.at[rounds], j, near(d))
        own_rows = pl.ds(pl.multiple_of(side * (half * rows), half * rows), half * rows)
        own_ops = pltpu.make_async_copy(op_ref.at[own_rows, :], ops.at[:, from_source(k)], own_copy.at[0])
        own_ops.start()
        own_blocks = pltpu.make_async_copy(p_ref, blocks.at[:, from_source(k), :], own_copy.at[1])
        own_blocks.start()
        far_op.start()
        tail_in.start()

        plane_entered()
        pl.semaphore_wait(ready.at[rounds], half - 1)
        signal(ready.at[rounds + 1], j, other)

        sources = [near(d) for d in range(1, half)] + [far(d) for d in range(half)]
        sibling = flip(1)

        def spread(s, at, to):
            part = op_part(s, at)
            remote(part, part, spread_send.at[s], op_recv.at[s, at], to, k).start()

        def arrived(s, at):
            part = op_part(s, at)
            wait_bytes(part, op_recv.at[s, at])

        for s in sources:
            arrived(s, j)
            for d in range(1, g // 2):
                spread(s, j, flip(2 * d))
            spread(s, j, sibling)
        own_part()

        def forward(i):
            for d in range(1, half):
                at = block_part(near(d), i)
                wait_bytes(at, blk_recv.at[near(d), i])
                remote(at, at, fwd_send.at[d - 1, i], blk_recv.at[near(d), i], j, other).start()

        def step_on(i):
            forward(i)

            @pl.when(jnp.logical_and(i >= ahead - 1, i + 1 < raw))
            def _():
                block_out(i + 1, other)

        for i in range(lead):
            step_on(jnp.int32(i))
        for s in sources:
            for d in range(1, g // 2):
                at = flip(2 * d)
                arrived(s, at)
                spread(s, at, sibling)
        for s in sources:
            for d in range(g // 2):
                arrived(s, flip(2 * d + 1))
        own_ops.wait()
        own_blocks.wait()

        def near_half():
            lane = pl.ds((parts - 1) * width, width)
            for d in range(1, half):
                wait_bytes(block_part(near(d), raw), blk_recv.at[near(d), raw])
            mine = pl.ds(pl.multiple_of(side * (half * rows), half * rows), half * rows)
            near_terms[...] = jnp.dot(
                ops[:, mine], blocks[planes - 1, mine, lane],
                preferred_element_type=jnp.float32).astype(near_terms.dtype)
            target = terms.at[1, :, pl.ds(pl.multiple_of(j * width, width), width)]
            for d in reversed(range(half)):
                for mask in reversed(range(1 if d == 0 else 0, g)):
                    to = flip(mask)
                    remote(near_terms.at[near_rows(d, to), :], target, near_send, terms_recv.at[1],
                           to, near(d)).start()
            pltpu.make_async_copy(near_terms.at[near_rows(0, j), :], target, terms_recv.at[1]).start()

        def far_half():
            target = terms.at[0, :, pl.ds(pl.multiple_of(j * width, width), width)]
            pl.semaphore_wait(ready.at[rounds + 1], 1)
            for at, (d, to) in enumerate(owners):
                band = far_rows(d, to)
                total = part[band, :]
                for m in range(half - 1):
                    wait_bytes(part_in.at[m, band, :], part_recv.at[m, at])
                    total = total + part_in[m, band, :]
                far_terms[band, :] = total.astype(far_terms.dtype)
                remote(far_terms.at[band, :], target, far_send, terms_recv.at[0], to, far(d)).start()

        def one(i, carry):
            c, h = lax.div(i, parts), lax.rem(i, parts)
            lane = pl.ds(pl.multiple_of(h * width, width), width)

            @pl.when(i + lead < raw)
            def _():
                step_on(i + lead)

            @pl.when(i == raw - 1)
            def _():
                near_half()
                far_half()

            final = far(half - 1)
            others = pl.ds(pl.multiple_of(side * rows, rows), (n - 1) * rows)
            for d in range(half - 1):
                wait_bytes(block_part(far(d), i), blk_recv.at[far(d), i])
            ahead_of[...] = jnp.dot(ops[:, others], blocks[c, others, lane], preferred_element_type=jnp.float32)
            wait_bytes(block_part(final, i), blk_recv.at[final, i])
            target = pl.ds(pl.multiple_of(j * cols + h * width, width), width)
            arrival = out_recv.at[lax.div(c, planes - 1)]
            for d in reversed(range(half)):
                rel = pl.multiple_of((near(d) - side * half) * rows, rows)
                total = ahead_of[pl.ds(rel, rows), :] + jnp.dot(
                    ops[pl.ds(rel, rows), from_source(final)], blocks[c, from_source(final), lane],
                    preferred_element_type=jnp.float32)
                res[d, c, :, lane] = total.astype(res.dtype)
                for mask in range(1 if d == 0 else 0, g):
                    to = flip(mask) if d == 0 else mask
                    remote(res.at[d, c, pl.ds(pl.multiple_of(to * outrows, outrows), outrows), lane],
                           out_ref.at[c, :, target], res_send.at[d, i], arrival, to, near(d)).start()
                if d == 0:
                    pltpu.make_async_copy(
                        res.at[d, c, pl.ds(pl.multiple_of(j * outrows, outrows), outrows), lane],
                        out_ref.at[c, :, target], arrival).start()
            return carry

        lax.fori_loop(0, raw, one, 0)
        wait_bytes(op_part(0, 0), op_send.at[0])
        for i in range(raw):
            wait_bytes(block_part(0, i), own_send.at[i])
            for d in range(1, half):
                wait_bytes(block_part(0, i), fwd_send.at[d - 1, i])
            for d in range(half):
                sent = rows - outrows if d == 0 else rows
                wait_bytes(res.at[d, 0, pl.ds(0, sent), pl.ds(0, width)], res_send.at[d, i])
        for s in sources:
            wait_bytes(ops.at[pl.ds(0, (g - 1) * piece), from_source(0)], spread_send.at[s])
        wait_bytes(far_terms, far_send)
        wait_bytes(near_terms.at[pl.ds(0, half * rows - outrows), :], near_send)

    @pl.when(jnp.logical_not(is_centre))
    def _():
        op_out(1, side, centre)
        far_op.start()
        tail_in.start()
        pl.semaphore_wait(ready.at[rounds], 1)
        op_out(0, 1 - side, other)
        for i in range(chunks):
            block_out(i, centre)
        plane_entered()
        signal(ready.at[rounds], j, centre)
        own_part()
        away = step * (centre - k) - 1
        for at, (d, to) in enumerate(owners):
            band = far_rows(d, to)
            remote(part.at[band, :], part_in.at[away, band, :], part_send, part_recv.at[away, at], j, centre).start()
        wait_bytes(op_part(0, 0), op_send.at[0])
        wait_bytes(op_part(0, 0), op_send.at[1])
        for i in range(chunks):
            wait_bytes(block_part(0, i), own_send.at[i])
        wait_bytes(part, part_send)

    for half_of in range(2):
        wait_bytes(terms.at[half_of], terms_recv.at[half_of])
    last[...] = (terms[0].astype(jnp.float32) + terms[1].astype(jnp.float32)).astype(last.dtype)
    for s in range(g):
        pltpu.make_async_copy(
            last.at[:, pl.ds(s * width, width)],
            out_ref.at[planes - 1, :, pl.ds(s * cols + (parts - 1) * width, width)], last_copy).start()
    wait_bytes(out_ref.at[pl.ds(0, planes - 1)], out_recv.at[0])
    if parts > 1:
        wait_bytes(out_ref.at[planes - 1, :, pl.ds(0, g * width * (parts - 1))], out_recv.at[1])
    wait_bytes(last, last_copy)


def at_centres(n, g, products, operator):
    rows, planes, cols = products.shape
    parts = 2 if cols % (2 * LANES) == 0 else 1
    half = n // 2
    chunks = planes * parts
    width, outer = cols // parts, max(half - 1, 1)
    out = pl.pallas_call(
        functools.partial(kernel, n, g, parts),
        out_shape=jax.ShapeDtypeStruct((planes, rows // g, cols * g), jnp.bfloat16),
        in_specs=[pl.BlockSpec(memory_space=pl.ANY)] * 2,
        out_specs=pl.BlockSpec(memory_space=pl.ANY),
        scratch_shapes=[
            pltpu.VMEM((planes, n * rows, cols), jnp.bfloat16),
            pltpu.VMEM((half * rows, n * rows), jnp.bfloat16),
            pltpu.VMEM((half, planes, rows, cols), jnp.bfloat16),
            pltpu.SemaphoreType.DMA((chunks,)),
            pltpu.SemaphoreType.DMA((half, chunks)),
            pltpu.SemaphoreType.DMA((2,)),
            pltpu.SemaphoreType.DMA((n,)),
            pltpu.SemaphoreType.DMA((half, chunks)),
            pltpu.SemaphoreType.DMA((n, chunks)),
            pltpu.SemaphoreType.DMA((n, g)),
            pltpu.SemaphoreType.DMA((2,)),
            pltpu.SemaphoreType.DMA((4,)),
            pltpu.SemaphoreType.REGULAR((g.bit_length() + 1,)),
            pltpu.VMEM((half * rows, width), jnp.float32),
            pltpu.VMEM((half * rows, rows), jnp.bfloat16),
            pltpu.VMEM((rows, width), jnp.bfloat16),
            pltpu.VMEM((half * rows, width), jnp.float32),
            pltpu.VMEM((outer, half * rows, width), jnp.float32),
            pltpu.VMEM((half * rows, width), jnp.bfloat16),
            pltpu.VMEM((half * rows, width), jnp.bfloat16),
            pltpu.VMEM((2, rows // g, g * width), jnp.bfloat16),
            pltpu.VMEM((rows // g, g * width), jnp.bfloat16),
            pltpu.SemaphoreType.DMA,
            pltpu.SemaphoreType.DMA((outer, half * g)),
            pltpu.SemaphoreType.DMA,
            pltpu.SemaphoreType.DMA,
            pltpu.SemaphoreType.DMA((2,)),
            pltpu.SemaphoreType.DMA,
        ],
        compiler_params=pltpu.CompilerParams(
            collective_id=0, has_side_effects=True, vmem_limit_bytes=GRANT),
    )(products.transpose(1, 0, 2), operator)
    return out.transpose(1, 0, 2)


def by_collectives(products, operator):
    y_local, three, m_local = products.shape
    flat = products.reshape(y_local, three * m_local)
    summed = lax.psum_scatter(
        jnp.dot(operator, flat, preferred_element_type=jnp.float32), "gy", scatter_dimension=0, tiled=True)
    result = summed.astype(jnp.bfloat16).reshape(y_local, three, m_local)
    return lax.all_to_all(result, "gx", split_axis=0, concat_axis=2, tiled=True)


def solution(mesh):
    n, g = mesh.shape["gy"], mesh.shape["gx"]

    def body(products, operator):
        rows, planes, cols = products.shape
        aligned = (n % 2 == 0 and planes > 2 and g & (g - 1) == 0 and g > 1 and rows % (g * SUBLANES) == 0
                   and rows % LANES == 0 and cols % LANES == 0)
        held = 2 * (products.size * (n + n // 2 + 2) + operator.size * (1 + n // 2))
        if aligned and held < VMEM_BYTES // 2:
            return at_centres(n, g, products, operator)
        return by_collectives(products, operator)

    return jax.shard_map(
        body,
        mesh=mesh,
        in_specs=(P("gy", None, "gx"), P(None, "gy")),
        out_specs=P(("gy", "gx"), None, None),
        check_vma=False,
    )
```

```python
import functools

import jax
import jax.numpy as jnp
from jax import lax
from jax.experimental import pallas as pl
from jax.experimental.pallas import tpu as pltpu
from jax.sharding import PartitionSpec as P

MESH = pl.DeviceIdType.MESH
LANES = 128
SUBLANES = 16
VMEM_BYTES = 60 * 1024 * 1024
GRANT = 54500 * 1024


def kernel(n, g, parts, p_ref, op_ref, out_ref, blocks, ops, far_ops, passing, res, wide, part, part_out, part_in,
           far_out, far_in, near_sum, late, own_send, fwd_send, op_send, spread_send, res_send, part_send, far_send,
           late_send, blk_recv, op_recv, pass_recv, plane_recv, sibling_recv, out_recv, part_recv, far_recv, own_copy,
           ready):
    j, k = lax.axis_index("gx"), lax.axis_index("gy")
    half = n // 2
    side = lax.div(k, half)
    step = 1 - 2 * side
    centre = jnp.where(side == 0, half - 1, half)
    other = n - 1 - centre
    is_centre = k == centre
    away = step * (centre - k)
    planes, rows, cols = p_ref.shape
    width = cols // parts
    raw = (planes - 1) * parts
    outrows = rows // g
    mine = pl.ds(pl.multiple_of(side * (half * rows), half * rows), half * rows)
    theirs = pl.ds(pl.multiple_of((1 - side) * (half * rows), half * rows), half * rows)

    def flip(mask):
        to = j
        for bit in (1 << b for b in range(mask.bit_length())):
            if mask & bit:
                to = to + bit * (1 - 2 * lax.rem(lax.div(j, bit), 2))
        return to

    def near(d):
        return centre - step * d

    def far(d):
        return other + step * d

    def from_source(s):
        return pl.ds(pl.multiple_of(s * rows, rows), rows)

    def near_rows(d, to, count=1):
        at = (near(d) - side * half) * rows + to * outrows
        return pl.ds(pl.multiple_of(at, outrows), count * outrows)

    def far_rows(d, to, count=1):
        at = (far(d) - (1 - side) * half) * rows + to * outrows
        return pl.ds(pl.multiple_of(at, outrows), count * outrows)

    def wait_bytes(ref, sem):
        pltpu.make_async_copy(ref, ref, sem).wait()

    def op_bytes(pieces):
        return ops.at[pl.ds(0, pieces * outrows), pl.ds(0, rows)]

    own_far = pltpu.make_async_copy(op_ref.at[theirs, :], far_ops, own_copy.at[0])
    own_far.start()
    own_blocks = pltpu.make_async_copy(p_ref, blocks.at[:, from_source(k), :], own_copy.at[1])
    own_blocks.start()
    own_ops = pltpu.make_async_copy(op_ref.at[mine, :], ops.at[:, from_source(k)], own_copy.at[2])
    own_ops.start()

    rounds = g.bit_length() - 1
    barrier = pltpu.get_barrier_semaphore()

    def signal(sem, gx, gy):
        pl.semaphore_signal(sem, inc=1, device_id=(gx, gy), device_id_type=MESH)

    for b in range(rounds):
        signal(barrier, flip(1 << b), k)

    @pl.when(is_centre)
    def _():
        signal(barrier, j, other)
        for d in range(1, half):
            signal(barrier, j, near(d))

    pl.semaphore_wait(barrier, rounds + 1)

    def plane_entered():
        for b in range(rounds):
            signal(ready.at[b], flip(1 << b), k)
            pl.semaphore_wait(ready.at[b], 1)

    def remote(src, dst, send, recv, gx, gy):
        return pltpu.make_async_remote_copy(
            src_ref=src, dst_ref=dst, send_sem=send, recv_sem=recv,
            device_id=(gx, gy), device_id_type=MESH)

    def lanes(i):
        return pl.ds(pl.multiple_of(lax.rem(i, parts) * width, width), width)

    def block_part(s, i):
        return blocks.at[lax.div(i, parts), from_source(s), lanes(i)]

    def last_plane(s):
        return blocks.at[planes - 1, from_source(s), :]

    sources = [near(d) for d in range(1, half)] + [far(d) for d in range(half)]

    def hops(owner):
        d, chip = owner
        return bin(chip).count("1") - d, chip

    pairs = sorted(((d, chip) for d in range(half) for chip in range(g // 2)), key=hops)
    outer_first = list(reversed(range(half)))

    def own_part():
        part[...] = jnp.dot(far_ops[...], last_plane(k)[...], preferred_element_type=jnp.float32)

    @pl.when(is_centre)
    def _():
        def block_out(i):
            at = block_part(k, i)
            remote(at, at, own_send, blk_recv.at[half - 1, i], j, other).start()

        own_far.wait()
        for d in outer_first:
            remote(far_ops.at[far_rows(d, j), :], ops.at[far_rows(d, j), from_source(k)],
                   op_send, op_recv.at[half - 1, d], j, other).start()
        own_blocks.wait()
        block_out(0)
        block_out(1)
        own_part()

        def spread(e, d, at, mask):
            part_of = ops.at[near_rows(d, at), from_source(sources[e])]
            sem = sibling_recv.at[d] if mask == 1 else plane_recv.at[e, d]
            remote(part_of, part_of, spread_send.at[e], sem, flip(mask), k).start()

        adjacent = [1 << b for b in reversed(range(rounds))]
        distant = [2 * m for m in range(1, g // 2) if 2 * m not in adjacent]

        def enter(e, d):
            wait_bytes(op_bytes(1), op_recv.at[e, d])
            for mask in adjacent:
                spread(e, d, j, mask)

        def enter_distant(e, d):
            for mask in distant:
                spread(e, d, j, mask)

        def share(d):
            for e in range(len(sources)):
                wait_bytes(op_bytes(g // 2 - 1), plane_recv.at[e, d])
                for mask in range(1, g // 2):
                    spread(e, d, flip(2 * mask), 1)

        def complete(d):
            wait_bytes(op_bytes(len(sources) * (g // 2)), sibling_recv.at[d])

        def pass_on(d):
            for m in range(half - 1):
                wait_bytes(op_bytes(1), pass_recv.at[m, d])
                remote(passing.at[m, d], ops.at[far_rows(d, j), from_source(near(m + 1))],
                       op_send, op_recv.at[half + m, d], j, other).start()

        def forward(i):
            for m in range(half - 1):
                at = block_part(near(m + 1), i)
                wait_bytes(at, blk_recv.at[m, i])
                remote(at, at, fwd_send.at[m], blk_recv.at[half + m, i], j, other).start()

        closest, rest = range(half), range(half, 2 * half - 1)
        first = half - 1
        for e in closest[:1]:
            enter(e, first)
        plane_entered()
        for e in closest[:1]:
            enter_distant(e, first)
        for e in closest[1:]:
            enter(e, first)
            enter_distant(e, first)
        for d in outer_first:
            pass_on(d)
        block_out(2)
        for e in rest:
            enter(e, first)
            enter_distant(e, first)
        for d in outer_first[1:]:
            for e in range(len(sources)):
                enter(e, d)
                enter_distant(e, d)
        forward(0)
        forward(1)
        own_ops.wait()
        share(first)
        complete(first)
        if half > 1:
            pl.semaphore_wait(ready.at[rounds], half - 1)
        forward(2)
        for i in range(3, raw):
            block_out(i)

        band_of = lambda d: from_source(near(d) - side * half)
        others = pl.ds(pl.multiple_of(side * rows, rows), (n - 1) * rows)
        final = far(half - 1)

        def results(d, c, lane, size):
            target = pl.ds(pl.multiple_of(j * cols + lane, width), size)
            lane = pl.ds(lane, size)

            def result(to):
                return res.at[d, c, pl.ds(pl.multiple_of(to * outrows, outrows), outrows), lane]

            @pl.when(d > 0)
            def _():
                for to in range(g):
                    remote(result(to), out_ref.at[c, :, target], res_send.at[d], out_recv.at[0], to, near(d)).start()

            @pl.when(d == 0)
            def _():
                for mask in range(1, g):
                    to = flip(mask)
                    remote(result(to), out_ref.at[c, :, target], res_send.at[d], out_recv.at[0], to, near(d)).start()
                pltpu.make_async_copy(result(j), out_ref.at[c, :, target], out_recv.at[0]).start()

        def product(d, c, lane, i_first, count):
            band = band_of(d)

            @pl.when(d == first)
            def _():
                for e in range(half - 1):
                    for i in range(count):
                        wait_bytes(block_part(0, 0), blk_recv.at[half - 1 + e, i_first + i])
            size = lane.size
            ahead = wide.at[:, pl.ds(0, size)]
            ahead[...] = jnp.dot(ops[band, others], blocks[c, others, lane], preferred_element_type=jnp.float32)

            @pl.when(d == first)
            def _():
                for i in range(count):
                    wait_bytes(block_part(0, 0), blk_recv.at[2 * half - 2, i_first + i])
            total = ahead[...] + jnp.dot(
                ops[band, from_source(final)], blocks[c, from_source(final), lane], preferred_element_type=jnp.float32)
            res[d, c, :, lane] = total.astype(res.dtype)

        def near_half():
            for m in range(half - 1):
                wait_bytes(last_plane(0), blk_recv.at[m, raw])
            near_sum[...] = jnp.dot(ops[:, mine], blocks[planes - 1, mine, :], preferred_element_type=jnp.float32)

        def far_half(at):
            d, chip = pairs[at]
            band = far_rows(d, 2 * chip, 2)
            total = part[band, :]
            for m in range(half - 1):
                wait_bytes(part_in.at[m, band, :], part_recv.at[m, at])
                total = total + part_in[m, band, :].astype(jnp.float32)
            far_out[band, :] = total.astype(far_out.dtype)
            remote(far_out.at[band, :], far_in.at[band, :], far_send, far_recv.at[at], j, other).start()

        def late_result(at):
            d, chip = pairs[at]
            band = near_rows(d, 2 * chip, 2)
            wait_bytes(far_in.at[band, :], far_recv.at[at])
            late[band, :] = (near_sum[band, :] + far_in[band, :].astype(jnp.float32)).astype(late.dtype)
            target = out_ref.at[planes - 1, :, pl.ds(pl.multiple_of(j * cols, cols), cols)]
            for to in (2 * chip, 2 * chip + 1):
                def send(to=to):
                    remote(late.at[near_rows(d, to), :], target, late_send, out_recv.at[1], to, near(d)).start()

                if d > 0:
                    send()
                else:
                    pl.when(j != to)(send)

                    @pl.when(j == to)
                    def _(to=to):
                        pltpu.make_async_copy(late.at[near_rows(d, to), :], target, out_recv.at[1]).start()

        def whole_plane(t, carry):
            c, d = lax.div(t, half), first - lax.rem(t, half)

            @pl.when(t == 1)
            def _():
                for e in outer_first[1:]:
                    share(e)
                    complete(e)
            product(d, c, pl.ds(0, cols), c * parts, parts)
            results(d, c, 0, cols)

            @pl.when(t == 0)
            def _():
                for i in range(3, raw):
                    forward(i)
            return carry

        def one_chunk(t, carry):
            h, d = lax.div(t, half), first - lax.rem(t, half)
            at = pl.multiple_of(h * width, width)

            @pl.when(t == half * (parts - 1))
            def _():
                for e in range(len(pairs) // 2):
                    far_half(e)
            i = (planes - 2) * parts + h
            product(d, planes - 2, pl.ds(at, width), i, 1)
            results(d, planes - 2, at, width)
            return carry

        lax.fori_loop(0, half * (planes - 2), whole_plane, 0)
        lax.fori_loop(0, half * parts, one_chunk, 0)
        near_half()
        split = len(pairs) // 2
        for at in range(split, len(pairs)):
            far_half(at)
            late_result(at - split)
        for at in range(len(pairs) - split, len(pairs)):
            late_result(at)
        wait_bytes(op_bytes(half * half), op_send)
        wait_bytes(blocks.at[pl.ds(0, planes - 1), from_source(0), :], own_send)
        for m in range(half - 1):
            wait_bytes(blocks.at[pl.ds(0, planes - 1), from_source(0), :], fwd_send.at[m])
        for d in range(half):
            sent = rows - outrows if d == 0 else rows
            wait_bytes(res.at[d, pl.ds(0, planes - 1), pl.ds(0, sent), :], res_send.at[d])
        for e in range(len(sources)):
            wait_bytes(op_bytes(half * (g - 1)), spread_send.at[e])
        wait_bytes(far_out, far_send)
        wait_bytes(late.at[pl.ds(0, half * rows - outrows), :], late_send)

    @pl.when(jnp.logical_not(is_centre))
    def _():
        m = away - 1

        def op_in(d):
            at = ops.at[near_rows(d, j), from_source(k)]
            remote(at, at, op_send, op_recv.at[m, d], j, centre).start()

        def op_past(d):
            remote(far_ops.at[far_rows(d, j), :], passing.at[m, d], op_send, pass_recv.at[m, d], j, centre).start()

        own_ops.wait()
        op_in(half - 1)
        own_far.wait()
        for d in outer_first:
            op_past(d)
        for d in outer_first[1:]:
            op_in(d)
        own_blocks.wait()
        for i in range(raw):
            at = block_part(k, i)
            remote(at, at, own_send, blk_recv.at[m, i], j, centre).start()
        own_part()
        part_out[...] = part[...].astype(part_out.dtype)
        for at, (d, chip) in enumerate(pairs):
            if at == len(pairs) // 2:
                remote(last_plane(k), last_plane(k), own_send, blk_recv.at[m, raw], j, centre).start()
            band = far_rows(d, 2 * chip, 2)
            remote(part_out.at[band, :], part_in.at[m, band, :], part_send, part_recv.at[m, at], j, centre).start()
        plane_entered()
        signal(ready.at[rounds], j, centre)
        wait_bytes(op_bytes(2 * half), op_send)
        wait_bytes(blocks.at[:, from_source(0), :], own_send)
        wait_bytes(part_out, part_send)

    wait_bytes(out_ref.at[pl.ds(0, planes - 1)], out_recv.at[0])
    wait_bytes(out_ref.at[planes - 1], out_recv.at[1])


def at_centres(n, g, products, operator):
    rows, planes, cols = products.shape
    parts = 2 if cols % (2 * LANES) == 0 else 1
    half = n // 2
    outer, roles, raw = max(half - 1, 1), 2 * half - 1, (planes - 1) * parts
    out = pl.pallas_call(
        functools.partial(kernel, n, g, parts),
        out_shape=jax.ShapeDtypeStruct((planes, rows // g, cols * g), jnp.bfloat16),
        in_specs=[pl.BlockSpec(memory_space=pl.ANY)] * 2,
        out_specs=pl.BlockSpec(memory_space=pl.ANY),
        scratch_shapes=[
            pltpu.VMEM((planes, n * rows, cols), jnp.bfloat16),
            pltpu.VMEM((half * rows, n * rows), jnp.bfloat16),
            pltpu.VMEM((half * rows, rows), jnp.bfloat16),
            pltpu.VMEM((outer, half, rows // g, rows), jnp.bfloat16),
            pltpu.VMEM((half, planes - 1, rows, cols), jnp.bfloat16),
            pltpu.VMEM((rows, cols), jnp.float32),
            pltpu.VMEM((half * rows, cols), jnp.float32),
            pltpu.VMEM((half * rows, cols), jnp.bfloat16),
            pltpu.VMEM((outer, half * rows, cols), jnp.bfloat16),
            pltpu.VMEM((half * rows, cols), jnp.bfloat16),
            pltpu.VMEM((half * rows, cols), jnp.bfloat16),
            pltpu.VMEM((half * rows, cols), jnp.float32),
            pltpu.VMEM((half * rows, cols), jnp.bfloat16),
            pltpu.SemaphoreType.DMA,
            pltpu.SemaphoreType.DMA((outer,)),
            pltpu.SemaphoreType.DMA,
            pltpu.SemaphoreType.DMA((roles,)),
            pltpu.SemaphoreType.DMA((half,)),
            pltpu.SemaphoreType.DMA,
            pltpu.SemaphoreType.DMA,
            pltpu.SemaphoreType.DMA,
            pltpu.SemaphoreType.DMA((roles, raw + 1)),
            pltpu.SemaphoreType.DMA((roles, half)),
            pltpu.SemaphoreType.DMA((outer, half)),
            pltpu.SemaphoreType.DMA((roles, half)),
            pltpu.SemaphoreType.DMA((half,)),
            pltpu.SemaphoreType.DMA((2,)),
            pltpu.SemaphoreType.DMA((outer, half * g // 2)),
            pltpu.SemaphoreType.DMA((half * g // 2,)),
            pltpu.SemaphoreType.DMA((3,)),
            pltpu.SemaphoreType.REGULAR((g.bit_length(),)),
        ],
        compiler_params=pltpu.CompilerParams(
            collective_id=0, has_side_effects=True, vmem_limit_bytes=GRANT),
    )(products.transpose(1, 0, 2), operator)
    return out.transpose(1, 0, 2)


def by_collectives(products, operator):
    y_local, three, m_local = products.shape
    flat = products.reshape(y_local, three * m_local)
    summed = lax.psum_scatter(
        jnp.dot(operator, flat, preferred_element_type=jnp.float32), "gy", scatter_dimension=0, tiled=True)
    result = summed.astype(jnp.bfloat16).reshape(y_local, three, m_local)
    return lax.all_to_all(result, "gx", split_axis=0, concat_axis=2, tiled=True)


def solution(mesh):
    n, g = mesh.shape["gy"], mesh.shape["gx"]

    def body(products, operator):
        rows, planes, cols = products.shape
        aligned = (n % 2 == 0 and n > 2 and planes > 2 and g & (g - 1) == 0 and g > 1 and rows % (g * SUBLANES) == 0
                   and rows % LANES == 0 and cols % LANES == 0)
        held = 2 * (products.size * (n + n // 2 + 2) + operator.size * (2 + n // 2)) + 20 * n * rows * cols
        if aligned and held < VMEM_BYTES // 2:
            return at_centres(n, g, products, operator)
        return by_collectives(products, operator)

    return jax.shard_map(
        body,
        mesh=mesh,
        in_specs=(P("gy", None, "gx"), P(None, "gy")),
        out_specs=P(("gy", "gx"), None, None),
        check_vma=False,
    )
```

```python
import functools

import jax
import jax.numpy as jnp
from jax import lax
from jax.experimental import pallas as pl
from jax.experimental.pallas import tpu as pltpu
from jax.sharding import PartitionSpec as P

MESH = pl.DeviceIdType.MESH
LANES = 128
SUBLANES = 16
VMEM_BYTES = 60 * 1024 * 1024
GRANT = 54500 * 1024


def kernel(n, g, parts, p_ref, op_ref, out_ref, blocks, ops, far_ops, first_ops, passing, res, wide, part, part_out, part_in,
           far_out, far_in, near_sum, near_out, late, terms, last, own_send, fwd_send, op_send, spread_send, res_send, part_send, far_send,
           late_send, near_send, blk_recv, op_recv, pass_recv, plane_recv, sibling_recv, out_recv, part_recv, far_recv, terms_recv, own_copy,
           ready):
    j, k = lax.axis_index("gx"), lax.axis_index("gy")
    half = n // 2
    side = lax.div(k, half)
    step = 1 - 2 * side
    centre = jnp.where(side == 0, half - 1, half)
    other = n - 1 - centre
    is_centre = k == centre
    away = step * (centre - k)
    planes, rows, cols = p_ref.shape
    width = cols // parts
    raw = (planes - 1) * parts
    outrows = rows // g
    mine = pl.ds(pl.multiple_of(side * (half * rows), half * rows), half * rows)
    theirs = pl.ds(pl.multiple_of((1 - side) * (half * rows), half * rows), half * rows)

    def flip(mask):
        to = j
        for bit in (1 << b for b in range(mask.bit_length())):
            if mask & bit:
                to = to + bit * (1 - 2 * lax.rem(lax.div(j, bit), 2))
        return to

    def near(d):
        return centre - step * d

    def far(d):
        return other + step * d

    def from_source(s):
        return pl.ds(pl.multiple_of(s * rows, rows), rows)

    def near_rows(d, to, count=1):
        at = (near(d) - side * half) * rows + to * outrows
        return pl.ds(pl.multiple_of(at, outrows), count * outrows)

    def far_rows(d, to, count=1):
        at = (far(d) - (1 - side) * half) * rows + to * outrows
        return pl.ds(pl.multiple_of(at, outrows), count * outrows)

    def wait_bytes(ref, sem):
        pltpu.make_async_copy(ref, ref, sem).wait()

    def op_bytes(pieces):
        return ops.at[pl.ds(0, pieces * outrows), pl.ds(0, rows)]

    def staged(slot, d):
        at = far_rows(d, j) if slot == 0 else near_rows(d, j)
        start = (theirs if slot == 0 else mine).start
        return pltpu.make_async_copy(
            op_ref.at[pl.ds(pl.multiple_of(start + at.start, outrows), outrows), :], first_ops.at[slot, d],
            own_copy.at[2 * d + slot])

    own_start = pltpu.make_async_copy(
        p_ref.at[0, :, pl.ds(0, width)], blocks.at[0, from_source(k), pl.ds(0, width)], own_copy.at[2 * half])
    own_rest = [pltpu.make_async_copy(
        p_ref.at[0, :, pl.ds(width, cols - width)], blocks.at[0, from_source(k), pl.ds(width, cols - width)],
        own_copy.at[2 * half + 1])] if parts > 1 else []
    own_rest.append(pltpu.make_async_copy(
        p_ref.at[pl.ds(1, planes - 1)], blocks.at[pl.ds(1, planes - 1), from_source(k), :], own_copy.at[2 * half + 2]))
    own_far = pltpu.make_async_copy(op_ref.at[theirs, :], far_ops, own_copy.at[2 * half + 3])
    own_ops = pltpu.make_async_copy(op_ref.at[mine, :], ops.at[:, from_source(k)], own_copy.at[2 * half + 4])
    for d in reversed(range(half)):
        for slot in (1, 0):
            staged(slot, d).start()
    own_start.start()
    for rest_of in own_rest + [own_far, own_ops]:
        rest_of.start()

    rounds = g.bit_length() - 1
    barrier = pltpu.get_barrier_semaphore()

    def signal(sem, gx, gy):
        pl.semaphore_signal(sem, inc=1, device_id=(gx, gy), device_id_type=MESH)

    for b in range(rounds):
        signal(barrier, flip(1 << b), k)

    @pl.when(is_centre)
    def _():
        signal(barrier, j, other)
        for d in range(1, half):
            signal(barrier, j, near(d))

    pl.semaphore_wait(barrier, rounds + 1)

    def plane_entered():
        for b in range(rounds):
            signal(ready.at[b], flip(1 << b), k)
            pl.semaphore_wait(ready.at[b], 1)

    def remote(src, dst, send, recv, gx, gy):
        return pltpu.make_async_remote_copy(
            src_ref=src, dst_ref=dst, send_sem=send, recv_sem=recv,
            device_id=(gx, gy), device_id_type=MESH)

    def lanes(i):
        return pl.ds(pl.multiple_of(lax.rem(i, parts) * width, width), width)

    def block_part(s, i):
        return blocks.at[lax.div(i, parts), from_source(s), lanes(i)]

    def last_plane(s):
        return blocks.at[planes - 1, from_source(s), :]

    sources = [near(d) for d in range(1, half)] + [far(d) for d in range(half)]

    chips = g // 2
    column = lax.div(j, 2)

    def pick(at):
        chip = jnp.int32(0)
        for c in range(chips):
            order = sorted(range(1, chips), key=lambda x: (-bin(x ^ c).count("1"), x))
            chip = jnp.where(column == c, order[at], chip)
        return chip

    held_back = half * chips * 3 // 4
    turns = [pick(at) for at in range(chips - 1)]
    outer_first = list(reversed(range(half)))
    pairs = [(d, 0) for d in outer_first[:-1]] + [(d, chip) for d in outer_first[:-1] for chip in turns]
    joined = len(pairs)
    pairs += [(0, chip) for chip in [0] + turns]

    def own_part():
        part[...] = jnp.dot(far_ops[...], last_plane(k)[...], preferred_element_type=jnp.float32)

    @pl.when(is_centre)
    def _():
        def block_out(i):
            at = block_part(k, i)
            remote(at, at, own_send, blk_recv.at[half - 1, i], j, other).start()

        for d in outer_first:
            staged(0, d).wait()
            remote(first_ops.at[0, d], ops.at[far_rows(d, j), from_source(k)],
                   op_send, op_recv.at[half - 1, d], j, other).start()
        own_start.wait()
        block_out(0)
        for rest_of in own_rest:
            rest_of.wait()
        block_out(1)
        for d in outer_first:
            staged(1, d).wait()
        own_far.wait()
        own_part()

        def spread(e, d, at, mask):
            part_of = ops.at[near_rows(d, at), from_source(sources[e])]
            sem = sibling_recv.at[d] if mask == 1 else plane_recv.at[e, d]
            remote(part_of, part_of, spread_send.at[e], sem, flip(mask), k).start()

        adjacent = [1 << b for b in reversed(range(rounds))]
        distant = [2 * m for m in range(1, g // 2) if 2 * m not in adjacent]

        def enter(e, d):
            wait_bytes(op_bytes(1), op_recv.at[e, d])
            for mask in adjacent:
                spread(e, d, j, mask)

        def enter_distant(e, d):
            for mask in distant:
                spread(e, d, j, mask)

        def share(d):
            for e in range(len(sources)):
                wait_bytes(op_bytes(g // 2 - 1), plane_recv.at[e, d])
                for mask in range(1, g // 2):
                    spread(e, d, flip(2 * mask), 1)

        def complete(d):
            wait_bytes(op_bytes(len(sources) * (g // 2)), sibling_recv.at[d])

        def pass_on(d):
            for m in range(half - 1):
                wait_bytes(op_bytes(1), pass_recv.at[m, d])
                remote(passing.at[m, d], ops.at[far_rows(d, j), from_source(near(m + 1))],
                       op_send, op_recv.at[half + m, d], j, other).start()

        def forward(i):
            for m in range(half - 1):
                at = block_part(near(m + 1), i)
                wait_bytes(at, blk_recv.at[m, i])
                remote(at, at, fwd_send.at[m], blk_recv.at[half + m, i], j, other).start()

        closest, rest = range(half), range(half, 2 * half - 1)
        first = half - 1
        for e in closest[:1]:
            enter(e, first)
        plane_entered()
        signal(ready.at[rounds + 1], j, other)
        for e in closest[:1]:
            enter_distant(e, first)
        for e in closest[1:]:
            enter(e, first)
            enter_distant(e, first)
        for d in outer_first:
            pass_on(d)
        block_out(2)
        for e in rest:
            enter(e, first)
            enter_distant(e, first)
        for d in outer_first[1:]:
            for e in range(len(sources)):
                enter(e, d)
                enter_distant(e, d)
        forward(0)
        forward(1)
        own_ops.wait()
        share(first)
        complete(first)
        if half > 1:
            pl.semaphore_wait(ready.at[rounds], half - 1)
        forward(2)
        for i in range(3, raw):
            block_out(i)

        band_of = lambda d: from_source(near(d) - side * half)
        others = pl.ds(pl.multiple_of(side * rows, rows), (n - 1) * rows)
        final = far(half - 1)

        def results(d, c, lane, size):
            target = pl.ds(pl.multiple_of(j * cols + lane, width), size)
            lane = pl.ds(lane, size)

            def result(to):
                return res.at[d, c, pl.ds(pl.multiple_of(to * outrows, outrows), outrows), lane]

            @pl.when(d > 0)
            def _():
                for to in range(g):
                    remote(result(to), out_ref.at[c, :, target], res_send.at[d], out_recv.at[0], to, near(d)).start()

            @pl.when(d == 0)
            def _():
                for mask in range(1, g):
                    to = flip(mask)
                    remote(result(to), out_ref.at[c, :, target], res_send.at[d], out_recv.at[0], to, near(d)).start()
                pltpu.make_async_copy(result(j), out_ref.at[c, :, target], out_recv.at[0]).start()

        def product(d, c, lane, i_first, count):
            band = band_of(d)

            @pl.when(d == first)
            def _():
                for e in range(half - 1):
                    for i in range(count):
                        wait_bytes(block_part(0, 0), blk_recv.at[half - 1 + e, i_first + i])
            size = lane.size
            ahead = wide.at[:, pl.ds(0, size)]
            ahead[...] = jnp.dot(ops[band, others], blocks[c, others, lane], preferred_element_type=jnp.float32)

            @pl.when(d == first)
            def _():
                for i in range(count):
                    wait_bytes(block_part(0, 0), blk_recv.at[2 * half - 2, i_first + i])
            total = ahead[...] + jnp.dot(
                ops[band, from_source(final)], blocks[c, from_source(final), lane], preferred_element_type=jnp.float32)
            res[d, c, :, lane] = total.astype(res.dtype)

        def near_half():
            for m in range(half - 1):
                wait_bytes(last_plane(0), blk_recv.at[m, raw])
            near_sum[...] = jnp.dot(ops[:, mine], blocks[planes - 1, mine, :], preferred_element_type=jnp.float32)
            near_out[...] = near_sum[band_of(0), :].astype(near_out.dtype)
            target = terms.at[1, :, pl.ds(pl.multiple_of(j * cols, cols), cols)]

            def term(to):
                return near_out.at[pl.ds(pl.multiple_of(to * outrows, outrows), outrows), :]
            for mask in reversed(range(1, g)):
                remote(term(flip(mask)), target, near_send, terms_recv.at[1], flip(mask), k).start()
            pltpu.make_async_copy(term(j), target, terms_recv.at[1]).start()

        def far_half(at):
            d, chip = pairs[at]
            band = far_rows(d, 2 * chip, 2)
            total = part[band, :]
            for m in range(half - 1):
                wait_bytes(part_in.at[m, band, :], part_recv.at[m, at])
                total = total + part_in[m, band, :].astype(jnp.float32)
            far_out[band, :] = total.astype(far_out.dtype)
            if at < joined:
                remote(far_out.at[band, :], far_in.at[band, :], far_send, far_recv.at[at], j, other).start()
                return
            for to in (2 * chip, 2 * chip + 1):
                remote(far_out.at[far_rows(d, to), :], terms.at[0, :, pl.ds(pl.multiple_of(j * cols, cols), cols)],
                       far_send, terms_recv.at[0], to, other).start()

        def late_result(at):
            d, chip = pairs[at]
            band = near_rows(d, 2 * chip, 2)
            wait_bytes(far_in.at[band, :], far_recv.at[at])
            late[band, :] = (near_sum[band, :] + far_in[band, :].astype(jnp.float32)).astype(late.dtype)
            target = out_ref.at[planes - 1, :, pl.ds(pl.multiple_of(j * cols, cols), cols)]
            for to in (2 * chip, 2 * chip + 1):
                remote(late.at[near_rows(d, to), :], target, late_send, out_recv.at[1], to, near(d)).start()

        def whole_plane(t, carry):
            c, d = lax.div(t, half), first - lax.rem(t, half)

            @pl.when(t == 1)
            def _():
                for e in outer_first[1:]:
                    share(e)
                    complete(e)
            product(d, c, pl.ds(0, cols), c * parts, parts)
            results(d, c, 0, cols)

            @pl.when(t == 0)
            def _():
                for i in range(3, raw):
                    forward(i)
            return carry

        def one_chunk(t, carry):
            h, d = lax.div(t, half), first - lax.rem(t, half)
            at = pl.multiple_of(h * width, width)

            @pl.when(t == max(half * (parts - 1) - 1, 0))
            def _():
                for e in range(len(pairs) // 4):
                    far_half(e)

            @pl.when(t == half * (parts - 1))
            def _():
                for e in range(len(pairs) // 4, len(pairs) // 2):
                    far_half(e)
            i = (planes - 2) * parts + h
            product(d, planes - 2, pl.ds(at, width), i, 1)
            results(d, planes - 2, at, width)
            return carry

        lax.fori_loop(0, half * (planes - 2), whole_plane, 0)
        lax.fori_loop(0, half * parts, one_chunk, 0)
        pl.semaphore_wait(ready.at[rounds + 1], 1)
        for at in range(len(pairs) // 2, held_back):
            far_half(at)
        near_half()
        for at in range(max(joined, len(pairs) - held_back)):
            if held_back + at < len(pairs):
                far_half(held_back + at)
            if at < joined:
                late_result(at)
        wait_bytes(op_bytes(half * half), op_send)
        wait_bytes(blocks.at[pl.ds(0, planes - 1), from_source(0), :], own_send)
        for m in range(half - 1):
            wait_bytes(blocks.at[pl.ds(0, planes - 1), from_source(0), :], fwd_send.at[m])
        for d in range(half):
            sent = rows - outrows if d == 0 else rows
            wait_bytes(res.at[d, pl.ds(0, planes - 1), pl.ds(0, sent), :], res_send.at[d])
        for e in range(len(sources)):
            wait_bytes(op_bytes(half * (g - 1)), spread_send.at[e])
        wait_bytes(far_out, far_send)
        wait_bytes(late.at[pl.ds(0, (half - 1) * rows), :], late_send)
        wait_bytes(near_out.at[pl.ds(0, rows - outrows), :], near_send)
        for b in (1, 0):
            wait_bytes(terms.at[b], terms_recv.at[b])
        last[...] = (terms[0].astype(jnp.float32) + terms[1].astype(jnp.float32)).astype(last.dtype)
        pltpu.make_async_copy(last, out_ref.at[planes - 1], out_recv.at[1]).start()

    @pl.when(jnp.logical_not(is_centre))
    def _():
        m = away - 1

        def op_in(d):
            staged(1, d).wait()
            remote(first_ops.at[1, d], ops.at[near_rows(d, j), from_source(k)],
                   op_send, op_recv.at[m, d], j, centre).start()

        def op_past(d):
            staged(0, d).wait()
            remote(first_ops.at[0, d], passing.at[m, d], op_send, pass_recv.at[m, d], j, centre).start()

        op_in(half - 1)
        for d in outer_first:
            op_past(d)
        for d in outer_first[1:]:
            op_in(d)
        for rest_of in [own_start] + own_rest:
            rest_of.wait()
        for i in range(raw):
            at = block_part(k, i)
            remote(at, at, own_send, blk_recv.at[m, i], j, centre).start()
        own_far.wait()
        own_ops.wait()
        own_part()
        part_out[...] = part[...].astype(part_out.dtype)
        for at, (d, chip) in enumerate(pairs):
            if at == held_back:
                remote(last_plane(k), last_plane(k), own_send, blk_recv.at[m, raw], j, centre).start()
            band = far_rows(d, 2 * chip, 2)
            remote(part_out.at[band, :], part_in.at[m, band, :], part_send, part_recv.at[m, at], j, centre).start()
        plane_entered()
        signal(ready.at[rounds], j, centre)
        wait_bytes(op_bytes(2 * half), op_send)
        wait_bytes(blocks.at[:, from_source(0), :], own_send)
        wait_bytes(part_out, part_send)

    wait_bytes(out_ref.at[pl.ds(0, planes - 1)], out_recv.at[0])
    wait_bytes(out_ref.at[planes - 1], out_recv.at[1])


def at_centres(n, g, products, operator):
    rows, planes, cols = products.shape
    parts = 2 if cols % (2 * LANES) == 0 else 1
    half = n // 2
    outer, roles, raw = max(half - 1, 1), 2 * half - 1, (planes - 1) * parts
    out = pl.pallas_call(
        functools.partial(kernel, n, g, parts),
        out_shape=jax.ShapeDtypeStruct((planes, rows // g, cols * g), jnp.bfloat16),
        in_specs=[pl.BlockSpec(memory_space=pl.ANY)] * 2,
        out_specs=pl.BlockSpec(memory_space=pl.ANY),
        scratch_shapes=[
            pltpu.VMEM((planes, n * rows, cols), jnp.bfloat16),
            pltpu.VMEM((half * rows, n * rows), jnp.bfloat16),
            pltpu.VMEM((half * rows, rows), jnp.bfloat16),
            pltpu.VMEM((2, half, rows // g, rows), jnp.bfloat16),
            pltpu.VMEM((outer, half, rows // g, rows), jnp.bfloat16),
            pltpu.VMEM((half, planes - 1, rows, cols), jnp.bfloat16),
            pltpu.VMEM((rows, cols), jnp.float32),
            pltpu.VMEM((half * rows, cols), jnp.float32),
            pltpu.VMEM((half * rows, cols), jnp.bfloat16),
            pltpu.VMEM((outer, half * rows, cols), jnp.bfloat16),
            pltpu.VMEM((half * rows, cols), jnp.bfloat16),
            pltpu.VMEM((half * rows, cols), jnp.bfloat16),
            pltpu.VMEM((half * rows, cols), jnp.float32),
            pltpu.VMEM((rows, cols), jnp.bfloat16),
            pltpu.VMEM((half * rows, cols), jnp.bfloat16),
            pltpu.VMEM((2, rows // g, g * cols), jnp.bfloat16),
            pltpu.VMEM((rows // g, g * cols), jnp.bfloat16),
            pltpu.SemaphoreType.DMA,
            pltpu.SemaphoreType.DMA((outer,)),
            pltpu.SemaphoreType.DMA,
            pltpu.SemaphoreType.DMA((roles,)),
            pltpu.SemaphoreType.DMA((half,)),
            pltpu.SemaphoreType.DMA,
            pltpu.SemaphoreType.DMA,
            pltpu.SemaphoreType.DMA,
            pltpu.SemaphoreType.DMA,
            pltpu.SemaphoreType.DMA((roles, raw + 1)),
            pltpu.SemaphoreType.DMA((roles, half)),
            pltpu.SemaphoreType.DMA((outer, half)),
            pltpu.SemaphoreType.DMA((roles, half)),
            pltpu.SemaphoreType.DMA((half,)),
            pltpu.SemaphoreType.DMA((2,)),
            pltpu.SemaphoreType.DMA((outer, half * g // 2)),
            pltpu.SemaphoreType.DMA((outer * g // 2,)),
            pltpu.SemaphoreType.DMA((2,)),
            pltpu.SemaphoreType.DMA((2 * half + 5,)),
            pltpu.SemaphoreType.REGULAR((g.bit_length() + 1,)),
        ],
        compiler_params=pltpu.CompilerParams(
            collective_id=0, has_side_effects=True, vmem_limit_bytes=GRANT),
    )(products.transpose(1, 0, 2), operator)
    return out.transpose(1, 0, 2)


def by_collectives(products, operator):
    y_local, three, m_local = products.shape
    flat = products.reshape(y_local, three * m_local)
    summed = lax.psum_scatter(
        jnp.dot(operator, flat, preferred_element_type=jnp.float32), "gy", scatter_dimension=0, tiled=True)
    result = summed.astype(jnp.bfloat16).reshape(y_local, three, m_local)
    return lax.all_to_all(result, "gx", split_axis=0, concat_axis=2, tiled=True)


def solution(mesh):
    n, g = mesh.shape["gy"], mesh.shape["gx"]

    def body(products, operator):
        rows, planes, cols = products.shape
        aligned = (n % 2 == 0 and n > 2 and planes > 2 and g & (g - 1) == 0 and g > 1 and rows % (g * SUBLANES) == 0
                   and rows % LANES == 0 and cols % LANES == 0)
        held = 2 * (products.size * (n + n // 2 + 2) + operator.size * (2 + n // 2)) + 20 * n * rows * cols
        if aligned and held < VMEM_BYTES // 2:
            return at_centres(n, g, products, operator)
        return by_collectives(products, operator)

    return jax.shard_map(
        body,
        mesh=mesh,
        in_specs=(P("gy", None, "gx"), P(None, "gy")),
        out_specs=P(("gy", "gx"), None, None),
        check_vma=False,
    )
```

```python
import functools

import jax
import jax.numpy as jnp
from jax import lax
from jax.experimental import pallas as pl
from jax.experimental.pallas import tpu as pltpu
from jax.sharding import PartitionSpec as P

MESH = pl.DeviceIdType.MESH
LANES = 128
SUBLANES = 16
VMEM_BYTES = 60 * 1024 * 1024
GRANT = 54500 * 1024


def kernel(n, g, parts, p_ref, op_ref, out_ref, blocks, ops, far_ops, first_ops, passing, res, wide, part, part_out, part_in,
           far_out, far_in, near_sum, near_out, late, terms, last, own_send, fwd_send, op_send, spread_send, res_send, part_send, far_send,
           late_send, near_send, blk_recv, op_recv, pass_recv, plane_recv, sibling_recv, out_recv, part_recv, far_recv, terms_recv, own_copy,
           ready):
    j, k = lax.axis_index("gx"), lax.axis_index("gy")
    half = n // 2
    side = lax.div(k, half)
    step = 1 - 2 * side
    centre = jnp.where(side == 0, half - 1, half)
    other = n - 1 - centre
    is_centre = k == centre
    away = step * (centre - k)
    planes, rows, cols = p_ref.shape
    width = cols // parts
    raw = (planes - 1) * parts
    outrows = rows // g
    mine = pl.ds(pl.multiple_of(side * (half * rows), half * rows), half * rows)
    theirs = pl.ds(pl.multiple_of((1 - side) * (half * rows), half * rows), half * rows)

    def flip(mask):
        to = j
        for bit in (1 << b for b in range(mask.bit_length())):
            if mask & bit:
                to = to + bit * (1 - 2 * lax.rem(lax.div(j, bit), 2))
        return to

    def near(d):
        return centre - step * d

    def far(d):
        return other + step * d

    def from_source(s):
        return pl.ds(pl.multiple_of(s * rows, rows), rows)

    def near_rows(d, to, count=1):
        at = (near(d) - side * half) * rows + to * outrows
        return pl.ds(pl.multiple_of(at, outrows), count * outrows)

    def far_rows(d, to, count=1):
        at = (far(d) - (1 - side) * half) * rows + to * outrows
        return pl.ds(pl.multiple_of(at, outrows), count * outrows)

    def wait_bytes(ref, sem):
        pltpu.make_async_copy(ref, ref, sem).wait()

    def op_bytes(pieces):
        return ops.at[pl.ds(0, pieces * outrows), pl.ds(0, rows)]

    def staged(slot, d):
        at = far_rows(d, j) if slot == 0 else near_rows(d, j)
        start = (theirs if slot == 0 else mine).start
        return pltpu.make_async_copy(
            op_ref.at[pl.ds(pl.multiple_of(start + at.start, outrows), outrows), :], first_ops.at[slot, d],
            own_copy.at[2 * d + slot])

    own_start = pltpu.make_async_copy(
        p_ref.at[0, :, pl.ds(0, width)], blocks.at[0, from_source(k), pl.ds(0, width)], own_copy.at[2 * half])
    own_rest = [pltpu.make_async_copy(
        p_ref.at[0, :, pl.ds(width, cols - width)], blocks.at[0, from_source(k), pl.ds(width, cols - width)],
        own_copy.at[2 * half + 1])] if parts > 1 else []
    own_rest.append(pltpu.make_async_copy(
        p_ref.at[pl.ds(1, planes - 1)], blocks.at[pl.ds(1, planes - 1), from_source(k), :], own_copy.at[2 * half + 2]))
    own_far = pltpu.make_async_copy(op_ref.at[theirs, :], far_ops, own_copy.at[2 * half + 3])
    own_ops = pltpu.make_async_copy(op_ref.at[mine, :], ops.at[:, from_source(k)], own_copy.at[2 * half + 4])
    for d in reversed(range(half)):
        for slot in (1, 0):
            staged(slot, d).start()
    own_start.start()
    for rest_of in own_rest + [own_far, own_ops]:
        rest_of.start()

    rounds = g.bit_length() - 1
    barrier = pltpu.get_barrier_semaphore()

    def signal(sem, gx, gy):
        pl.semaphore_signal(sem, inc=1, device_id=(gx, gy), device_id_type=MESH)

    for b in range(rounds):
        signal(barrier, flip(1 << b), k)

    @pl.when(is_centre)
    def _():
        signal(barrier, j, other)
        for d in range(1, half):
            signal(barrier, j, near(d))

    pl.semaphore_wait(barrier, rounds + 1)

    def plane_entered():
        for b in range(rounds):
            signal(ready.at[b], flip(1 << b), k)
            pl.semaphore_wait(ready.at[b], 1)

    def remote(src, dst, send, recv, gx, gy):
        return pltpu.make_async_remote_copy(
            src_ref=src, dst_ref=dst, send_sem=send, recv_sem=recv,
            device_id=(gx, gy), device_id_type=MESH)

    def lanes(i):
        return pl.ds(pl.multiple_of(lax.rem(i, parts) * width, width), width)

    def block_part(s, i):
        return blocks.at[lax.div(i, parts), from_source(s), lanes(i)]

    def last_plane(s):
        return blocks.at[planes - 1, from_source(s), :]

    sources = [near(d) for d in range(1, half)] + [far(d) for d in range(half)]

    chips = g // 2
    column = lax.div(j, 2)

    def bits(x):
        return bin(x).count("1")

    def pick(at):
        chip = jnp.int32(0)
        for c in range(chips):
            order = sorted(range(1, chips), key=lambda x: (bits(x) - bits(x ^ c), x == c, x))
            chip = jnp.where(column == c, order[at], chip)
        return chip

    held_back = half * chips // 2
    turns = [pick(at) for at in range(chips - 1)]
    outer_first = list(reversed(range(half)))
    pairs = [(d, 0) for d in outer_first[:-1]] + [(d, chip) for d in outer_first[:-1] for chip in turns]
    joined = len(pairs)
    pairs += [(0, chip) for chip in [0] + turns]

    def own_part():
        part[...] = jnp.dot(far_ops[...], last_plane(k)[...], preferred_element_type=jnp.float32)

    @pl.when(is_centre)
    def _():
        def block_out(i):
            at = block_part(k, i)
            remote(at, at, own_send, blk_recv.at[half - 1, i], j, other).start()

        for d in outer_first:
            staged(0, d).wait()
            remote(first_ops.at[0, d], ops.at[far_rows(d, j), from_source(k)],
                   op_send, op_recv.at[half - 1, d], j, other).start()
        own_start.wait()
        block_out(0)
        for rest_of in own_rest:
            rest_of.wait()
        block_out(1)
        for d in outer_first:
            staged(1, d).wait()
        own_far.wait()
        own_part()

        def spread(e, d, at, mask):
            part_of = ops.at[near_rows(d, at), from_source(sources[e])]
            sem = sibling_recv.at[d] if mask == 1 else plane_recv.at[e, d]
            remote(part_of, part_of, spread_send.at[e], sem, flip(mask), k).start()

        adjacent = [1 << b for b in reversed(range(rounds))]
        distant = [2 * m for m in range(1, g // 2) if 2 * m not in adjacent]

        def enter(e, d, everywhere):
            wait_bytes(op_bytes(1), op_recv.at[e, d])
            for mask in (distant if everywhere else []) + adjacent:
                spread(e, d, j, mask)

        def share(d):
            for e in range(len(sources)):
                wait_bytes(op_bytes(g // 2 - 1), plane_recv.at[e, d])
                for mask in range(1, g // 2):
                    spread(e, d, flip(2 * mask), 1)

        def complete(d):
            wait_bytes(op_bytes(len(sources) * (g // 2)), sibling_recv.at[d])

        def pass_on(d):
            for m in range(half - 1):
                wait_bytes(op_bytes(1), pass_recv.at[m, d])
                remote(passing.at[m, d], ops.at[far_rows(d, j), from_source(near(m + 1))],
                       op_send, op_recv.at[half + m, d], j, other).start()

        def forward(i):
            for m in range(half - 1):
                at = block_part(near(m + 1), i)
                wait_bytes(at, blk_recv.at[m, i])
                remote(at, at, fwd_send.at[m], blk_recv.at[half + m, i], j, other).start()

        closest, rest = range(half), range(half, 2 * half - 1)
        first = half - 1
        enter(0, first, False)
        plane_entered()
        signal(ready.at[rounds + 1], j, other)
        for mask in distant:
            spread(0, first, j, mask)
        for e in closest[1:]:
            enter(e, first, True)
        for d in outer_first:
            pass_on(d)
        block_out(2)
        forward(0)
        for e in rest:
            enter(e, first, True)
        for d in outer_first[1:]:
            for e in range(len(sources)):
                enter(e, d, True)
        forward(1)
        own_ops.wait()
        share(first)
        forward(2)
        for i in range(3, raw):
            block_out(i)
        complete(first)
        if half > 1:
            pl.semaphore_wait(ready.at[rounds], half - 1)

        band_of = lambda d: from_source(near(d) - side * half)
        others = pl.ds(pl.multiple_of(side * rows, rows), (n - 1) * rows)
        final = far(half - 1)

        def results(d, c, lane, size):
            target = pl.ds(pl.multiple_of(j * cols + lane, width), size)
            lane = pl.ds(lane, size)

            def result(to):
                return res.at[d, c, pl.ds(pl.multiple_of(to * outrows, outrows), outrows), lane]

            @pl.when(d > 0)
            def _():
                for to in range(g):
                    remote(result(to), out_ref.at[c, :, target], res_send.at[d], out_recv.at[0], to, near(d)).start()

            @pl.when(d == 0)
            def _():
                for mask in range(1, g):
                    to = flip(mask)
                    remote(result(to), out_ref.at[c, :, target], res_send.at[d], out_recv.at[0], to, near(d)).start()
                pltpu.make_async_copy(result(j), out_ref.at[c, :, target], out_recv.at[0]).start()

        def product(d, c, lane, i_first, count):
            band = band_of(d)

            @pl.when(d == first)
            def _():
                for e in range(half - 1):
                    for i in range(count):
                        wait_bytes(block_part(0, 0), blk_recv.at[half - 1 + e, i_first + i])
            size = lane.size
            ahead = wide.at[:, pl.ds(0, size)]
            ahead[...] = jnp.dot(ops[band, others], blocks[c, others, lane], preferred_element_type=jnp.float32)

            @pl.when(d == first)
            def _():
                for i in range(count):
                    wait_bytes(block_part(0, 0), blk_recv.at[2 * half - 2, i_first + i])
            total = ahead[...] + jnp.dot(
                ops[band, from_source(final)], blocks[c, from_source(final), lane], preferred_element_type=jnp.float32)
            res[d, c, :, lane] = total.astype(res.dtype)

        def near_half():
            for m in range(half - 1):
                wait_bytes(last_plane(0), blk_recv.at[m, raw])
            near_sum[...] = jnp.dot(ops[:, mine], blocks[planes - 1, mine, :], preferred_element_type=jnp.float32)
            near_out[...] = near_sum[band_of(0), :].astype(near_out.dtype)
            target = terms.at[1, :, pl.ds(pl.multiple_of(j * cols, cols), cols)]

            def term(to):
                return near_out.at[pl.ds(pl.multiple_of(to * outrows, outrows), outrows), :]
            for mask in reversed(range(1, g)):
                remote(term(flip(mask)), target, near_send, terms_recv.at[1], flip(mask), k).start()
            pltpu.make_async_copy(term(j), target, terms_recv.at[1]).start()

        def far_half(at):
            d, chip = pairs[at]
            band = far_rows(d, 2 * chip, 2)
            total = part[band, :]
            for m in range(half - 1):
                wait_bytes(part_in.at[m, band, :], part_recv.at[m, at])
                total = total + part_in[m, band, :].astype(jnp.float32)
            far_out[band, :] = total.astype(far_out.dtype)
            if at < joined:
                remote(far_out.at[band, :], far_in.at[band, :], far_send, far_recv.at[at], j, other).start()
                return
            for to in (2 * chip, 2 * chip + 1):
                remote(far_out.at[far_rows(d, to), :], terms.at[0, :, pl.ds(pl.multiple_of(j * cols, cols), cols)],
                       far_send, terms_recv.at[0], to, other).start()

        def late_result(at):
            d, chip = pairs[at]
            band = near_rows(d, 2 * chip, 2)
            wait_bytes(far_in.at[band, :], far_recv.at[at])
            late[band, :] = (near_sum[band, :] + far_in[band, :].astype(jnp.float32)).astype(late.dtype)
            target = out_ref.at[planes - 1, :, pl.ds(pl.multiple_of(j * cols, cols), cols)]
            for to in (2 * chip, 2 * chip + 1):
                remote(late.at[near_rows(d, to), :], target, late_send, out_recv.at[1], to, near(d)).start()

        early = (planes - 2) * parts

        def one(t, carry):
            i = jnp.where(t < early, t, early + lax.div(t - early, half))
            d = jnp.where(t < early, first, first - lax.rem(t - early, half))
            c, h = lax.div(i, parts), lax.rem(i, parts)
            at = pl.multiple_of(h * width, width)

            @pl.when(t == 1)
            def _():
                for e in range(3, raw):
                    forward(e)

            @pl.when(t == early)
            def _():
                for e in outer_first[1:]:
                    share(e)
                    complete(e)

            @pl.when(t == early + 1)
            def _():
                near_half()
                far_half(0)
                for e in outer_first[1:]:
                    for whole in range(planes - 2):
                        product(jnp.int32(e), whole, pl.ds(0, cols), 0, 0)
                        results(jnp.int32(e), whole, 0, cols)
                far_half(1)

            @pl.when(t == early + 2)
            def _():
                far_half(2)

            @pl.when(t == last_turn)
            def _():
                far_half(3)
                late_result(0)
                pl.semaphore_wait(ready.at[rounds + 1], 1)
                far_half(4)
                late_result(1)

            product(d, c, pl.ds(at, width), i, 1)
            results(d, c, at, width)
            return carry

        last_turn = early + half * parts - 1
        lax.fori_loop(0, last_turn + 1, one, 0)
        for at in range(5, len(pairs)):
            far_half(at)
            if at - 3 < joined:
                late_result(at - 3)
        for at in range(len(pairs) - 3, joined):
            late_result(at)
        wait_bytes(op_bytes(half * half), op_send)
        wait_bytes(blocks.at[pl.ds(0, planes - 1), from_source(0), :], own_send)
        for m in range(half - 1):
            wait_bytes(blocks.at[pl.ds(0, planes - 1), from_source(0), :], fwd_send.at[m])
        for d in range(half):
            sent = rows - outrows if d == 0 else rows
            wait_bytes(res.at[d, pl.ds(0, planes - 1), pl.ds(0, sent), :], res_send.at[d])
        for e in range(len(sources)):
            wait_bytes(op_bytes(half * (g - 1)), spread_send.at[e])
        wait_bytes(far_out, far_send)
        wait_bytes(late.at[pl.ds(0, (half - 1) * rows), :], late_send)
        wait_bytes(near_out.at[pl.ds(0, rows - outrows), :], near_send)
        for b in (1, 0):
            wait_bytes(terms.at[b], terms_recv.at[b])
        last[...] = (terms[0].astype(jnp.float32) + terms[1].astype(jnp.float32)).astype(last.dtype)
        pltpu.make_async_copy(last, out_ref.at[planes - 1], out_recv.at[1]).start()

    @pl.when(jnp.logical_not(is_centre))
    def _():
        m = away - 1

        def op_in(d):
            staged(1, d).wait()
            remote(first_ops.at[1, d], ops.at[near_rows(d, j), from_source(k)],
                   op_send, op_recv.at[m, d], j, centre).start()

        def op_past(d):
            staged(0, d).wait()
            remote(first_ops.at[0, d], passing.at[m, d], op_send, pass_recv.at[m, d], j, centre).start()

        op_in(half - 1)
        for d in outer_first:
            op_past(d)
        for d in outer_first[1:]:
            op_in(d)
        for rest_of in [own_start] + own_rest:
            rest_of.wait()
        for i in range(raw):
            at = block_part(k, i)
            remote(at, at, own_send, blk_recv.at[m, i], j, centre).start()
        remote(last_plane(k), last_plane(k), own_send, blk_recv.at[m, raw], j, centre).start()
        own_far.wait()
        own_ops.wait()
        own_part()
        part_out[...] = part[...].astype(part_out.dtype)
        for at, (d, chip) in enumerate(pairs):
            band = far_rows(d, 2 * chip, 2)
            remote(part_out.at[band, :], part_in.at[m, band, :], part_send, part_recv.at[m, at], j, centre).start()
        plane_entered()
        signal(ready.at[rounds], j, centre)
        wait_bytes(op_bytes(2 * half), op_send)
        wait_bytes(blocks.at[:, from_source(0), :], own_send)
        wait_bytes(part_out, part_send)

    wait_bytes(out_ref.at[pl.ds(0, planes - 1)], out_recv.at[0])
    wait_bytes(out_ref.at[planes - 1], out_recv.at[1])


def at_centres(n, g, products, operator):
    rows, planes, cols = products.shape
    parts = 2 if cols % (2 * LANES) == 0 else 1
    half = n // 2
    outer, roles, raw = max(half - 1, 1), 2 * half - 1, (planes - 1) * parts
    out = pl.pallas_call(
        functools.partial(kernel, n, g, parts),
        out_shape=jax.ShapeDtypeStruct((planes, rows // g, cols * g), jnp.bfloat16),
        in_specs=[pl.BlockSpec(memory_space=pl.ANY)] * 2,
        out_specs=pl.BlockSpec(memory_space=pl.ANY),
        scratch_shapes=[
            pltpu.VMEM((planes, n * rows, cols), jnp.bfloat16),
            pltpu.VMEM((half * rows, n * rows), jnp.bfloat16),
            pltpu.VMEM((half * rows, rows), jnp.bfloat16),
            pltpu.VMEM((2, half, rows // g, rows), jnp.bfloat16),
            pltpu.VMEM((outer, half, rows // g, rows), jnp.bfloat16),
            pltpu.VMEM((half, planes - 1, rows, cols), jnp.bfloat16),
            pltpu.VMEM((rows, cols), jnp.float32),
            pltpu.VMEM((half * rows, cols), jnp.float32),
            pltpu.VMEM((half * rows, cols), jnp.bfloat16),
            pltpu.VMEM((outer, half * rows, cols), jnp.bfloat16),
            pltpu.VMEM((half * rows, cols), jnp.bfloat16),
            pltpu.VMEM((half * rows, cols), jnp.bfloat16),
            pltpu.VMEM((half * rows, cols), jnp.float32),
            pltpu.VMEM((rows, cols), jnp.bfloat16),
            pltpu.VMEM((half * rows, cols), jnp.bfloat16),
            pltpu.VMEM((2, rows // g, g * cols), jnp.bfloat16),
            pltpu.VMEM((rows // g, g * cols), jnp.bfloat16),
            pltpu.SemaphoreType.DMA,
            pltpu.SemaphoreType.DMA((outer,)),
            pltpu.SemaphoreType.DMA,
            pltpu.SemaphoreType.DMA((roles,)),
            pltpu.SemaphoreType.DMA((half,)),
            pltpu.SemaphoreType.DMA,
            pltpu.SemaphoreType.DMA,
            pltpu.SemaphoreType.DMA,
            pltpu.SemaphoreType.DMA,
            pltpu.SemaphoreType.DMA((roles, raw + 1)),
            pltpu.SemaphoreType.DMA((roles, half)),
            pltpu.SemaphoreType.DMA((outer, half)),
            pltpu.SemaphoreType.DMA((roles, half)),
            pltpu.SemaphoreType.DMA((half,)),
            pltpu.SemaphoreType.DMA((2,)),
            pltpu.SemaphoreType.DMA((outer, half * g // 2)),
            pltpu.SemaphoreType.DMA((outer * g // 2,)),
            pltpu.SemaphoreType.DMA((2,)),
            pltpu.SemaphoreType.DMA((2 * half + 5,)),
            pltpu.SemaphoreType.REGULAR((g.bit_length() + 1,)),
        ],
        compiler_params=pltpu.CompilerParams(
            collective_id=0, has_side_effects=True, vmem_limit_bytes=GRANT),
    )(products.transpose(1, 0, 2), operator)
    return out.transpose(1, 0, 2)


def by_collectives(products, operator):
    y_local, three, m_local = products.shape
    flat = products.reshape(y_local, three * m_local)
    summed = lax.psum_scatter(
        jnp.dot(operator, flat, preferred_element_type=jnp.float32), "gy", scatter_dimension=0, tiled=True)
    result = summed.astype(jnp.bfloat16).reshape(y_local, three, m_local)
    return lax.all_to_all(result, "gx", split_axis=0, concat_axis=2, tiled=True)


def solution(mesh):
    n, g = mesh.shape["gy"], mesh.shape["gx"]

    def body(products, operator):
        rows, planes, cols = products.shape
        aligned = (n // 2 == 2 and n % 2 == 0 and planes > 2 and g & (g - 1) == 0 and g > 1 and rows % (g * SUBLANES) == 0
                   and rows % LANES == 0 and cols % (2 * LANES) == 0)
        held = 2 * (products.size * (n + n // 2 + 2) + operator.size * (2 + n // 2)) + 20 * n * rows * cols
        if aligned and held < VMEM_BYTES // 2:
            return at_centres(n, g, products, operator)
        return by_collectives(products, operator)

    return jax.shard_map(
        body,
        mesh=mesh,
        in_specs=(P("gy", None, "gx"), P(None, "gy")),
        out_specs=P(("gy", "gx"), None, None),
        check_vma=False,
    )
```

```python
import functools

import jax
import jax.numpy as jnp
from jax import lax
from jax.experimental import pallas as pl
from jax.experimental.pallas import tpu as pltpu
from jax.sharding import PartitionSpec as P

MESH = pl.DeviceIdType.MESH
LANES = 128
SUBLANES = 16
VMEM_BYTES = 60 * 1024 * 1024
GRANT = 54500 * 1024


def kernel(n, g, parts, p_ref, op_ref, out_ref, blocks, ops, far_ops, first_ops, passing, res, wide, part, part_out, part_in,
           far_out, far_in, near_sum, near_out, late, terms, last, own_send, fwd_send, op_send, spread_send, res_send, part_send, far_send,
           late_send, near_send, blk_recv, op_recv, pass_recv, plane_recv, sibling_recv, out_recv, part_recv, far_recv, terms_recv, own_copy,
           ready):
    j, k = lax.axis_index("gx"), lax.axis_index("gy")
    half = n // 2
    side = lax.div(k, half)
    step = 1 - 2 * side
    centre = jnp.where(side == 0, half - 1, half)
    other = n - 1 - centre
    is_centre = k == centre
    away = step * (centre - k)
    planes, rows, cols = p_ref.shape
    width = cols // parts
    raw = (planes - 1) * parts
    outrows = rows // g
    mine = pl.ds(pl.multiple_of(side * (half * rows), half * rows), half * rows)
    theirs = pl.ds(pl.multiple_of((1 - side) * (half * rows), half * rows), half * rows)

    def flip(mask):
        to = j
        for bit in (1 << b for b in range(mask.bit_length())):
            if mask & bit:
                to = to + bit * (1 - 2 * lax.rem(lax.div(j, bit), 2))
        return to

    def near(d):
        return centre - step * d

    def far(d):
        return other + step * d

    def from_source(s):
        return pl.ds(pl.multiple_of(s * rows, rows), rows)

    def near_rows(d, to, count=1):
        at = (near(d) - side * half) * rows + to * outrows
        return pl.ds(pl.multiple_of(at, outrows), count * outrows)

    def far_rows(d, to, count=1):
        at = (far(d) - (1 - side) * half) * rows + to * outrows
        return pl.ds(pl.multiple_of(at, outrows), count * outrows)

    def wait_bytes(ref, sem):
        pltpu.make_async_copy(ref, ref, sem).wait()

    def op_bytes(pieces):
        return ops.at[pl.ds(0, pieces * outrows), pl.ds(0, rows)]

    def staged(slot, d):
        at = far_rows(d, j) if slot == 0 else near_rows(d, j)
        start = (theirs if slot == 0 else mine).start
        return pltpu.make_async_copy(
            op_ref.at[pl.ds(pl.multiple_of(start + at.start, outrows), outrows), :], first_ops.at[slot, d],
            own_copy.at[2 * d + slot])

    own_start = pltpu.make_async_copy(
        p_ref.at[0, :, pl.ds(0, width)], blocks.at[0, from_source(k), pl.ds(0, width)], own_copy.at[2 * half])
    own_rest = [pltpu.make_async_copy(
        p_ref.at[0, :, pl.ds(width, cols - width)], blocks.at[0, from_source(k), pl.ds(width, cols - width)],
        own_copy.at[2 * half + 1])] if parts > 1 else []
    own_rest.append(pltpu.make_async_copy(
        p_ref.at[pl.ds(1, planes - 1)], blocks.at[pl.ds(1, planes - 1), from_source(k), :], own_copy.at[2 * half + 2]))
    own_far = pltpu.make_async_copy(op_ref.at[theirs, :], far_ops, own_copy.at[2 * half + 3])
    own_ops = pltpu.make_async_copy(op_ref.at[mine, :], ops.at[:, from_source(k)], own_copy.at[2 * half + 4])
    for d in reversed(range(half)):
        for slot in (1, 0):
            staged(slot, d).start()
    own_start.start()
    for rest_of in own_rest + [own_far, own_ops]:
        rest_of.start()

    rounds = g.bit_length() - 1
    barrier = pltpu.get_barrier_semaphore()

    def signal(sem, gx, gy):
        pl.semaphore_signal(sem, inc=1, device_id=(gx, gy), device_id_type=MESH)

    for b in range(rounds):
        signal(barrier, flip(1 << b), k)

    @pl.when(is_centre)
    def _():
        signal(barrier, j, other)
        for d in range(1, half):
            signal(barrier, j, near(d))

    pl.semaphore_wait(barrier, rounds + 1)

    def plane_entered():
        for b in range(rounds):
            signal(ready.at[b], flip(1 << b), k)
            pl.semaphore_wait(ready.at[b], 1)

    def remote(src, dst, send, recv, gx, gy):
        return pltpu.make_async_remote_copy(
            src_ref=src, dst_ref=dst, send_sem=send, recv_sem=recv,
            device_id=(gx, gy), device_id_type=MESH)

    def lanes(i):
        return pl.ds(pl.multiple_of(lax.rem(i, parts) * width, width), width)

    def block_part(s, i):
        return blocks.at[lax.div(i, parts), from_source(s), lanes(i)]

    def last_plane(s):
        return blocks.at[planes - 1, from_source(s), :]

    sources = [near(d) for d in range(1, half)] + [far(d) for d in range(half)]

    chips = g // 2
    column = lax.div(j, 2)

    def bits(x):
        return bin(x).count("1")

    def pick(at):
        chip = jnp.int32(0)
        for c in range(chips):
            order = sorted(range(1, chips), key=lambda x: (bits(x) - bits(x ^ c), x == c, x))
            chip = jnp.where(column == c, order[at], chip)
        return chip

    held_back = half * chips // 2
    turns = [pick(at) for at in range(chips - 1)]
    outer_first = list(reversed(range(half)))
    pairs = [(d, 0) for d in outer_first[:-1]] + [(d, chip) for d in outer_first[:-1] for chip in turns]
    joined = len(pairs)
    pairs += [(0, chip) for chip in [0] + turns]

    def own_part():
        part[...] = jnp.dot(far_ops[...], last_plane(k)[...], preferred_element_type=jnp.float32)

    @pl.when(is_centre)
    def _():
        def block_out(i):
            at = block_part(k, i)
            remote(at, at, own_send, blk_recv.at[half - 1, i], j, other).start()

        for d in outer_first:
            staged(0, d).wait()
            remote(first_ops.at[0, d], ops.at[far_rows(d, j), from_source(k)],
                   op_send, op_recv.at[half - 1, d], j, other).start()
        own_start.wait()
        block_out(0)
        for rest_of in own_rest:
            rest_of.wait()
        block_out(1)
        for d in outer_first:
            staged(1, d).wait()
        own_far.wait()
        own_part()

        def spread(e, d, at, mask):
            part_of = ops.at[near_rows(d, at), from_source(sources[e])]
            sem = sibling_recv.at[d] if mask == 1 else plane_recv.at[e, d]
            remote(part_of, part_of, spread_send.at[e], sem, flip(mask), k).start()

        adjacent = [1 << b for b in reversed(range(rounds))]
        distant = [2 * m for m in range(1, g // 2) if 2 * m not in adjacent]

        def enter(e, d, everywhere):
            wait_bytes(op_bytes(1), op_recv.at[e, d])
            for mask in (distant if everywhere else []) + adjacent:
                spread(e, d, j, mask)

        def share(d):
            for e in range(len(sources)):
                wait_bytes(op_bytes(g // 2 - 1), plane_recv.at[e, d])
                for mask in range(1, g // 2):
                    spread(e, d, flip(2 * mask), 1)

        def complete(d):
            wait_bytes(op_bytes(len(sources) * (g // 2)), sibling_recv.at[d])

        def pass_on(d):
            for m in range(half - 1):
                wait_bytes(op_bytes(1), pass_recv.at[m, d])
                remote(passing.at[m, d], ops.at[far_rows(d, j), from_source(near(m + 1))],
                       op_send, op_recv.at[half + m, d], j, other).start()

        def forward(i):
            for m in range(half - 1):
                at = block_part(near(m + 1), i)
                wait_bytes(at, blk_recv.at[m, i])
                remote(at, at, fwd_send.at[m], blk_recv.at[half + m, i], j, other).start()

        closest, rest = range(half), range(half, 2 * half - 1)
        first = half - 1
        enter(0, first, False)
        plane_entered()
        signal(ready.at[rounds + 1], j, other)
        for mask in distant:
            spread(0, first, j, mask)
        for e in closest[1:]:
            enter(e, first, True)
        for d in outer_first:
            pass_on(d)
        block_out(2)
        forward(0)
        for e in rest:
            enter(e, first, True)
        for d in outer_first[1:]:
            for e in range(len(sources)):
                enter(e, d, True)
        forward(1)
        own_ops.wait()
        share(first)
        forward(2)
        for i in range(3, raw):
            block_out(i)
        complete(first)
        if half > 1:
            pl.semaphore_wait(ready.at[rounds], half - 1)

        band_of = lambda d: from_source(near(d) - side * half)
        others = pl.ds(pl.multiple_of(side * rows, rows), (n - 1) * rows)
        final = far(half - 1)

        def results(d, c, lane, size):
            target = pl.ds(pl.multiple_of(j * cols + lane, width), size)
            lane = pl.ds(lane, size)

            def result(to):
                return res.at[d, c, pl.ds(pl.multiple_of(to * outrows, outrows), outrows), lane]

            @pl.when(d > 0)
            def _():
                for to in range(g):
                    remote(result(to), out_ref.at[c, :, target], res_send.at[d], out_recv.at[0], to, near(d)).start()

            @pl.when(d == 0)
            def _():
                for mask in range(1, g):
                    to = flip(mask)
                    remote(result(to), out_ref.at[c, :, target], res_send.at[d], out_recv.at[0], to, near(d)).start()
                pltpu.make_async_copy(result(j), out_ref.at[c, :, target], out_recv.at[0]).start()

        def product(d, c, lane, i_first, count):
            band = band_of(d)

            @pl.when(d == first)
            def _():
                for e in range(half - 1):
                    for i in range(count):
                        wait_bytes(block_part(0, 0), blk_recv.at[half - 1 + e, i_first + i])
            size = lane.size
            ahead = wide.at[:, pl.ds(0, size)]
            ahead[...] = jnp.dot(ops[band, others], blocks[c, others, lane], preferred_element_type=jnp.float32)

            @pl.when(d == first)
            def _():
                for i in range(count):
                    wait_bytes(block_part(0, 0), blk_recv.at[2 * half - 2, i_first + i])
            total = ahead[...] + jnp.dot(
                ops[band, from_source(final)], blocks[c, from_source(final), lane], preferred_element_type=jnp.float32)
            res[d, c, :, lane] = total.astype(res.dtype)

        def near_half():
            for m in range(half - 1):
                wait_bytes(last_plane(0), blk_recv.at[m, raw])
            near_sum[...] = jnp.dot(ops[:, mine], blocks[planes - 1, mine, :], preferred_element_type=jnp.float32)
            near_out[...] = near_sum[band_of(0), :].astype(near_out.dtype)
            target = terms.at[1, :, pl.ds(pl.multiple_of(j * cols, cols), cols)]

            def term(to):
                return near_out.at[pl.ds(pl.multiple_of(to * outrows, outrows), outrows), :]
            for mask in reversed(range(1, g)):
                remote(term(flip(mask)), target, near_send, terms_recv.at[1], flip(mask), k).start()
            pltpu.make_async_copy(term(j), target, terms_recv.at[1]).start()

        def far_half(at):
            d, chip = pairs[at]
            band = far_rows(d, 2 * chip, 2)
            total = part[band, :]
            for m in range(half - 1):
                wait_bytes(part_in.at[m, band, :], part_recv.at[m, at])
                total = total + part_in[m, band, :].astype(jnp.float32)
            far_out[band, :] = total.astype(far_out.dtype)
            if at < joined:
                remote(far_out.at[band, :], far_in.at[band, :], far_send, far_recv.at[at], j, other).start()
                return
            for to in (2 * chip, 2 * chip + 1):
                remote(far_out.at[far_rows(d, to), :], terms.at[0, :, pl.ds(pl.multiple_of(j * cols, cols), cols)],
                       far_send, terms_recv.at[0], to, other).start()

        def late_result(at):
            d, chip = pairs[at]
            band = near_rows(d, 2 * chip, 2)
            wait_bytes(far_in.at[band, :], far_recv.at[at])
            late[band, :] = (near_sum[band, :] + far_in[band, :].astype(jnp.float32)).astype(late.dtype)
            target = out_ref.at[planes - 1, :, pl.ds(pl.multiple_of(j * cols, cols), cols)]
            for to in (2 * chip, 2 * chip + 1):
                remote(late.at[near_rows(d, to), :], target, late_send, out_recv.at[1], to, near(d)).start()

        early = (planes - 2) * parts

        def one(t, carry):
            i = jnp.where(t < early, t, early + lax.div(t - early, half))
            d = jnp.where(t < early, first, first - lax.rem(t - early, half))
            c, h = lax.div(i, parts), lax.rem(i, parts)
            at = pl.multiple_of(h * width, width)

            @pl.when(t == 1)
            def _():
                for e in range(3, raw):
                    forward(e)
                for e in outer_first[1:]:
                    share(e)

            @pl.when(t == early)
            def _():
                for e in outer_first[1:]:
                    complete(e)
                    for whole in range(planes - 2):
                        product(jnp.int32(e), whole, pl.ds(0, cols), 0, 0)
                        results(jnp.int32(e), whole, 0, cols)

            @pl.when(t == early + 1)
            def _():
                near_half()
                far_half(0)
                far_half(1)

            @pl.when(t == early + 2)
            def _():
                far_half(2)

            @pl.when(t == last_turn)
            def _():
                far_half(3)
                late_result(0)
                pl.semaphore_wait(ready.at[rounds + 1], 1)
                far_half(4)
                late_result(1)

            product(d, c, pl.ds(at, width), i, 1)
            results(d, c, at, width)
            return carry

        last_turn = early + half * parts - 1
        lax.fori_loop(0, last_turn + 1, one, 0)
        for at in range(5, len(pairs)):
            far_half(at)
            if at - 3 < joined:
                late_result(at - 3)
        for at in range(len(pairs) - 3, joined):
            late_result(at)
        wait_bytes(op_bytes(half * half), op_send)
        wait_bytes(blocks.at[pl.ds(0, planes - 1), from_source(0), :], own_send)
        for m in range(half - 1):
            wait_bytes(blocks.at[pl.ds(0, planes - 1), from_source(0), :], fwd_send.at[m])
        for d in range(half):
            sent = rows - outrows if d == 0 else rows
            wait_bytes(res.at[d, pl.ds(0, planes - 1), pl.ds(0, sent), :], res_send.at[d])
        for e in range(len(sources)):
            wait_bytes(op_bytes(half * (g - 1)), spread_send.at[e])
        wait_bytes(far_out, far_send)
        wait_bytes(late.at[pl.ds(0, (half - 1) * rows), :], late_send)
        wait_bytes(near_out.at[pl.ds(0, rows - outrows), :], near_send)
        for b in (1, 0):
            wait_bytes(terms.at[b], terms_recv.at[b])
        last[...] = (terms[0].astype(jnp.float32) + terms[1].astype(jnp.float32)).astype(last.dtype)
        pltpu.make_async_copy(last, out_ref.at[planes - 1], out_recv.at[1]).start()

    @pl.when(jnp.logical_not(is_centre))
    def _():
        m = away - 1

        def op_in(d):
            staged(1, d).wait()
            remote(first_ops.at[1, d], ops.at[near_rows(d, j), from_source(k)],
                   op_send, op_recv.at[m, d], j, centre).start()

        def op_past(d):
            staged(0, d).wait()
            remote(first_ops.at[0, d], passing.at[m, d], op_send, pass_recv.at[m, d], j, centre).start()

        op_in(half - 1)
        for d in outer_first:
            op_past(d)
        for d in outer_first[1:]:
            op_in(d)
        for rest_of in [own_start] + own_rest:
            rest_of.wait()
        for i in range(raw):
            at = block_part(k, i)
            remote(at, at, own_send, blk_recv.at[m, i], j, centre).start()
        remote(last_plane(k), last_plane(k), own_send, blk_recv.at[m, raw], j, centre).start()
        own_far.wait()
        own_ops.wait()
        own_part()
        part_out[...] = part[...].astype(part_out.dtype)
        for at, (d, chip) in enumerate(pairs):
            band = far_rows(d, 2 * chip, 2)
            remote(part_out.at[band, :], part_in.at[m, band, :], part_send, part_recv.at[m, at], j, centre).start()
        plane_entered()
        signal(ready.at[rounds], j, centre)
        wait_bytes(op_bytes(2 * half), op_send)
        wait_bytes(blocks.at[:, from_source(0), :], own_send)
        wait_bytes(part_out, part_send)

    wait_bytes(out_ref.at[pl.ds(0, planes - 1)], out_recv.at[0])
    wait_bytes(out_ref.at[planes - 1], out_recv.at[1])


def at_centres(n, g, products, operator):
    rows, planes, cols = products.shape
    parts = 2 if cols % (2 * LANES) == 0 else 1
    half = n // 2
    outer, roles, raw = max(half - 1, 1), 2 * half - 1, (planes - 1) * parts
    out = pl.pallas_call(
        functools.partial(kernel, n, g, parts),
        out_shape=jax.ShapeDtypeStruct((planes, rows // g, cols * g), jnp.bfloat16),
        in_specs=[pl.BlockSpec(memory_space=pl.ANY)] * 2,
        out_specs=pl.BlockSpec(memory_space=pl.ANY),
        scratch_shapes=[
            pltpu.VMEM((planes, n * rows, cols), jnp.bfloat16),
            pltpu.VMEM((half * rows, n * rows), jnp.bfloat16),
            pltpu.VMEM((half * rows, rows), jnp.bfloat16),
            pltpu.VMEM((2, half, rows // g, rows), jnp.bfloat16),
            pltpu.VMEM((outer, half, rows // g, rows), jnp.bfloat16),
            pltpu.VMEM((half, planes - 1, rows, cols), jnp.bfloat16),
            pltpu.VMEM((rows, cols), jnp.float32),
            pltpu.VMEM((half * rows, cols), jnp.float32),
            pltpu.VMEM((half * rows, cols), jnp.bfloat16),
            pltpu.VMEM((outer, half * rows, cols), jnp.bfloat16),
            pltpu.VMEM((half * rows, cols), jnp.bfloat16),
            pltpu.VMEM((half * rows, cols), jnp.bfloat16),
            pltpu.VMEM((half * rows, cols), jnp.float32),
            pltpu.VMEM((rows, cols), jnp.bfloat16),
            pltpu.VMEM((half * rows, cols), jnp.bfloat16),
            pltpu.VMEM((2, rows // g, g * cols), jnp.bfloat16),
            pltpu.VMEM((rows // g, g * cols), jnp.bfloat16),
            pltpu.SemaphoreType.DMA,
            pltpu.SemaphoreType.DMA((outer,)),
            pltpu.SemaphoreType.DMA,
            pltpu.SemaphoreType.DMA((roles,)),
            pltpu.SemaphoreType.DMA((half,)),
            pltpu.SemaphoreType.DMA,
            pltpu.SemaphoreType.DMA,
            pltpu.SemaphoreType.DMA,
            pltpu.SemaphoreType.DMA,
            pltpu.SemaphoreType.DMA((roles, raw + 1)),
            pltpu.SemaphoreType.DMA((roles, half)),
            pltpu.SemaphoreType.DMA((outer, half)),
            pltpu.SemaphoreType.DMA((roles, half)),
            pltpu.SemaphoreType.DMA((half,)),
            pltpu.SemaphoreType.DMA((2,)),
            pltpu.SemaphoreType.DMA((outer, half * g // 2)),
            pltpu.SemaphoreType.DMA((outer * g // 2,)),
            pltpu.SemaphoreType.DMA((2,)),
            pltpu.SemaphoreType.DMA((2 * half + 5,)),
            pltpu.SemaphoreType.REGULAR((g.bit_length() + 1,)),
        ],
        compiler_params=pltpu.CompilerParams(
            collective_id=0, has_side_effects=True, vmem_limit_bytes=GRANT),
    )(products.transpose(1, 0, 2), operator)
    return out.transpose(1, 0, 2)


def by_collectives(products, operator):
    y_local, three, m_local = products.shape
    flat = products.reshape(y_local, three * m_local)
    summed = lax.psum_scatter(
        jnp.dot(operator, flat, preferred_element_type=jnp.float32), "gy", scatter_dimension=0, tiled=True)
    result = summed.astype(jnp.bfloat16).reshape(y_local, three, m_local)
    return lax.all_to_all(result, "gx", split_axis=0, concat_axis=2, tiled=True)


def solution(mesh):
    n, g = mesh.shape["gy"], mesh.shape["gx"]

    def body(products, operator):
        rows, planes, cols = products.shape
        aligned = (n // 2 == 2 and n % 2 == 0 and planes > 2 and g & (g - 1) == 0 and g > 1 and rows % (g * SUBLANES) == 0
                   and rows % LANES == 0 and cols % (2 * LANES) == 0)
        held = 2 * (products.size * (n + n // 2 + 2) + operator.size * (2 + n // 2)) + 20 * n * rows * cols
        if aligned and held < VMEM_BYTES // 2:
            return at_centres(n, g, products, operator)
        return by_collectives(products, operator)

    return jax.shard_map(
        body,
        mesh=mesh,
        in_specs=(P("gy", None, "gx"), P(None, "gy")),
        out_specs=P(("gy", "gx"), None, None),
        check_vma=False,
    )
```

```python
import functools

import jax
import jax.numpy as jnp
from jax import lax
from jax.experimental import pallas as pl
from jax.experimental.pallas import tpu as pltpu
from jax.sharding import PartitionSpec as P

MESH = pl.DeviceIdType.MESH
LANES = 128
SUBLANES = 16
VMEM_BYTES = 60 * 1024 * 1024
GRANT = 54500 * 1024


def kernel(n, g, parts, p_ref, op_ref, out_ref, blocks, ops, far_ops, first_ops, passing, res, wide, part, part_out, part_in,
           far_out, far_in, near_sum, near_out, late, terms, own_send, fwd_send, op_send, spread_send, res_send, part_send, far_send,
           late_send, near_send, blk_recv, op_recv, pass_recv, plane_recv, sibling_recv, out_recv, part_recv, far_recv, terms_recv, own_copy,
           ready):
    j, k = lax.axis_index("gx"), lax.axis_index("gy")
    half = n // 2
    side = lax.div(k, half)
    step = 1 - 2 * side
    centre = jnp.where(side == 0, half - 1, half)
    other = n - 1 - centre
    is_centre = k == centre
    away = step * (centre - k)
    planes, rows, cols = p_ref.shape
    width = cols // parts
    raw = (planes - 1) * parts
    outrows = rows // g
    mine = pl.ds(pl.multiple_of(side * (half * rows), half * rows), half * rows)
    theirs = pl.ds(pl.multiple_of((1 - side) * (half * rows), half * rows), half * rows)

    def flip(mask):
        to = j
        for bit in (1 << b for b in range(mask.bit_length())):
            if mask & bit:
                to = to + bit * (1 - 2 * lax.rem(lax.div(j, bit), 2))
        return to

    def near(d):
        return centre - step * d

    def far(d):
        return other + step * d

    def from_source(s):
        return pl.ds(pl.multiple_of(s * rows, rows), rows)

    def near_rows(d, to, count=1):
        at = (near(d) - side * half) * rows + to * outrows
        return pl.ds(pl.multiple_of(at, outrows), count * outrows)

    def far_rows(d, to, count=1):
        at = (far(d) - (1 - side) * half) * rows + to * outrows
        return pl.ds(pl.multiple_of(at, outrows), count * outrows)

    def wait_bytes(ref, sem):
        pltpu.make_async_copy(ref, ref, sem).wait()

    def op_bytes(pieces):
        return ops.at[pl.ds(0, pieces * outrows), pl.ds(0, rows)]

    def staged(slot, d):
        at = far_rows(d, j) if slot == 0 else near_rows(d, j)
        start = (theirs if slot == 0 else mine).start
        return pltpu.make_async_copy(
            op_ref.at[pl.ds(pl.multiple_of(start + at.start, outrows), outrows), :], first_ops.at[slot, d],
            own_copy.at[2 * d + slot])

    own_start = pltpu.make_async_copy(
        p_ref.at[0, :, pl.ds(0, width)], blocks.at[0, from_source(k), pl.ds(0, width)], own_copy.at[2 * half])
    own_rest = [pltpu.make_async_copy(
        p_ref.at[0, :, pl.ds(width, cols - width)], blocks.at[0, from_source(k), pl.ds(width, cols - width)],
        own_copy.at[2 * half + 1])] if parts > 1 else []
    own_rest.append(pltpu.make_async_copy(
        p_ref.at[pl.ds(1, planes - 1)], blocks.at[pl.ds(1, planes - 1), from_source(k), :], own_copy.at[2 * half + 2]))
    own_far = pltpu.make_async_copy(op_ref.at[theirs, :], far_ops, own_copy.at[2 * half + 3])
    own_ops = pltpu.make_async_copy(op_ref.at[mine, :], ops.at[:, from_source(k)], own_copy.at[2 * half + 4])
    for d in reversed(range(half)):
        for slot in (1, 0):
            staged(slot, d).start()
    own_start.start()
    for rest_of in own_rest + [own_far, own_ops]:
        rest_of.start()

    rounds = g.bit_length() - 1
    barrier = pltpu.get_barrier_semaphore()

    def signal(sem, gx, gy):
        pl.semaphore_signal(sem, inc=1, device_id=(gx, gy), device_id_type=MESH)

    for b in range(rounds):
        signal(barrier, flip(1 << b), k)

    @pl.when(is_centre)
    def _():
        signal(barrier, j, other)
        for d in range(1, half):
            signal(barrier, j, near(d))

    pl.semaphore_wait(barrier, rounds + 1)

    def plane_entered():
        for b in range(rounds):
            signal(ready.at[b], flip(1 << b), k)
            pl.semaphore_wait(ready.at[b], 1)

    def remote(src, dst, send, recv, gx, gy):
        return pltpu.make_async_remote_copy(
            src_ref=src, dst_ref=dst, send_sem=send, recv_sem=recv,
            device_id=(gx, gy), device_id_type=MESH)

    def lanes(i):
        return pl.ds(pl.multiple_of(lax.rem(i, parts) * width, width), width)

    def block_part(s, i):
        return blocks.at[lax.div(i, parts), from_source(s), lanes(i)]

    def last_plane(s):
        return blocks.at[planes - 1, from_source(s), :]

    sources = [near(d) for d in range(1, half)] + [far(d) for d in range(half)]

    chips = g // 2
    column = lax.div(j, 2)

    def bits(x):
        return bin(x).count("1")

    def pick(at):
        chip = jnp.int32(0)
        for c in range(chips):
            order = sorted(range(1, chips), key=lambda x: (bits(x) - bits(x ^ c), x == c, x))
            chip = jnp.where(column == c, order[at], chip)
        return chip

    held_back = half * chips // 2
    turns = [pick(at) for at in range(chips - 1)]
    outer_first = list(reversed(range(half)))
    pairs = [(d, 0) for d in outer_first[:-1]] + [(d, chip) for d in outer_first[:-1] for chip in turns]
    joined = len(pairs)
    pairs += [(0, chip) for chip in [0] + turns]

    def own_part():
        part[...] = jnp.dot(far_ops[...], last_plane(k)[...], preferred_element_type=jnp.float32)

    @pl.when(is_centre)
    def _():
        def block_out(i):
            at = block_part(k, i)
            remote(at, at, own_send, blk_recv.at[half - 1, i], j, other).start()

        for d in outer_first:
            staged(0, d).wait()
            remote(first_ops.at[0, d], ops.at[far_rows(d, j), from_source(k)],
                   op_send, op_recv.at[half - 1, d], j, other).start()
        own_start.wait()
        block_out(0)
        for rest_of in own_rest:
            rest_of.wait()
        block_out(1)
        for d in outer_first:
            staged(1, d).wait()
        own_far.wait()
        own_part()

        def spread(e, d, at, mask):
            part_of = ops.at[near_rows(d, at), from_source(sources[e])]
            sem = sibling_recv.at[d] if mask == 1 else plane_recv.at[e, d]
            remote(part_of, part_of, spread_send.at[e], sem, flip(mask), k).start()

        adjacent = [1 << b for b in reversed(range(rounds))]
        distant = [2 * m for m in range(1, g // 2) if 2 * m not in adjacent]

        def enter(e, d, everywhere):
            wait_bytes(op_bytes(1), op_recv.at[e, d])
            for mask in (distant if everywhere else []) + adjacent:
                spread(e, d, j, mask)

        def share(d):
            for e in range(len(sources)):
                wait_bytes(op_bytes(g // 2 - 1), plane_recv.at[e, d])
                for mask in range(1, g // 2):
                    spread(e, d, flip(2 * mask), 1)

        def complete(d):
            wait_bytes(op_bytes(len(sources) * (g // 2)), sibling_recv.at[d])

        def pass_on(d):
            for m in range(half - 1):
                wait_bytes(op_bytes(1), pass_recv.at[m, d])
                remote(passing.at[m, d], ops.at[far_rows(d, j), from_source(near(m + 1))],
                       op_send, op_recv.at[half + m, d], j, other).start()

        def forward(i):
            for m in range(half - 1):
                at = block_part(near(m + 1), i)
                wait_bytes(at, blk_recv.at[m, i])
                remote(at, at, fwd_send.at[m], blk_recv.at[half + m, i], j, other).start()

        closest, rest = range(half), range(half, 2 * half - 1)
        first = half - 1
        enter(0, first, False)
        plane_entered()
        signal(ready.at[rounds + 1], j, other)
        for mask in distant:
            spread(0, first, j, mask)
        for e in closest[1:]:
            enter(e, first, True)
        for d in outer_first:
            pass_on(d)
        block_out(2)
        forward(0)
        for e in rest:
            enter(e, first, True)
        for d in outer_first[1:]:
            for e in range(len(sources)):
                enter(e, d, True)
        forward(1)
        forward(2)
        for i in range(3, raw):
            block_out(i)
        own_ops.wait()
        share(first)
        complete(first)
        if half > 1:
            pl.semaphore_wait(ready.at[rounds], half - 1)

        band_of = lambda d: from_source(near(d) - side * half)
        others = pl.ds(pl.multiple_of(side * rows, rows), (n - 1) * rows)
        final = far(half - 1)

        def results(d, c, lane, size):
            target = pl.ds(pl.multiple_of(j * cols + lane, width), size)
            lane = pl.ds(lane, size)

            def result(to):
                return res.at[d, c, pl.ds(pl.multiple_of(to * outrows, outrows), outrows), lane]

            @pl.when(d > 0)
            def _():
                for to in range(g):
                    remote(result(to), out_ref.at[c, :, target], res_send.at[d], out_recv.at[0], to, near(d)).start()

            @pl.when(d == 0)
            def _():
                for mask in range(1, g):
                    to = flip(mask)
                    remote(result(to), out_ref.at[c, :, target], res_send.at[d], out_recv.at[0], to, near(d)).start()
                pltpu.make_async_copy(result(j), out_ref.at[c, :, target], out_recv.at[0]).start()

        def product(d, c, lane, i_first, count):
            band = band_of(d)

            @pl.when(d == first)
            def _():
                for e in range(half - 1):
                    for i in range(count):
                        wait_bytes(block_part(0, 0), blk_recv.at[half - 1 + e, i_first + i])
            size = lane.size
            ahead = wide.at[:, pl.ds(0, size)]
            ahead[...] = jnp.dot(ops[band, others], blocks[c, others, lane], preferred_element_type=jnp.float32)

            @pl.when(d == first)
            def _():
                for i in range(count):
                    wait_bytes(block_part(0, 0), blk_recv.at[2 * half - 2, i_first + i])
            total = ahead[...] + jnp.dot(
                ops[band, from_source(final)], blocks[c, from_source(final), lane], preferred_element_type=jnp.float32)
            res[d, c, :, lane] = total.astype(res.dtype)

        def near_half():
            for m in range(half - 1):
                wait_bytes(last_plane(0), blk_recv.at[m, raw])
            near_sum[...] = jnp.dot(ops[:, mine], blocks[planes - 1, mine, :], preferred_element_type=jnp.float32)
            near_out[...] = near_sum[band_of(0), :].astype(near_out.dtype)
            target = terms.at[1, :, pl.ds(pl.multiple_of(j * cols, cols), cols)]

            def term(to):
                return near_out.at[pl.ds(pl.multiple_of(to * outrows, outrows), outrows), :]
            for mask in reversed(range(1, g)):
                remote(term(flip(mask)), target, near_send, terms_recv.at[1], flip(mask), k).start()
            pltpu.make_async_copy(term(j), target, terms_recv.at[1]).start()

        def far_half(at):
            d, chip = pairs[at]
            band = far_rows(d, 2 * chip, 2)
            total = part[band, :]
            for m in range(half - 1):
                wait_bytes(part_in.at[m, band, :], part_recv.at[m, at])
                total = total + part_in[m, band, :].astype(jnp.float32)
            far_out[band, :] = total.astype(far_out.dtype)
            if at < joined:
                remote(far_out.at[band, :], far_in.at[band, :], far_send, far_recv.at[at], j, other).start()
                return
            for to in (2 * chip, 2 * chip + 1):
                remote(far_out.at[far_rows(d, to), :], terms.at[0, :, pl.ds(pl.multiple_of(j * cols, cols), cols)],
                       far_send, terms_recv.at[0], to, other).start()

        def late_result(at):
            d, chip = pairs[at]
            band = near_rows(d, 2 * chip, 2)
            wait_bytes(far_in.at[band, :], far_recv.at[at])
            late[band, :] = (near_sum[band, :] + far_in[band, :].astype(jnp.float32)).astype(late.dtype)
            target = out_ref.at[planes - 1, :, pl.ds(pl.multiple_of(j * cols, cols), cols)]
            for to in (2 * chip, 2 * chip + 1):
                remote(late.at[near_rows(d, to), :], target, late_send, out_recv.at[1], to, near(d)).start()

        early = (planes - 2) * parts

        def one(t, carry):
            i = jnp.where(t < early, t, early + lax.div(t - early, half))
            d = jnp.where(t < early, first, first - lax.rem(t - early, half))
            c, h = lax.div(i, parts), lax.rem(i, parts)
            at = pl.multiple_of(h * width, width)

            @pl.when(t == 1)
            def _():
                for e in range(3, raw):
                    forward(e)
                for e in outer_first[1:]:
                    share(e)

            @pl.when(t == early)
            def _():
                for e in outer_first[1:]:
                    complete(e)
                    for whole in range(planes - 2):
                        product(jnp.int32(e), whole, pl.ds(0, cols), 0, 0)
                        results(jnp.int32(e), whole, 0, cols)

            @pl.when(t == early + 1)
            def _():
                near_half()
                far_half(0)
                far_half(1)

            @pl.when(t == early + 2)
            def _():
                far_half(2)

            @pl.when(t == last_turn)
            def _():
                far_half(3)
                late_result(0)
                pl.semaphore_wait(ready.at[rounds + 1], 1)
                far_half(4)
                late_result(1)

            product(d, c, pl.ds(at, width), i, 1)
            results(d, c, at, width)
            return carry

        last_turn = early + half * parts - 1
        lax.fori_loop(0, last_turn + 1, one, 0)
        for at in range(5, len(pairs)):
            far_half(at)
            if at - 3 < joined:
                late_result(at - 3)
        for at in range(len(pairs) - 3, joined):
            late_result(at)
        wait_bytes(op_bytes(half * half), op_send)
        wait_bytes(blocks.at[pl.ds(0, planes - 1), from_source(0), :], own_send)
        for m in range(half - 1):
            wait_bytes(blocks.at[pl.ds(0, planes - 1), from_source(0), :], fwd_send.at[m])
        for d in range(half):
            sent = rows - outrows if d == 0 else rows
            wait_bytes(res.at[d, pl.ds(0, planes - 1), pl.ds(0, sent), :], res_send.at[d])
        for e in range(len(sources)):
            wait_bytes(op_bytes(half * (g - 1)), spread_send.at[e])
        wait_bytes(far_out, far_send)
        wait_bytes(late.at[pl.ds(0, (half - 1) * rows), :], late_send)
        wait_bytes(near_out.at[pl.ds(0, rows - outrows), :], near_send)
        for b in (1, 0):
            wait_bytes(terms.at[b], terms_recv.at[b])
        out_ref[planes - 1] = (terms[0].astype(jnp.float32) + terms[1].astype(jnp.float32)).astype(out_ref.dtype)

    @pl.when(jnp.logical_not(is_centre))
    def _():
        m = away - 1

        def op_in(d):
            staged(1, d).wait()
            remote(first_ops.at[1, d], ops.at[near_rows(d, j), from_source(k)],
                   op_send, op_recv.at[m, d], j, centre).start()

        def op_past(d):
            staged(0, d).wait()
            remote(first_ops.at[0, d], passing.at[m, d], op_send, pass_recv.at[m, d], j, centre).start()

        op_in(half - 1)
        for d in outer_first:
            op_past(d)
        for d in outer_first[1:]:
            op_in(d)
        for rest_of in [own_start] + own_rest:
            rest_of.wait()
        for i in range(raw):
            at = block_part(k, i)
            remote(at, at, own_send, blk_recv.at[m, i], j, centre).start()
        remote(last_plane(k), last_plane(k), own_send, blk_recv.at[m, raw], j, centre).start()
        own_far.wait()
        own_ops.wait()
        own_part()
        part_out[...] = part[...].astype(part_out.dtype)
        for at, (d, chip) in enumerate(pairs):
            band = far_rows(d, 2 * chip, 2)
            remote(part_out.at[band, :], part_in.at[m, band, :], part_send, part_recv.at[m, at], j, centre).start()
        plane_entered()
        signal(ready.at[rounds], j, centre)
        wait_bytes(op_bytes(2 * half), op_send)
        wait_bytes(blocks.at[:, from_source(0), :], own_send)
        wait_bytes(part_out, part_send)

    wait_bytes(out_ref.at[pl.ds(0, planes - 1)], out_recv.at[0])

    @pl.when(jnp.logical_not(is_centre))
    def _():
        wait_bytes(out_ref.at[planes - 1], out_recv.at[1])


def at_centres(n, g, products, operator):
    rows, planes, cols = products.shape
    parts = 2 if cols % (2 * LANES) == 0 else 1
    half = n // 2
    outer, roles, raw = max(half - 1, 1), 2 * half - 1, (planes - 1) * parts
    out = pl.pallas_call(
        functools.partial(kernel, n, g, parts),
        out_shape=jax.ShapeDtypeStruct((planes, rows // g, cols * g), jnp.bfloat16),
        in_specs=[pl.BlockSpec(memory_space=pl.ANY)] * 2,
        out_specs=pl.BlockSpec(memory_space=pltpu.VMEM),
        scratch_shapes=[
            pltpu.VMEM((planes, n * rows, cols), jnp.bfloat16),
            pltpu.VMEM((half * rows, n * rows), jnp.bfloat16),
            pltpu.VMEM((half * rows, rows), jnp.bfloat16),
            pltpu.VMEM((2, half, rows // g, rows), jnp.bfloat16),
            pltpu.VMEM((outer, half, rows // g, rows), jnp.bfloat16),
            pltpu.VMEM((half, planes - 1, rows, cols), jnp.bfloat16),
            pltpu.VMEM((rows, cols), jnp.float32),
            pltpu.VMEM((half * rows, cols), jnp.float32),
            pltpu.VMEM((half * rows, cols), jnp.bfloat16),
            pltpu.VMEM((outer, half * rows, cols), jnp.bfloat16),
            pltpu.VMEM((half * rows, cols), jnp.bfloat16),
            pltpu.VMEM((half * rows, cols), jnp.bfloat16),
            pltpu.VMEM((half * rows, cols), jnp.float32),
            pltpu.VMEM((rows, cols), jnp.bfloat16),
            pltpu.VMEM((half * rows, cols), jnp.bfloat16),
            pltpu.VMEM((2, rows // g, g * cols), jnp.bfloat16),
            pltpu.SemaphoreType.DMA,
            pltpu.SemaphoreType.DMA((outer,)),
            pltpu.SemaphoreType.DMA,
            pltpu.SemaphoreType.DMA((roles,)),
            pltpu.SemaphoreType.DMA((half,)),
            pltpu.SemaphoreType.DMA,
            pltpu.SemaphoreType.DMA,
            pltpu.SemaphoreType.DMA,
            pltpu.SemaphoreType.DMA,
            pltpu.SemaphoreType.DMA((roles, raw + 1)),
            pltpu.SemaphoreType.DMA((roles, half)),
            pltpu.SemaphoreType.DMA((outer, half)),
            pltpu.SemaphoreType.DMA((roles, half)),
            pltpu.SemaphoreType.DMA((half,)),
            pltpu.SemaphoreType.DMA((2,)),
            pltpu.SemaphoreType.DMA((outer, half * g // 2)),
            pltpu.SemaphoreType.DMA((outer * g // 2,)),
            pltpu.SemaphoreType.DMA((2,)),
            pltpu.SemaphoreType.DMA((2 * half + 5,)),
            pltpu.SemaphoreType.REGULAR((g.bit_length() + 1,)),
        ],
        compiler_params=pltpu.CompilerParams(
            collective_id=0, has_side_effects=True, vmem_limit_bytes=GRANT),
    )(products.transpose(1, 0, 2), operator)
    return out.transpose(1, 0, 2)


def by_collectives(products, operator):
    y_local, three, m_local = products.shape
    flat = products.reshape(y_local, three * m_local)
    summed = lax.psum_scatter(
        jnp.dot(operator, flat, preferred_element_type=jnp.float32), "gy", scatter_dimension=0, tiled=True)
    result = summed.astype(jnp.bfloat16).reshape(y_local, three, m_local)
    return lax.all_to_all(result, "gx", split_axis=0, concat_axis=2, tiled=True)


def solution(mesh):
    n, g = mesh.shape["gy"], mesh.shape["gx"]

    def body(products, operator):
        rows, planes, cols = products.shape
        aligned = (n // 2 == 2 and n % 2 == 0 and planes > 2 and g & (g - 1) == 0 and g > 1 and rows % (g * SUBLANES) == 0
                   and rows % LANES == 0 and cols % (2 * LANES) == 0)
        held = 2 * (products.size * (n + n // 2 + 2) + operator.size * (2 + n // 2)) + 20 * n * rows * cols
        if aligned and held < VMEM_BYTES // 2:
            return at_centres(n, g, products, operator)
        return by_collectives(products, operator)

    return jax.shard_map(
        body,
        mesh=mesh,
        in_specs=(P("gy", None, "gx"), P(None, "gy")),
        out_specs=P(("gy", "gx"), None, None),
        check_vma=False,
    )
```

```python
import functools

import jax
import jax.numpy as jnp
from jax import lax
from jax.experimental import pallas as pl
from jax.experimental.pallas import tpu as pltpu
from jax.sharding import PartitionSpec as P

MESH = pl.DeviceIdType.MESH
LANES = 128
SUBLANES = 16
VMEM_BYTES = 60 * 1024 * 1024
GRANT = 54500 * 1024


def kernel(n, g, parts, p_ref, op_ref, out_ref, blocks, ops, far_ops, first_ops, passing, res, wide, part, part_out,
           part_in, far_out, far_in, near_sum, near_out, late, terms, block_send, op_send, spread_send, res_send,
           far_send, late_send, blk_recv, op_recv, pass_recv, plane_recv, sibling_recv, out_recv, part_recv, far_recv,
           terms_recv, own_copy, ready):
    j, k = lax.axis_index("gx"), lax.axis_index("gy")
    half = n // 2
    side = lax.div(k, half)
    step = 1 - 2 * side
    centre = jnp.where(side == 0, half - 1, half)
    other = n - 1 - centre
    is_centre = k == centre
    away = step * (centre - k)
    planes, rows, cols = p_ref.shape
    width = cols // parts
    raw = (planes - 1) * parts
    outrows = rows // g
    mine = pl.ds(pl.multiple_of(side * (half * rows), half * rows), half * rows)
    theirs = pl.ds(pl.multiple_of((1 - side) * (half * rows), half * rows), half * rows)

    def flip(mask):
        to = j
        for bit in (1 << b for b in range(mask.bit_length())):
            if mask & bit:
                to = to + bit * (1 - 2 * lax.rem(lax.div(j, bit), 2))
        return to

    def near(d):
        return centre - step * d

    def far(d):
        return other + step * d

    def from_source(s):
        return pl.ds(pl.multiple_of(s * rows, rows), rows)

    def near_rows(d, to, count=1):
        at = (near(d) - side * half) * rows + to * outrows
        return pl.ds(pl.multiple_of(at, outrows), count * outrows)

    def far_rows(d, to, count=1):
        at = (far(d) - (1 - side) * half) * rows + to * outrows
        return pl.ds(pl.multiple_of(at, outrows), count * outrows)

    def wait_bytes(ref, sem):
        pltpu.make_async_copy(ref, ref, sem).wait()

    def op_bytes(pieces):
        return ops.at[pl.ds(0, pieces * outrows), pl.ds(0, rows)]

    def staged(slot, d):
        at = far_rows(d, j) if slot == 0 else near_rows(d, j)
        start = (theirs if slot == 0 else mine).start
        return pltpu.make_async_copy(
            op_ref.at[pl.ds(pl.multiple_of(start + at.start, outrows), outrows), :], first_ops.at[slot, d],
            own_copy.at[slot])

    own_start = pltpu.make_async_copy(p_ref.at[0], blocks.at[0, from_source(k), :], own_copy.at[2])
    own_rest = pltpu.make_async_copy(
        p_ref.at[pl.ds(1, planes - 1)], blocks.at[pl.ds(1, planes - 1), from_source(k), :], own_copy.at[3])
    own_far = pltpu.make_async_copy(op_ref.at[theirs, :], far_ops, own_copy.at[4])
    own_ops = pltpu.make_async_copy(op_ref.at[mine, :], ops.at[:, from_source(k)], own_copy.at[4])
    for d in reversed(range(half)):
        for slot in (1, 0):
            staged(slot, d).start()
    own_start.start()
    for copy in (own_rest, own_far, own_ops):
        copy.start()

    def staged_in(slot):
        wait_bytes(first_ops.at[slot], own_copy.at[slot])

    def operator_in():
        wait_bytes(ops.at[:, pl.ds(0, 2 * rows)], own_copy.at[4])

    rounds = g.bit_length() - 1
    barrier = pltpu.get_barrier_semaphore()

    def signal(sem, gx, gy):
        pl.semaphore_signal(sem, inc=1, device_id=(gx, gy), device_id_type=MESH)

    for b in range(rounds):
        signal(barrier, flip(1 << b), k)

    @pl.when(is_centre)
    def _():
        signal(barrier, j, other)
        for d in range(1, half):
            signal(barrier, j, near(d))

    pl.semaphore_wait(barrier, rounds + 1)

    def plane_entered():
        for b in range(rounds):
            signal(ready.at[b], flip(1 << b), k)
            pl.semaphore_wait(ready.at[b], 1)

    def remote(src, dst, send, recv, gx, gy):
        return pltpu.make_async_remote_copy(
            src_ref=src, dst_ref=dst, send_sem=send, recv_sem=recv,
            device_id=(gx, gy), device_id_type=MESH)

    def lanes(i):
        return pl.ds(pl.multiple_of(lax.rem(i, parts) * width, width), width)

    def block_part(s, i):
        return blocks.at[lax.div(i, parts), from_source(s), lanes(i)]

    def near_slot(m, i):
        return m * (raw + 1) + i

    def far_slot(m, i):
        return (half - 1) * (raw + 1) + m * raw + i

    def last_plane(s):
        return blocks.at[planes - 1, from_source(s), :]

    sources = [near(d) for d in range(1, half)] + [far(d) for d in range(half)]

    chips = g // 2
    column = lax.div(j, 2)

    def bits(x):
        return bin(x).count("1")

    def pick(at):
        chip = jnp.int32(0)
        for c in range(chips):
            order = sorted(range(1, chips), key=lambda x: (bits(x) - bits(x ^ c), x == c, x))
            chip = jnp.where(column == c, order[at], chip)
        return chip

    turns = [pick(at) for at in range(chips - 1)]
    outer_first = list(reversed(range(half)))
    pairs = [(d, 0) for d in outer_first[:-1]] + [(d, chip) for d in outer_first[:-1] for chip in turns]
    joined = len(pairs)
    pairs += [(0, chip) for chip in [0] + turns]

    def own_part():
        part[...] = jnp.dot(far_ops[...], last_plane(k)[...], preferred_element_type=jnp.float32)

    @pl.when(is_centre)
    def _():
        def block_out(i):
            at = block_part(k, i)
            remote(at, at, block_send, blk_recv.at[far_slot(0, i)], j, other).start()

        staged_in(0)
        for d in outer_first:
            remote(first_ops.at[0, d], ops.at[far_rows(d, j), from_source(k)],
                   op_send, op_recv.at[half - 1, d], j, other).start()
        own_start.wait()
        block_out(0)
        block_out(1)
        staged_in(1)
        own_rest.wait()
        operator_in()
        own_part()

        def spread(e, d, at, mask):
            part_of = ops.at[near_rows(d, at), from_source(sources[e])]
            sem = sibling_recv.at[d] if mask == 1 else plane_recv.at[e, d]
            remote(part_of, part_of, spread_send.at[e], sem, flip(mask), k).start()

        adjacent = [1 << b for b in reversed(range(rounds))]
        distant = [2 * m for m in range(1, g // 2) if 2 * m not in adjacent]

        def enter(e, d, everywhere):
            wait_bytes(op_bytes(1), op_recv.at[e, d])
            for mask in (distant if everywhere else []) + adjacent:
                spread(e, d, j, mask)

        def share(d):
            for e in range(len(sources)):
                wait_bytes(op_bytes(g // 2 - 1), plane_recv.at[e, d])
                for mask in range(1, g // 2):
                    spread(e, d, flip(2 * mask), 1)

        def complete(d):
            wait_bytes(op_bytes(len(sources) * (g // 2)), sibling_recv.at[d])

        def pass_on(d):
            for m in range(half - 1):
                wait_bytes(op_bytes(1), pass_recv.at[m, d])
                remote(passing.at[m, d], ops.at[far_rows(d, j), from_source(near(m + 1))],
                       op_send, op_recv.at[half + m, d], j, other).start()

        def forward(i):
            for m in range(half - 1):
                at = block_part(near(m + 1), i)
                wait_bytes(at, blk_recv.at[near_slot(m, i)])
                remote(at, at, block_send, blk_recv.at[far_slot(m + 1, i)], j, other).start()

        closest, rest = range(half), range(half, 2 * half - 1)
        first = half - 1
        enter(0, first, False)
        plane_entered()
        signal(ready.at[rounds + 1], j, other)
        for mask in distant:
            spread(0, first, j, mask)
        for e in closest[1:]:
            enter(e, first, True)
        for d in outer_first:
            pass_on(d)
        block_out(2)
        forward(0)
        for e in rest:
            enter(e, first, True)
        for d in outer_first[1:]:
            for e in range(len(sources)):
                enter(e, d, True)
        forward(1)
        forward(2)
        for i in range(3, raw):
            block_out(i)
        share(first)
        complete(first)
        if half > 1:
            pl.semaphore_wait(ready.at[rounds], half - 1)

        band_of = lambda d: from_source(near(d) - side * half)
        others = pl.ds(pl.multiple_of(side * rows, rows), (n - 1) * rows)
        final = far(half - 1)

        def results(d, c, lane, size):
            target = pl.ds(pl.multiple_of(j * cols + lane, width), size)
            lane = pl.ds(lane, size)

            def result(to):
                return res.at[d, c, pl.ds(pl.multiple_of(to * outrows, outrows), outrows), lane]

            @pl.when(d > 0)
            def _():
                for to in range(g):
                    remote(result(to), out_ref.at[c, :, target], res_send, out_recv.at[0], to, near(d)).start()

            @pl.when(d == 0)
            def _():
                for mask in range(1, g):
                    to = flip(mask)
                    remote(result(to), out_ref.at[c, :, target], res_send, out_recv.at[0], to, near(d)).start()
                pltpu.make_async_copy(result(j), out_ref.at[c, :, target], out_recv.at[0]).start()

        def product(d, c, lane, i_first, count):
            band = band_of(d)

            @pl.when(d == first)
            def _():
                for e in range(half - 1):
                    for i in range(count):
                        wait_bytes(block_part(0, 0), blk_recv.at[far_slot(e, i_first + i)])
            size = lane.size
            ahead = wide.at[:, pl.ds(0, size)]
            ahead[...] = jnp.dot(ops[band, others], blocks[c, others, lane], preferred_element_type=jnp.float32)

            @pl.when(d == first)
            def _():
                for i in range(count):
                    wait_bytes(block_part(0, 0), blk_recv.at[far_slot(half - 1, i_first + i)])
            total = ahead[...] + jnp.dot(
                ops[band, from_source(final)], blocks[c, from_source(final), lane], preferred_element_type=jnp.float32)
            res[d, c, :, lane] = total.astype(res.dtype)

        def near_half():
            for m in range(half - 1):
                wait_bytes(last_plane(0), blk_recv.at[near_slot(m, raw)])
            near_sum[...] = jnp.dot(ops[:, mine], blocks[planes - 1, mine, :], preferred_element_type=jnp.float32)
            near_out[...] = near_sum[band_of(0), :].astype(near_out.dtype)
            target = terms.at[1, :, pl.ds(pl.multiple_of(j * cols, cols), cols)]

            def term(to):
                return near_out.at[pl.ds(pl.multiple_of(to * outrows, outrows), outrows), :]
            for mask in reversed(range(1, g)):
                remote(term(flip(mask)), target, late_send, terms_recv.at[1], flip(mask), k).start()
            pltpu.make_async_copy(term(j), target, terms_recv.at[1]).start()

        def far_half(at):
            d, chip = pairs[at]
            band = far_rows(d, 2 * chip, 2)
            total = part[band, :]
            for m in range(half - 1):
                wait_bytes(part_in.at[m, band, :], part_recv.at[m, at])
                total = total + part_in[m, band, :].astype(jnp.float32)
            far_out[band, :] = total.astype(far_out.dtype)
            if at < joined:
                remote(far_out.at[band, :], far_in.at[band, :], far_send, far_recv.at[at], j, other).start()
                return
            for to in (2 * chip, 2 * chip + 1):
                remote(far_out.at[far_rows(d, to), :], terms.at[0, :, pl.ds(pl.multiple_of(j * cols, cols), cols)],
                       far_send, terms_recv.at[0], to, other).start()

        def late_result(at):
            d, chip = pairs[at]
            band = near_rows(d, 2 * chip, 2)
            wait_bytes(far_in.at[band, :], far_recv.at[at])
            late[band, :] = (near_sum[band, :] + far_in[band, :].astype(jnp.float32)).astype(late.dtype)
            target = out_ref.at[planes - 1, :, pl.ds(pl.multiple_of(j * cols, cols), cols)]
            for to in (2 * chip, 2 * chip + 1):
                remote(late.at[near_rows(d, to), :], target, late_send, out_recv.at[1], to, near(d)).start()

        early = (planes - 2) * parts

        def one(t, carry):
            i = jnp.where(t < early, t, early + lax.div(t - early, half))
            d = jnp.where(t < early, first, first - lax.rem(t - early, half))
            c, h = lax.div(i, parts), lax.rem(i, parts)
            at = pl.multiple_of(h * width, width)

            @pl.when(t == 1)
            def _():
                for e in range(3, raw):
                    forward(e)
                for e in outer_first[1:]:
                    share(e)

            @pl.when(t == early)
            def _():
                for e in outer_first[1:]:
                    complete(e)
                    for whole in range(planes - 2):
                        product(jnp.int32(e), whole, pl.ds(0, cols), 0, 0)
                        results(jnp.int32(e), whole, 0, cols)

            @pl.when(t == early + 1)
            def _():
                near_half()
                far_half(0)
                far_half(1)

            @pl.when(t == early + 2)
            def _():
                far_half(2)

            @pl.when(t == last_turn)
            def _():
                far_half(3)
                late_result(0)
                pl.semaphore_wait(ready.at[rounds + 1], 1)
                far_half(4)
                late_result(1)

            product(d, c, pl.ds(at, width), i, 1)
            results(d, c, at, width)
            return carry

        last_turn = early + half * parts - 1
        lax.fori_loop(0, last_turn + 1, one, 0)
        for at in range(5, len(pairs)):
            far_half(at)
            if at - 3 < joined:
                late_result(at - 3)
        for at in range(len(pairs) - 3, joined):
            late_result(at)
        wait_bytes(op_bytes(half * half), op_send)
        wait_bytes(blocks.at[pl.ds(0, planes - 1), pl.ds(0, half * rows), :], block_send)
        wait_bytes(blocks.at[pl.ds(0, planes - 1), pl.ds(0, half * rows - outrows), :], res_send)
        for e in range(len(sources)):
            wait_bytes(op_bytes(half * (g - 1)), spread_send.at[e])
        wait_bytes(far_out, far_send)
        wait_bytes(late.at[pl.ds(0, half * rows - outrows), :], late_send)
        for b in (1, 0):
            wait_bytes(terms.at[b], terms_recv.at[b])
        out_ref[planes - 1] = (terms[0].astype(jnp.float32) + terms[1].astype(jnp.float32)).astype(out_ref.dtype)

    @pl.when(jnp.logical_not(is_centre))
    def _():
        m = away - 1

        def op_in(d):
            remote(first_ops.at[1, d], ops.at[near_rows(d, j), from_source(k)],
                   op_send, op_recv.at[m, d], j, centre).start()

        def op_past(d):
            remote(first_ops.at[0, d], passing.at[m, d], op_send, pass_recv.at[m, d], j, centre).start()

        staged_in(1)
        op_in(half - 1)
        staged_in(0)
        for d in outer_first:
            op_past(d)
        for d in outer_first[1:]:
            op_in(d)
        own_start.wait()
        own_rest.wait()
        for i in range(raw):
            at = block_part(k, i)
            remote(at, at, block_send, blk_recv.at[near_slot(m, i)], j, centre).start()
        remote(last_plane(k), last_plane(k), block_send, blk_recv.at[near_slot(m, raw)], j, centre).start()
        operator_in()
        own_part()
        part_out[...] = part[...].astype(part_out.dtype)
        for at, (d, chip) in enumerate(pairs):
            band = far_rows(d, 2 * chip, 2)
            remote(part_out.at[band, :], part_in.at[m, band, :], far_send, part_recv.at[m, at], j, centre).start()
        plane_entered()
        signal(ready.at[rounds], j, centre)
        wait_bytes(op_bytes(2 * half), op_send)
        wait_bytes(blocks.at[:, from_source(0), :], block_send)
        wait_bytes(part_out, far_send)

    wait_bytes(out_ref.at[pl.ds(0, planes - 1)], out_recv.at[0])

    @pl.when(jnp.logical_not(is_centre))
    def _():
        wait_bytes(out_ref.at[planes - 1], out_recv.at[1])


def at_centres(n, g, products, operator):
    rows, planes, cols = products.shape
    parts = 2 if cols % (2 * LANES) == 0 else 1
    half = n // 2
    outer, roles, raw = max(half - 1, 1), 2 * half - 1, (planes - 1) * parts
    out = pl.pallas_call(
        functools.partial(kernel, n, g, parts),
        out_shape=jax.ShapeDtypeStruct((planes, rows // g, cols * g), jnp.bfloat16),
        in_specs=[pl.BlockSpec(memory_space=pl.ANY)] * 2,
        out_specs=pl.BlockSpec(memory_space=pltpu.VMEM),
        scratch_shapes=[
            pltpu.VMEM((planes, n * rows, cols), jnp.bfloat16),
            pltpu.VMEM((half * rows, n * rows), jnp.bfloat16),
            pltpu.VMEM((half * rows, rows), jnp.bfloat16),
            pltpu.VMEM((2, half, rows // g, rows), jnp.bfloat16),
            pltpu.VMEM((outer, half, rows // g, rows), jnp.bfloat16),
            pltpu.VMEM((half, planes - 1, rows, cols), jnp.bfloat16),
            pltpu.VMEM((rows, cols), jnp.float32),
            pltpu.VMEM((half * rows, cols), jnp.float32),
            pltpu.VMEM((half * rows, cols), jnp.bfloat16),
            pltpu.VMEM((outer, half * rows, cols), jnp.bfloat16),
            pltpu.VMEM((half * rows, cols), jnp.bfloat16),
            pltpu.VMEM((half * rows, cols), jnp.bfloat16),
            pltpu.VMEM((half * rows, cols), jnp.float32),
            pltpu.VMEM((rows, cols), jnp.bfloat16),
            pltpu.VMEM((half * rows, cols), jnp.bfloat16),
            pltpu.VMEM((2, rows // g, g * cols), jnp.bfloat16),
            pltpu.SemaphoreType.DMA,
            pltpu.SemaphoreType.DMA,
            pltpu.SemaphoreType.DMA((roles,)),
            pltpu.SemaphoreType.DMA,
            pltpu.SemaphoreType.DMA,
            pltpu.SemaphoreType.DMA,
            pltpu.SemaphoreType.DMA((outer * (raw + 1) + half * raw,)),
            pltpu.SemaphoreType.DMA((roles, half)),
            pltpu.SemaphoreType.DMA((outer, half)),
            pltpu.SemaphoreType.DMA((roles, half)),
            pltpu.SemaphoreType.DMA((half,)),
            pltpu.SemaphoreType.DMA((2,)),
            pltpu.SemaphoreType.DMA((outer, half * g // 2)),
            pltpu.SemaphoreType.DMA((outer * g // 2,)),
            pltpu.SemaphoreType.DMA((2,)),
            pltpu.SemaphoreType.DMA((5,)),
            pltpu.SemaphoreType.REGULAR((g.bit_length() + 1,)),
        ],
        compiler_params=pltpu.CompilerParams(
            collective_id=0, has_side_effects=True, vmem_limit_bytes=GRANT),
    )(products.transpose(1, 0, 2), operator)
    return out.transpose(1, 0, 2)


def by_collectives(products, operator):
    y_local, three, m_local = products.shape
    flat = products.reshape(y_local, three * m_local)
    summed = lax.psum_scatter(
        jnp.dot(operator, flat, preferred_element_type=jnp.float32), "gy", scatter_dimension=0, tiled=True)
    result = summed.astype(jnp.bfloat16).reshape(y_local, three, m_local)
    return lax.all_to_all(result, "gx", split_axis=0, concat_axis=2, tiled=True)


def solution(mesh):
    n, g = mesh.shape["gy"], mesh.shape["gx"]

    def body(products, operator):
        rows, planes, cols = products.shape
        aligned = (n // 2 == 2 and n % 2 == 0 and planes > 2 and g & (g - 1) == 0 and g > 4 and rows % (g * SUBLANES) == 0
                   and rows % LANES == 0 and cols % (2 * LANES) == 0)
        held = 2 * (products.size * (n + n // 2 + 2) + operator.size * (2 + n // 2)) + 20 * n * rows * cols
        if aligned and held < VMEM_BYTES // 2:
            return at_centres(n, g, products, operator)
        return by_collectives(products, operator)

    return jax.shard_map(
        body,
        mesh=mesh,
        in_specs=(P("gy", None, "gx"), P(None, "gy")),
        out_specs=P(("gy", "gx"), None, None),
        check_vma=False,
    )
```

```python
import functools

import jax
import jax.numpy as jnp
from jax import lax
from jax.experimental import pallas as pl
from jax.experimental.pallas import tpu as pltpu
from jax.sharding import PartitionSpec as P

MESH = pl.DeviceIdType.MESH
LANES = 128
SUBLANES = 16
VMEM_BYTES = 60 * 1024 * 1024
GRANT = 54500 * 1024


def kernel(n, g, parts, p_ref, op_ref, out_ref, blocks, ops, far_ops, first_ops, passing, res, wide, part, part_out,
           part_in, far_out, far_in, near_sum, near_out, late, terms, block_send, op_send, spread_send, res_send,
           far_send, late_send, blk_recv, op_recv, pass_recv, plane_recv, sibling_recv, out_recv, part_recv, far_recv,
           terms_recv, own_copy, ready):
    j, k = lax.axis_index("gx"), lax.axis_index("gy")
    half = n // 2
    side = lax.div(k, half)
    step = 1 - 2 * side
    centre = jnp.where(side == 0, half - 1, half)
    other = n - 1 - centre
    is_centre = k == centre
    away = step * (centre - k)
    planes, rows, cols = p_ref.shape
    width = cols // parts
    raw = (planes - 1) * parts
    outrows = rows // g
    mine = pl.ds(pl.multiple_of(side * (half * rows), half * rows), half * rows)
    theirs = pl.ds(pl.multiple_of((1 - side) * (half * rows), half * rows), half * rows)

    def flip(mask):
        to = j
        for bit in (1 << b for b in range(mask.bit_length())):
            if mask & bit:
                to = to + bit * (1 - 2 * lax.rem(lax.div(j, bit), 2))
        return to

    def near(d):
        return centre - step * d

    def far(d):
        return other + step * d

    def from_source(s):
        return pl.ds(pl.multiple_of(s * rows, rows), rows)

    def near_rows(d, to, count=1):
        at = (near(d) - side * half) * rows + to * outrows
        return pl.ds(pl.multiple_of(at, outrows), count * outrows)

    def far_rows(d, to, count=1):
        at = (far(d) - (1 - side) * half) * rows + to * outrows
        return pl.ds(pl.multiple_of(at, outrows), count * outrows)

    def wait_bytes(ref, sem):
        pltpu.make_async_copy(ref, ref, sem).wait()

    def op_bytes(pieces):
        return ops.at[pl.ds(0, pieces * outrows), pl.ds(0, rows)]

    rounds = g.bit_length() - 1
    barrier = pltpu.get_barrier_semaphore()

    def signal(sem, gx, gy):
        pl.semaphore_signal(sem, inc=1, device_id=(gx, gy), device_id_type=MESH)

    @pl.when(is_centre)
    def _():
        signal(barrier, j, other)
        for d in range(1, half):
            signal(barrier, j, near(d))

    for b in range(rounds):
        signal(barrier, flip(1 << b), k)

    def staged(slot, d):
        at = far_rows(d, j) if slot == 0 else near_rows(d, j)
        start = (theirs if slot == 0 else mine).start
        return pltpu.make_async_copy(
            op_ref.at[pl.ds(pl.multiple_of(start + at.start, outrows), outrows), :], first_ops.at[slot, d],
            own_copy.at[slot])

    own_start = pltpu.make_async_copy(p_ref.at[0], blocks.at[0, from_source(k), :], own_copy.at[2])
    own_rest = pltpu.make_async_copy(
        p_ref.at[pl.ds(1, planes - 1)], blocks.at[pl.ds(1, planes - 1), from_source(k), :], own_copy.at[3])
    own_far = pltpu.make_async_copy(op_ref.at[theirs, :], far_ops, own_copy.at[4])
    own_ops = pltpu.make_async_copy(op_ref.at[mine, :], ops.at[:, from_source(k)], own_copy.at[4])
    for d in reversed(range(half)):
        for slot in (1, 0):
            staged(slot, d).start()
    own_start.start()
    for copy in (own_rest, own_far, own_ops):
        copy.start()

    def staged_in(slot):
        wait_bytes(first_ops.at[slot], own_copy.at[slot])

    def operator_in():
        wait_bytes(ops.at[:, pl.ds(0, 2 * rows)], own_copy.at[4])

    pl.semaphore_wait(barrier, rounds + 1)

    def plane_entered():
        for b in range(rounds):
            signal(ready.at[b], flip(1 << b), k)
            pl.semaphore_wait(ready.at[b], 1)

    def remote(src, dst, send, recv, gx, gy):
        return pltpu.make_async_remote_copy(
            src_ref=src, dst_ref=dst, send_sem=send, recv_sem=recv,
            device_id=(gx, gy), device_id_type=MESH)

    def lanes(i):
        return pl.ds(pl.multiple_of(lax.rem(i, parts) * width, width), width)

    def block_part(s, i):
        return blocks.at[lax.div(i, parts), from_source(s), lanes(i)]

    def near_slot(m, i):
        return m * (raw + 1) + i

    def far_slot(m, i):
        return (half - 1) * (raw + 1) + m * raw + i

    def last_plane(s):
        return blocks.at[planes - 1, from_source(s), :]

    sources = [near(d) for d in range(1, half)] + [far(d) for d in range(half)]

    chips = g // 2
    column = lax.div(j, 2)

    def bits(x):
        return bin(x).count("1")

    def pick(at):
        chip = jnp.int32(0)
        for c in range(chips):
            order = sorted(range(1, chips), key=lambda x: (bits(x) - bits(x ^ c), x == c, x))
            chip = jnp.where(column == c, order[at], chip)
        return chip

    turns = [pick(at) for at in range(chips - 1)]
    outer_first = list(reversed(range(half)))
    pairs = [(d, 0) for d in outer_first[:-1]] + [(d, chip) for d in outer_first[:-1] for chip in turns]
    joined = len(pairs)
    pairs += [(0, chip) for chip in [0] + turns]

    def own_part():
        part[...] = jnp.dot(far_ops[...], last_plane(k)[...], preferred_element_type=jnp.float32)

    @pl.when(is_centre)
    def _():
        def block_out(i):
            at = block_part(k, i)
            remote(at, at, block_send, blk_recv.at[far_slot(0, i)], j, other).start()

        staged_in(0)
        for d in outer_first:
            remote(first_ops.at[0, d], ops.at[far_rows(d, j), from_source(k)],
                   op_send, op_recv.at[half - 1, d], j, other).start()
        own_start.wait()
        block_out(0)
        block_out(1)
        staged_in(1)
        own_rest.wait()
        operator_in()
        own_part()

        def spread(e, d, at, mask):
            part_of = ops.at[near_rows(d, at), from_source(sources[e])]
            sem = sibling_recv.at[d] if mask == 1 else plane_recv.at[e, d]
            remote(part_of, part_of, spread_send.at[e], sem, flip(mask), k).start()

        adjacent = [1 << b for b in reversed(range(rounds))]
        distant = [2 * m for m in range(1, g // 2) if 2 * m not in adjacent]

        def enter(e, d, everywhere):
            wait_bytes(op_bytes(1), op_recv.at[e, d])
            for mask in (distant if everywhere else []) + adjacent:
                spread(e, d, j, mask)

        def share(d):
            for e in range(len(sources)):
                wait_bytes(op_bytes(g // 2 - 1), plane_recv.at[e, d])
                for mask in range(1, g // 2):
                    spread(e, d, flip(2 * mask), 1)

        def complete(d):
            wait_bytes(op_bytes(len(sources) * (g // 2)), sibling_recv.at[d])

        def pass_on(d):
            for m in range(half - 1):
                wait_bytes(op_bytes(1), pass_recv.at[m, d])
                remote(passing.at[m, d], ops.at[far_rows(d, j), from_source(near(m + 1))],
                       op_send, op_recv.at[half + m, d], j, other).start()

        def forward(i):
            for m in range(half - 1):
                at = block_part(near(m + 1), i)
                wait_bytes(at, blk_recv.at[near_slot(m, i)])
                remote(at, at, block_send, blk_recv.at[far_slot(m + 1, i)], j, other).start()

        closest, rest = range(half), range(half, 2 * half - 1)
        first = half - 1
        enter(0, first, False)
        plane_entered()
        signal(ready.at[rounds + 1], j, other)
        for mask in distant:
            spread(0, first, j, mask)
        for e in closest[1:]:
            enter(e, first, True)
        for d in outer_first:
            pass_on(d)
        block_out(2)
        forward(0)
        for e in rest:
            enter(e, first, True)
        for d in outer_first[1:]:
            for e in range(len(sources)):
                enter(e, d, True)
        forward(1)
        forward(2)
        for i in range(3, raw):
            block_out(i)
        share(first)
        complete(first)
        if half > 1:
            pl.semaphore_wait(ready.at[rounds], half - 1)

        band_of = lambda d: from_source(near(d) - side * half)
        others = pl.ds(pl.multiple_of(side * rows, rows), (n - 1) * rows)
        final = far(half - 1)

        def results(d, c, lane, size):
            target = pl.ds(pl.multiple_of(j * cols + lane, width), size)
            lane = pl.ds(lane, size)

            def result(to):
                return res.at[d, c, pl.ds(pl.multiple_of(to * outrows, outrows), outrows), lane]

            @pl.when(d > 0)
            def _():
                for to in range(g):
                    remote(result(to), out_ref.at[c, :, target], res_send, out_recv.at[0], to, near(d)).start()

            @pl.when(d == 0)
            def _():
                for mask in range(1, g):
                    to = flip(mask)
                    remote(result(to), out_ref.at[c, :, target], res_send, out_recv.at[0], to, near(d)).start()
                pltpu.make_async_copy(result(j), out_ref.at[c, :, target], out_recv.at[0]).start()

        def product(d, c, lane, i_first, count):
            band = band_of(d)

            @pl.when(d == first)
            def _():
                for e in range(half - 1):
                    for i in range(count):
                        wait_bytes(block_part(0, 0), blk_recv.at[far_slot(e, i_first + i)])
            size = lane.size
            ahead = wide.at[:, pl.ds(0, size)]
            ahead[...] = jnp.dot(ops[band, others], blocks[c, others, lane], preferred_element_type=jnp.float32)

            @pl.when(d == first)
            def _():
                for i in range(count):
                    wait_bytes(block_part(0, 0), blk_recv.at[far_slot(half - 1, i_first + i)])
            total = ahead[...] + jnp.dot(
                ops[band, from_source(final)], blocks[c, from_source(final), lane], preferred_element_type=jnp.float32)
            res[d, c, :, lane] = total.astype(res.dtype)

        def near_half():
            for m in range(half - 1):
                wait_bytes(last_plane(0), blk_recv.at[near_slot(m, raw)])
            near_sum[...] = jnp.dot(ops[:, mine], blocks[planes - 1, mine, :], preferred_element_type=jnp.float32)
            near_out[...] = near_sum[band_of(0), :].astype(near_out.dtype)
            target = terms.at[1, :, pl.ds(pl.multiple_of(j * cols, cols), cols)]

            def term(to):
                return near_out.at[pl.ds(pl.multiple_of(to * outrows, outrows), outrows), :]
            for mask in reversed(range(1, g)):
                remote(term(flip(mask)), target, late_send, terms_recv.at[1], flip(mask), k).start()
            pltpu.make_async_copy(term(j), target, terms_recv.at[1]).start()

        def far_half(at):
            d, chip = pairs[at]
            band = far_rows(d, 2 * chip, 2)
            total = part[band, :]
            for m in range(half - 1):
                wait_bytes(part_in.at[m, band, :], part_recv.at[m, at])
                total = total + part_in[m, band, :].astype(jnp.float32)
            far_out[band, :] = total.astype(far_out.dtype)
            if at < joined:
                remote(far_out.at[band, :], far_in.at[band, :], far_send, far_recv.at[at], j, other).start()
                return
            for to in (2 * chip, 2 * chip + 1):
                remote(far_out.at[far_rows(d, to), :], terms.at[0, :, pl.ds(pl.multiple_of(j * cols, cols), cols)],
                       far_send, terms_recv.at[0], to, other).start()

        def late_result(at):
            d, chip = pairs[at]
            band = near_rows(d, 2 * chip, 2)
            wait_bytes(far_in.at[band, :], far_recv.at[at])
            late[band, :] = (near_sum[band, :] + far_in[band, :].astype(jnp.float32)).astype(late.dtype)
            target = out_ref.at[planes - 1, :, pl.ds(pl.multiple_of(j * cols, cols), cols)]
            for to in (2 * chip, 2 * chip + 1):
                remote(late.at[near_rows(d, to), :], target, late_send, out_recv.at[1], to, near(d)).start()

        early = (planes - 2) * parts

        def one(t, carry):
            i = jnp.where(t < early, t, early + lax.div(t - early, half))
            d = jnp.where(t < early, first, first - lax.rem(t - early, half))
            c, h = lax.div(i, parts), lax.rem(i, parts)
            at = pl.multiple_of(h * width, width)

            @pl.when(t == 1)
            def _():
                for e in range(3, raw):
                    forward(e)
                for e in outer_first[1:]:
                    share(e)

            @pl.when(t == early)
            def _():
                for e in outer_first[1:]:
                    complete(e)
                    for whole in range(planes - 2):
                        product(jnp.int32(e), whole, pl.ds(0, cols), 0, 0)
                        results(jnp.int32(e), whole, 0, cols)

            @pl.when(t == early + 1)
            def _():
                near_half()
                far_half(0)
                far_half(1)

            @pl.when(t == early + 2)
            def _():
                far_half(2)

            @pl.when(t == last_turn)
            def _():
                far_half(3)
                late_result(0)
                pl.semaphore_wait(ready.at[rounds + 1], 1)
                far_half(4)
                late_result(1)

            product(d, c, pl.ds(at, width), i, 1)
            results(d, c, at, width)
            return carry

        last_turn = early + half * parts - 1
        lax.fori_loop(0, last_turn + 1, one, 0)
        for at in range(5, len(pairs)):
            far_half(at)
            if at - 3 < joined:
                late_result(at - 3)
        for at in range(len(pairs) - 3, joined):
            late_result(at)
        wait_bytes(op_bytes(half * half), op_send)
        wait_bytes(blocks.at[pl.ds(0, planes - 1), pl.ds(0, half * rows), :], block_send)
        wait_bytes(blocks.at[pl.ds(0, planes - 1), pl.ds(0, half * rows - outrows), :], res_send)
        for e in range(len(sources)):
            wait_bytes(op_bytes(half * (g - 1)), spread_send.at[e])
        wait_bytes(far_out, far_send)
        wait_bytes(late.at[pl.ds(0, half * rows - outrows), :], late_send)
        for b in (1, 0):
            wait_bytes(terms.at[b], terms_recv.at[b])
        out_ref[planes - 1] = (terms[0].astype(jnp.float32) + terms[1].astype(jnp.float32)).astype(out_ref.dtype)

    @pl.when(jnp.logical_not(is_centre))
    def _():
        m = away - 1

        def op_in(d):
            remote(first_ops.at[1, d], ops.at[near_rows(d, j), from_source(k)],
                   op_send, op_recv.at[m, d], j, centre).start()

        def op_past(d):
            remote(first_ops.at[0, d], passing.at[m, d], op_send, pass_recv.at[m, d], j, centre).start()

        staged_in(1)
        op_in(half - 1)
        staged_in(0)
        for d in outer_first:
            op_past(d)
        for d in outer_first[1:]:
            op_in(d)
        own_start.wait()
        own_rest.wait()
        for i in range(raw):
            at = block_part(k, i)
            remote(at, at, block_send, blk_recv.at[near_slot(m, i)], j, centre).start()
        remote(last_plane(k), last_plane(k), block_send, blk_recv.at[near_slot(m, raw)], j, centre).start()
        operator_in()
        own_part()
        part_out[...] = part[...].astype(part_out.dtype)
        for at, (d, chip) in enumerate(pairs):
            band = far_rows(d, 2 * chip, 2)
            remote(part_out.at[band, :], part_in.at[m, band, :], far_send, part_recv.at[m, at], j, centre).start()
        plane_entered()
        signal(ready.at[rounds], j, centre)
        wait_bytes(op_bytes(2 * half), op_send)
        wait_bytes(blocks.at[:, from_source(0), :], block_send)
        wait_bytes(part_out, far_send)

    wait_bytes(out_ref.at[pl.ds(0, planes - 1)], out_recv.at[0])

    @pl.when(jnp.logical_not(is_centre))
    def _():
        wait_bytes(out_ref.at[planes - 1], out_recv.at[1])


def at_centres(n, g, products, operator):
    rows, planes, cols = products.shape
    parts = 2 if cols % (2 * LANES) == 0 else 1
    half = n // 2
    outer, roles, raw = max(half - 1, 1), 2 * half - 1, (planes - 1) * parts
    out = pl.pallas_call(
        functools.partial(kernel, n, g, parts),
        out_shape=jax.ShapeDtypeStruct((planes, rows // g, cols * g), jnp.bfloat16),
        in_specs=[pl.BlockSpec(memory_space=pl.ANY)] * 2,
        out_specs=pl.BlockSpec(memory_space=pltpu.VMEM),
        scratch_shapes=[
            pltpu.VMEM((planes, n * rows, cols), jnp.bfloat16),
            pltpu.VMEM((half * rows, n * rows), jnp.bfloat16),
            pltpu.VMEM((half * rows, rows), jnp.bfloat16),
            pltpu.VMEM((2, half, rows // g, rows), jnp.bfloat16),
            pltpu.VMEM((outer, half, rows // g, rows), jnp.bfloat16),
            pltpu.VMEM((half, planes - 1, rows, cols), jnp.bfloat16),
            pltpu.VMEM((rows, cols), jnp.float32),
            pltpu.VMEM((half * rows, cols), jnp.float32),
            pltpu.VMEM((half * rows, cols), jnp.bfloat16),
            pltpu.VMEM((outer, half * rows, cols), jnp.bfloat16),
            pltpu.VMEM((half * rows, cols), jnp.bfloat16),
            pltpu.VMEM((half * rows, cols), jnp.bfloat16),
            pltpu.VMEM((half * rows, cols), jnp.float32),
            pltpu.VMEM((rows, cols), jnp.bfloat16),
            pltpu.VMEM((half * rows, cols), jnp.bfloat16),
            pltpu.VMEM((2, rows // g, g * cols), jnp.bfloat16),
            pltpu.SemaphoreType.DMA,
            pltpu.SemaphoreType.DMA,
            pltpu.SemaphoreType.DMA((roles,)),
            pltpu.SemaphoreType.DMA,
            pltpu.SemaphoreType.DMA,
            pltpu.SemaphoreType.DMA,
            pltpu.SemaphoreType.DMA((outer * (raw + 1) + half * raw,)),
            pltpu.SemaphoreType.DMA((roles, half)),
            pltpu.SemaphoreType.DMA((outer, half)),
            pltpu.SemaphoreType.DMA((roles, half)),
            pltpu.SemaphoreType.DMA((half,)),
            pltpu.SemaphoreType.DMA((2,)),
            pltpu.SemaphoreType.DMA((outer, half * g // 2)),
            pltpu.SemaphoreType.DMA((outer * g // 2,)),
            pltpu.SemaphoreType.DMA((2,)),
            pltpu.SemaphoreType.DMA((5,)),
            pltpu.SemaphoreType.REGULAR((g.bit_length() + 1,)),
        ],
        compiler_params=pltpu.CompilerParams(
            collective_id=0, has_side_effects=True, vmem_limit_bytes=GRANT),
    )(products.transpose(1, 0, 2), operator)
    return out.transpose(1, 0, 2)


def by_collectives(products, operator):
    y_local, three, m_local = products.shape
    flat = products.reshape(y_local, three * m_local)
    summed = lax.psum_scatter(
        jnp.dot(operator, flat, preferred_element_type=jnp.float32), "gy", scatter_dimension=0, tiled=True)
    result = summed.astype(jnp.bfloat16).reshape(y_local, three, m_local)
    return lax.all_to_all(result, "gx", split_axis=0, concat_axis=2, tiled=True)


def solution(mesh):
    n, g = mesh.shape["gy"], mesh.shape["gx"]

    def body(products, operator):
        rows, planes, cols = products.shape
        aligned = (n // 2 == 2 and n % 2 == 0 and planes > 2 and g & (g - 1) == 0 and g > 4 and rows % (g * SUBLANES) == 0
                   and rows % LANES == 0 and cols % (2 * LANES) == 0)
        held = 2 * (products.size * (n + n // 2 + 2) + operator.size * (2 + n // 2)) + 20 * n * rows * cols
        if aligned and held < VMEM_BYTES // 2:
            return at_centres(n, g, products, operator)
        return by_collectives(products, operator)

    return jax.shard_map(
        body,
        mesh=mesh,
        in_specs=(P("gy", None, "gx"), P(None, "gy")),
        out_specs=P(("gy", "gx"), None, None),
        check_vma=False,
    )
```

```python
import functools

import jax
import jax.numpy as jnp
from jax import lax
from jax.experimental import pallas as pl
from jax.experimental.pallas import tpu as pltpu
from jax.sharding import PartitionSpec as P

MESH = pl.DeviceIdType.MESH
LANES = 128
SUBLANES = 16
VMEM_BYTES = 60 * 1024 * 1024
GRANT = 54500 * 1024


def kernel(n, g, parts, p_ref, op_ref, out_ref, blocks, ops, far_ops, first_ops, passing, res, wide, part, part_out,
           part_in, far_out, far_in, near_sum, near_out, late, terms, block_send, op_send, spread_send, res_send,
           far_send, late_send, blk_recv, op_recv, pass_recv, plane_recv, sibling_recv, out_recv, part_recv, far_recv,
           terms_recv, own_copy, ready):
    j, k = lax.axis_index("gx"), lax.axis_index("gy")
    half = n // 2
    side = lax.div(k, half)
    step = 1 - 2 * side
    centre = jnp.where(side == 0, half - 1, half)
    other = n - 1 - centre
    is_centre = k == centre
    away = step * (centre - k)
    planes, rows, cols = p_ref.shape
    width = cols // parts
    raw = (planes - 1) * parts
    outrows = rows // g
    mine = pl.ds(pl.multiple_of(side * (half * rows), half * rows), half * rows)
    theirs = pl.ds(pl.multiple_of((1 - side) * (half * rows), half * rows), half * rows)

    def flip(mask):
        to = j
        for bit in (1 << b for b in range(mask.bit_length())):
            if mask & bit:
                to = to + bit * (1 - 2 * lax.rem(lax.div(j, bit), 2))
        return to

    def near(d):
        return centre - step * d

    def far(d):
        return other + step * d

    def from_source(s):
        return pl.ds(pl.multiple_of(s * rows, rows), rows)

    def near_rows(d, to, count=1):
        at = (near(d) - side * half) * rows + to * outrows
        return pl.ds(pl.multiple_of(at, outrows), count * outrows)

    def far_rows(d, to, count=1):
        at = (far(d) - (1 - side) * half) * rows + to * outrows
        return pl.ds(pl.multiple_of(at, outrows), count * outrows)

    def wait_bytes(ref, sem):
        pltpu.make_async_copy(ref, ref, sem).wait()

    def op_bytes(pieces):
        return ops.at[pl.ds(0, pieces * outrows), pl.ds(0, rows)]

    rounds = g.bit_length() - 1
    barrier = pltpu.get_barrier_semaphore()

    def signal(sem, gx, gy):
        pl.semaphore_signal(sem, inc=1, device_id=(gx, gy), device_id_type=MESH)

    @pl.when(is_centre)
    def _():
        signal(barrier, j, other)
        for d in range(1, half):
            signal(barrier, j, near(d))

    for b in range(rounds):
        signal(barrier, flip(1 << b), k)

    def staged(slot, d):
        at = far_rows(d, j) if slot == 0 else near_rows(d, j)
        start = (theirs if slot == 0 else mine).start
        return pltpu.make_async_copy(
            op_ref.at[pl.ds(pl.multiple_of(start + at.start, outrows), outrows), :], first_ops.at[slot, d],
            own_copy.at[slot])

    own_start = pltpu.make_async_copy(p_ref.at[0], blocks.at[0, from_source(k), :], own_copy.at[2])
    own_rest = pltpu.make_async_copy(
        p_ref.at[pl.ds(1, planes - 1)], blocks.at[pl.ds(1, planes - 1), from_source(k), :], own_copy.at[3])
    own_far = pltpu.make_async_copy(op_ref.at[theirs, :], far_ops, own_copy.at[4])
    own_ops = pltpu.make_async_copy(op_ref.at[mine, :], ops.at[:, from_source(k)], own_copy.at[4])
    for d in reversed(range(half)):
        for slot in (1, 0):
            staged(slot, d).start()
    own_start.start()
    for copy in (own_rest, own_far, own_ops):
        copy.start()

    def staged_in(slot):
        wait_bytes(first_ops.at[slot], own_copy.at[slot])

    def operator_in():
        wait_bytes(ops.at[:, pl.ds(0, 2 * rows)], own_copy.at[4])

    pl.semaphore_wait(barrier, rounds + 1)

    def plane_entered():
        for b in range(rounds):
            signal(ready.at[b], flip(1 << b), k)
            pl.semaphore_wait(ready.at[b], 1)

    def remote(src, dst, send, recv, gx, gy):
        return pltpu.make_async_remote_copy(
            src_ref=src, dst_ref=dst, send_sem=send, recv_sem=recv,
            device_id=(gx, gy), device_id_type=MESH)

    def lanes(i):
        return pl.ds(pl.multiple_of(lax.rem(i, parts) * width, width), width)

    def block_part(s, i):
        return blocks.at[lax.div(i, parts), from_source(s), lanes(i)]

    def near_slot(m, i):
        return m * (raw + 1) + i

    def far_slot(m, i):
        return (half - 1) * (raw + 1) + m * raw + i

    def last_plane(s):
        return blocks.at[planes - 1, from_source(s), :]

    sources = [near(d) for d in range(1, half)] + [far(d) for d in range(half)]

    chips = g // 2
    column = lax.div(j, 2)

    def bits(x):
        return bin(x).count("1")

    def pick(at):
        chip = jnp.int32(0)
        for c in range(chips):
            order = sorted(range(1, chips), key=lambda x: (bits(x) - bits(x ^ c), x == c, x))
            chip = jnp.where(column == c, order[at], chip)
        return chip

    turns = [pick(at) for at in range(chips - 1)]
    outer_first = list(reversed(range(half)))
    pairs = [(d, 0) for d in outer_first[:-1]] + [(d, chip) for d in outer_first[:-1] for chip in turns]
    joined = len(pairs)
    pairs += [(0, chip) for chip in [0] + turns]

    def own_part():
        part[...] = jnp.dot(far_ops[...], last_plane(k)[...], preferred_element_type=jnp.float32)

    @pl.when(is_centre)
    def _():
        def block_out(i):
            at = block_part(k, i)
            remote(at, at, block_send, blk_recv.at[far_slot(0, i)], j, other).start()

        staged_in(0)
        for d in outer_first:
            remote(first_ops.at[0, d], ops.at[far_rows(d, j), from_source(k)],
                   op_send, op_recv.at[half - 1, d], j, other).start()
        own_start.wait()
        block_out(0)
        block_out(1)
        staged_in(1)
        own_rest.wait()
        operator_in()
        own_part()

        def spread(e, d, at, mask):
            part_of = ops.at[near_rows(d, at), from_source(sources[e])]
            sem = sibling_recv.at[d] if mask == 1 else plane_recv.at[e, d]
            remote(part_of, part_of, spread_send.at[e], sem, flip(mask), k).start()

        adjacent = [1 << b for b in reversed(range(rounds))]
        distant = [2 * m for m in range(1, g // 2) if 2 * m not in adjacent]

        def enter(e, d, everywhere):
            wait_bytes(op_bytes(1), op_recv.at[e, d])
            for mask in (distant if everywhere else []) + adjacent:
                spread(e, d, j, mask)

        def share(d):
            for e in range(len(sources)):
                wait_bytes(op_bytes(g // 2 - 1), plane_recv.at[e, d])
                for mask in range(1, g // 2):
                    spread(e, d, flip(2 * mask), 1)

        def complete(d):
            wait_bytes(op_bytes(len(sources) * (g // 2)), sibling_recv.at[d])

        def pass_on(d):
            for m in range(half - 1):
                wait_bytes(op_bytes(1), pass_recv.at[m, d])
                remote(passing.at[m, d], ops.at[far_rows(d, j), from_source(near(m + 1))],
                       op_send, op_recv.at[half + m, d], j, other).start()

        def forward(i):
            for m in range(half - 1):
                at = block_part(near(m + 1), i)
                wait_bytes(at, blk_recv.at[near_slot(m, i)])
                remote(at, at, block_send, blk_recv.at[far_slot(m + 1, i)], j, other).start()

        closest, rest = range(half), range(half, 2 * half - 1)
        first = half - 1
        enter(0, first, False)
        plane_entered()
        signal(ready.at[rounds + 1], j, other)
        for mask in distant:
            spread(0, first, j, mask)
        for e in closest[1:]:
            enter(e, first, True)
        for d in outer_first:
            pass_on(d)
        block_out(2)
        forward(0)
        for e in rest:
            enter(e, first, True)
        for d in outer_first[1:]:
            for e in range(len(sources)):
                enter(e, d, True)
        forward(1)
        forward(2)
        for i in range(3, raw):
            block_out(i)
        share(first)
        complete(first)
        if half > 1:
            pl.semaphore_wait(ready.at[rounds], half - 1)

        band_of = lambda d: from_source(near(d) - side * half)
        others = pl.ds(pl.multiple_of(side * rows, rows), (n - 1) * rows)
        final = far(half - 1)

        def results(d, c, lane, size):
            target = pl.ds(pl.multiple_of(j * cols + lane, width), size)
            lane = pl.ds(lane, size)

            def result(to):
                return res.at[d, c, pl.ds(pl.multiple_of(to * outrows, outrows), outrows), lane]

            @pl.when(d > 0)
            def _():
                for to in range(g):
                    remote(result(to), out_ref.at[c, :, target], res_send, out_recv.at[0], to, near(d)).start()

            @pl.when(d == 0)
            def _():
                for mask in range(1, g):
                    to = flip(mask)
                    remote(result(to), out_ref.at[c, :, target], res_send, out_recv.at[0], to, near(d)).start()
                pltpu.make_async_copy(result(j), out_ref.at[c, :, target], out_recv.at[0]).start()

        def product(d, c, lane, i_first, count):
            band = band_of(d)

            @pl.when(d == first)
            def _():
                for e in range(half - 1):
                    for i in range(count):
                        wait_bytes(block_part(0, 0), blk_recv.at[far_slot(e, i_first + i)])
            size = lane.size
            ahead = wide.at[:, pl.ds(0, size)]
            ahead[...] = jnp.dot(ops[band, others], blocks[c, others, lane], preferred_element_type=jnp.float32)

            @pl.when(d == first)
            def _():
                for i in range(count):
                    wait_bytes(block_part(0, 0), blk_recv.at[far_slot(half - 1, i_first + i)])
            total = ahead[...] + jnp.dot(
                ops[band, from_source(final)], blocks[c, from_source(final), lane], preferred_element_type=jnp.float32)
            res[d, c, :, lane] = total.astype(res.dtype)

        def near_half():
            for m in range(half - 1):
                wait_bytes(last_plane(0), blk_recv.at[near_slot(m, raw)])
            near_sum[...] = jnp.dot(ops[:, mine], blocks[planes - 1, mine, :], preferred_element_type=jnp.float32)
            near_out[...] = near_sum[band_of(0), :].astype(near_out.dtype)
            target = terms.at[1, :, pl.ds(pl.multiple_of(j * cols, cols), cols)]

            def term(to):
                return near_out.at[pl.ds(pl.multiple_of(to * outrows, outrows), outrows), :]
            for mask in reversed(range(1, g)):
                remote(term(flip(mask)), target, late_send, terms_recv.at[1], flip(mask), k).start()
            pltpu.make_async_copy(term(j), target, terms_recv.at[1]).start()

        def far_half(at):
            d, chip = pairs[at]
            band = far_rows(d, 2 * chip, 2)
            total = part[band, :]
            for m in range(half - 1):
                wait_bytes(part_in.at[m, band, :], part_recv.at[m, at])
                total = total + part_in[m, band, :].astype(jnp.float32)
            far_out[band, :] = total.astype(far_out.dtype)
            if at < joined:
                remote(far_out.at[band, :], far_in.at[band, :], far_send, far_recv.at[at], j, other).start()
                return
            for to in (2 * chip, 2 * chip + 1):
                remote(far_out.at[far_rows(d, to), :], terms.at[0, :, pl.ds(pl.multiple_of(j * cols, cols), cols)],
                       far_send, terms_recv.at[0], to, other).start()

        def late_result(at):
            d, chip = pairs[at]
            band = near_rows(d, 2 * chip, 2)
            wait_bytes(far_in.at[band, :], far_recv.at[at])
            late[band, :] = (near_sum[band, :] + far_in[band, :].astype(jnp.float32)).astype(late.dtype)
            target = out_ref.at[planes - 1, :, pl.ds(pl.multiple_of(j * cols, cols), cols)]
            for to in (2 * chip, 2 * chip + 1):
                remote(late.at[near_rows(d, to), :], target, late_send, out_recv.at[1], to, near(d)).start()

        early = (planes - 2) * parts

        def one(t, carry):
            i = jnp.where(t < early, t, early + lax.div(t - early, half))
            d = jnp.where(t < early, first, first - lax.rem(t - early, half))
            c, h = lax.div(i, parts), lax.rem(i, parts)
            at = pl.multiple_of(h * width, width)

            @pl.when(t == 1)
            def _():
                for e in range(3, raw):
                    forward(e)
                for e in outer_first[1:]:
                    share(e)

            @pl.when(t == early)
            def _():
                for e in outer_first[1:]:
                    complete(e)
                    for whole in range(planes - 2):
                        product(jnp.int32(e), whole, pl.ds(0, cols), 0, 0)
                        results(jnp.int32(e), whole, 0, cols)

            @pl.when(t == early + 1)
            def _():
                near_half()
                far_half(0)
                far_half(1)

            @pl.when(t == early + 2)
            def _():
                far_half(2)

            @pl.when(t == last_turn)
            def _():
                far_half(3)

            product(d, c, pl.ds(at, width), i, 1)
            results(d, c, at, width)
            return carry

        last_turn = early + half * parts - 1
        lax.fori_loop(0, last_turn + 1, one, 0)
        late_result(0)
        pl.semaphore_wait(ready.at[rounds + 1], 1)
        far_half(4)
        late_result(1)
        for at in range(5, len(pairs)):
            far_half(at)
            if at - 3 < joined:
                late_result(at - 3)
        for at in range(len(pairs) - 3, joined):
            late_result(at)
        wait_bytes(op_bytes(half * half), op_send)
        wait_bytes(blocks.at[pl.ds(0, planes - 1), pl.ds(0, half * rows), :], block_send)
        wait_bytes(blocks.at[pl.ds(0, planes - 1), pl.ds(0, half * rows - outrows), :], res_send)
        for e in range(len(sources)):
            wait_bytes(op_bytes(half * (g - 1)), spread_send.at[e])
        wait_bytes(far_out, far_send)
        wait_bytes(late.at[pl.ds(0, half * rows - outrows), :], late_send)
        for b in (1, 0):
            wait_bytes(terms.at[b], terms_recv.at[b])
        out_ref[planes - 1] = (terms[0].astype(jnp.float32) + terms[1].astype(jnp.float32)).astype(out_ref.dtype)

    @pl.when(jnp.logical_not(is_centre))
    def _():
        m = away - 1

        def op_in(d):
            remote(first_ops.at[1, d], ops.at[near_rows(d, j), from_source(k)],
                   op_send, op_recv.at[m, d], j, centre).start()

        def op_past(d):
            remote(first_ops.at[0, d], passing.at[m, d], op_send, pass_recv.at[m, d], j, centre).start()

        staged_in(1)
        op_in(half - 1)
        staged_in(0)
        for d in outer_first:
            op_past(d)
        for d in outer_first[1:]:
            op_in(d)
        own_start.wait()
        own_rest.wait()
        for i in range(raw):
            at = block_part(k, i)
            remote(at, at, block_send, blk_recv.at[near_slot(m, i)], j, centre).start()
        remote(last_plane(k), last_plane(k), block_send, blk_recv.at[near_slot(m, raw)], j, centre).start()
        operator_in()
        own_part()
        part_out[...] = part[...].astype(part_out.dtype)
        for at, (d, chip) in enumerate(pairs):
            band = far_rows(d, 2 * chip, 2)
            remote(part_out.at[band, :], part_in.at[m, band, :], far_send, part_recv.at[m, at], j, centre).start()
        plane_entered()
        signal(ready.at[rounds], j, centre)
        wait_bytes(op_bytes(2 * half), op_send)
        wait_bytes(blocks.at[:, from_source(0), :], block_send)
        wait_bytes(part_out, far_send)

    wait_bytes(out_ref.at[pl.ds(0, planes - 1)], out_recv.at[0])

    @pl.when(jnp.logical_not(is_centre))
    def _():
        wait_bytes(out_ref.at[planes - 1], out_recv.at[1])


def at_centres(n, g, products, operator):
    rows, planes, cols = products.shape
    parts = 2 if cols % (2 * LANES) == 0 else 1
    half = n // 2
    outer, roles, raw = max(half - 1, 1), 2 * half - 1, (planes - 1) * parts
    out = pl.pallas_call(
        functools.partial(kernel, n, g, parts),
        out_shape=jax.ShapeDtypeStruct((planes, rows // g, cols * g), jnp.bfloat16),
        in_specs=[pl.BlockSpec(memory_space=pl.ANY)] * 2,
        out_specs=pl.BlockSpec(memory_space=pltpu.VMEM),
        scratch_shapes=[
            pltpu.VMEM((planes, n * rows, cols), jnp.bfloat16),
            pltpu.VMEM((half * rows, n * rows), jnp.bfloat16),
            pltpu.VMEM((half * rows, rows), jnp.bfloat16),
            pltpu.VMEM((2, half, rows // g, rows), jnp.bfloat16),
            pltpu.VMEM((outer, half, rows // g, rows), jnp.bfloat16),
            pltpu.VMEM((half, planes - 1, rows, cols), jnp.bfloat16),
            pltpu.VMEM((rows, cols), jnp.float32),
            pltpu.VMEM((half * rows, cols), jnp.float32),
            pltpu.VMEM((half * rows, cols), jnp.bfloat16),
            pltpu.VMEM((outer, half * rows, cols), jnp.bfloat16),
            pltpu.VMEM((half * rows, cols), jnp.bfloat16),
            pltpu.VMEM((half * rows, cols), jnp.bfloat16),
            pltpu.VMEM((half * rows, cols), jnp.float32),
            pltpu.VMEM((rows, cols), jnp.bfloat16),
            pltpu.VMEM((half * rows, cols), jnp.bfloat16),
            pltpu.VMEM((2, rows // g, g * cols), jnp.bfloat16),
            pltpu.SemaphoreType.DMA,
            pltpu.SemaphoreType.DMA,
            pltpu.SemaphoreType.DMA((roles,)),
            pltpu.SemaphoreType.DMA,
            pltpu.SemaphoreType.DMA,
            pltpu.SemaphoreType.DMA,
            pltpu.SemaphoreType.DMA((outer * (raw + 1) + half * raw,)),
            pltpu.SemaphoreType.DMA((roles, half)),
            pltpu.SemaphoreType.DMA((outer, half)),
            pltpu.SemaphoreType.DMA((roles, half)),
            pltpu.SemaphoreType.DMA((half,)),
            pltpu.SemaphoreType.DMA((2,)),
            pltpu.SemaphoreType.DMA((outer, half * g // 2)),
            pltpu.SemaphoreType.DMA((outer * g // 2,)),
            pltpu.SemaphoreType.DMA((2,)),
            pltpu.SemaphoreType.DMA((5,)),
            pltpu.SemaphoreType.REGULAR((g.bit_length() + 1,)),
        ],
        compiler_params=pltpu.CompilerParams(
            collective_id=0, has_side_effects=True, vmem_limit_bytes=GRANT),
    )(products.transpose(1, 0, 2), operator)
    return out.transpose(1, 0, 2)


def by_collectives(products, operator):
    y_local, three, m_local = products.shape
    flat = products.reshape(y_local, three * m_local)
    summed = lax.psum_scatter(
        jnp.dot(operator, flat, preferred_element_type=jnp.float32), "gy", scatter_dimension=0, tiled=True)
    result = summed.astype(jnp.bfloat16).reshape(y_local, three, m_local)
    return lax.all_to_all(result, "gx", split_axis=0, concat_axis=2, tiled=True)


def solution(mesh):
    n, g = mesh.shape["gy"], mesh.shape["gx"]

    def body(products, operator):
        rows, planes, cols = products.shape
        aligned = (n // 2 == 2 and n % 2 == 0 and planes > 2 and g & (g - 1) == 0 and g > 4 and rows % (g * SUBLANES) == 0
                   and rows % LANES == 0 and cols % (2 * LANES) == 0)
        held = 2 * (products.size * (n + n // 2 + 2) + operator.size * (2 + n // 2)) + 20 * n * rows * cols
        if aligned and held < VMEM_BYTES // 2:
            return at_centres(n, g, products, operator)
        return by_collectives(products, operator)

    return jax.shard_map(
        body,
        mesh=mesh,
        in_specs=(P("gy", None, "gx"), P(None, "gy")),
        out_specs=P(("gy", "gx"), None, None),
        check_vma=False,
    )
```

```python
import functools

import jax
import jax.numpy as jnp
from jax import lax
from jax.experimental import pallas as pl
from jax.experimental.pallas import tpu as pltpu
from jax.sharding import PartitionSpec as P

MESH = pl.DeviceIdType.MESH
LANES = 128
SUBLANES = 16
VMEM_BYTES = 60 * 1024 * 1024
GRANT = 54500 * 1024


def kernel(n, g, parts, p_ref, op_ref, out_ref, blocks, ops, far_ops, first_ops, passing, res, wide, part, part_out,
           part_in, far_out, far_in, near_sum, near_out, late, terms, block_send, op_send, spread_send, res_send,
           far_send, late_send, blk_recv, op_recv, pass_recv, plane_recv, sibling_recv, out_recv, part_recv, far_recv,
           terms_recv, own_copy, ready):
    j, k = lax.axis_index("gx"), lax.axis_index("gy")
    half = n // 2
    side = lax.div(k, half)
    step = 1 - 2 * side
    centre = jnp.where(side == 0, half - 1, half)
    other = n - 1 - centre
    is_centre = k == centre
    away = step * (centre - k)
    planes, rows, cols = p_ref.shape
    width = cols // parts
    raw = (planes - 1) * parts
    outrows = rows // g
    mine = pl.ds(pl.multiple_of(side * (half * rows), half * rows), half * rows)
    theirs = pl.ds(pl.multiple_of((1 - side) * (half * rows), half * rows), half * rows)

    def flip(mask):
        to = j
        for bit in (1 << b for b in range(mask.bit_length())):
            if mask & bit:
                to = to + bit * (1 - 2 * lax.rem(lax.div(j, bit), 2))
        return to

    def near(d):
        return centre - step * d

    def far(d):
        return other + step * d

    def from_source(s):
        return pl.ds(pl.multiple_of(s * rows, rows), rows)

    def near_rows(d, to, count=1):
        at = (near(d) - side * half) * rows + to * outrows
        return pl.ds(pl.multiple_of(at, outrows), count * outrows)

    def far_rows(d, to, count=1):
        at = (far(d) - (1 - side) * half) * rows + to * outrows
        return pl.ds(pl.multiple_of(at, outrows), count * outrows)

    def wait_bytes(ref, sem):
        pltpu.make_async_copy(ref, ref, sem).wait()

    def op_bytes(pieces):
        return ops.at[pl.ds(0, pieces * outrows), pl.ds(0, rows)]

    rounds = g.bit_length() - 1
    barrier = pltpu.get_barrier_semaphore()

    def signal(sem, gx, gy):
        pl.semaphore_signal(sem, inc=1, device_id=(gx, gy), device_id_type=MESH)

    @pl.when(is_centre)
    def _():
        signal(barrier, j, other)
        for d in range(1, half):
            signal(barrier, j, near(d))

    for b in range(rounds):
        signal(barrier, flip(1 << b), k)

    def staged(slot, d):
        at = far_rows(d, j) if slot == 0 else near_rows(d, j)
        start = (theirs if slot == 0 else mine).start
        return pltpu.make_async_copy(
            op_ref.at[pl.ds(pl.multiple_of(start + at.start, outrows), outrows), :], first_ops.at[slot, d],
            own_copy.at[slot])

    own_start = pltpu.make_async_copy(p_ref.at[0], blocks.at[0, from_source(k), :], own_copy.at[2])
    own_rest = pltpu.make_async_copy(
        p_ref.at[pl.ds(1, planes - 1)], blocks.at[pl.ds(1, planes - 1), from_source(k), :], own_copy.at[3])
    own_far = pltpu.make_async_copy(op_ref.at[theirs, :], far_ops, own_copy.at[4])
    own_ops = pltpu.make_async_copy(op_ref.at[mine, :], ops.at[:, from_source(k)], own_copy.at[4])
    for d in reversed(range(half)):
        for slot in (1, 0):
            staged(slot, d).start()
    own_start.start()
    for copy in (own_rest, own_far, own_ops):
        copy.start()

    def staged_in(slot):
        wait_bytes(first_ops.at[slot], own_copy.at[slot])

    def operator_in():
        wait_bytes(ops.at[:, pl.ds(0, 2 * rows)], own_copy.at[4])

    pl.semaphore_wait(barrier, rounds + 1)

    def plane_entered():
        for b in range(rounds):
            signal(ready.at[b], flip(1 << b), k)
            pl.semaphore_wait(ready.at[b], 1)

    def remote(src, dst, send, recv, gx, gy):
        return pltpu.make_async_remote_copy(
            src_ref=src, dst_ref=dst, send_sem=send, recv_sem=recv,
            device_id=(gx, gy), device_id_type=MESH)

    def lanes(i):
        return pl.ds(pl.multiple_of(lax.rem(i, parts) * width, width), width)

    def block_part(s, i):
        return blocks.at[lax.div(i, parts), from_source(s), lanes(i)]

    def near_slot(m, i):
        return m * (raw + 1) + i

    def far_slot(m, i):
        return (half - 1) * (raw + 1) + m * raw + i

    def last_plane(s):
        return blocks.at[planes - 1, from_source(s), :]

    sources = [near(d) for d in range(1, half)] + [far(d) for d in range(half)]

    chips = g // 2
    column = lax.div(j, 2)

    def bits(x):
        return bin(x).count("1")

    def pick(at):
        chip = jnp.int32(0)
        for c in range(chips):
            order = sorted(range(1, chips), key=lambda x: (bits(x) - bits(x ^ c), x == c, x))
            chip = jnp.where(column == c, order[at], chip)
        return chip

    turns = [pick(at) for at in range(chips - 1)]
    outer_first = list(reversed(range(half)))
    pairs = [(d, 0) for d in outer_first[:-1]] + [(d, chip) for d in outer_first[:-1] for chip in turns]
    joined = len(pairs)
    pairs += [(0, chip) for chip in [0] + turns]

    def own_part():
        part[...] = jnp.dot(far_ops[...], last_plane(k)[...], preferred_element_type=jnp.float32)

    @pl.when(is_centre)
    def _():
        def block_out(i):
            at = block_part(k, i)
            remote(at, at, block_send, blk_recv.at[far_slot(0, i)], j, other).start()

        staged_in(0)
        for d in outer_first:
            remote(first_ops.at[0, d], ops.at[far_rows(d, j), from_source(k)],
                   op_send, op_recv.at[half - 1, d], j, other).start()
        own_start.wait()
        block_out(0)
        block_out(1)
        staged_in(1)
        own_rest.wait()
        operator_in()
        own_part()

        def spread(e, d, at, mask):
            part_of = ops.at[near_rows(d, at), from_source(sources[e])]
            sem = sibling_recv.at[d] if mask == 1 else plane_recv.at[e, d]
            remote(part_of, part_of, spread_send.at[e], sem, flip(mask), k).start()

        adjacent = [1 << b for b in reversed(range(rounds))]
        distant = [2 * m for m in range(1, g // 2) if 2 * m not in adjacent]

        def enter(e, d, everywhere):
            wait_bytes(op_bytes(1), op_recv.at[e, d])
            for mask in [1] + (distant if everywhere else []) + adjacent[:-1]:
                spread(e, d, j, mask)

        def share(d):
            for e in range(len(sources)):
                wait_bytes(op_bytes(g // 2 - 1), plane_recv.at[e, d])
                for mask in range(1, g // 2):
                    spread(e, d, flip(2 * mask), 1)

        def complete(d):
            wait_bytes(op_bytes(len(sources) * (g // 2)), sibling_recv.at[d])

        def pass_on(d):
            for m in range(half - 1):
                wait_bytes(op_bytes(1), pass_recv.at[m, d])
                remote(passing.at[m, d], ops.at[far_rows(d, j), from_source(near(m + 1))],
                       op_send, op_recv.at[half + m, d], j, other).start()

        def forward(i):
            for m in range(half - 1):
                at = block_part(near(m + 1), i)
                wait_bytes(at, blk_recv.at[near_slot(m, i)])
                remote(at, at, block_send, blk_recv.at[far_slot(m + 1, i)], j, other).start()

        closest, rest = range(half), range(half, 2 * half - 1)
        first = half - 1
        enter(0, first, False)
        plane_entered()
        signal(ready.at[rounds + 1], j, other)
        for mask in distant:
            spread(0, first, j, mask)
        for e in closest[1:]:
            enter(e, first, True)
        for d in outer_first:
            pass_on(d)
        block_out(2)
        forward(0)
        for e in rest:
            enter(e, first, True)
        for d in outer_first[1:]:
            for e in range(len(sources)):
                enter(e, d, True)
        forward(1)
        forward(2)
        for i in range(3, raw):
            block_out(i)
        share(first)
        complete(first)
        if half > 1:
            pl.semaphore_wait(ready.at[rounds], half - 1)

        band_of = lambda d: from_source(near(d) - side * half)
        others = pl.ds(pl.multiple_of(side * rows, rows), (n - 1) * rows)
        final = far(half - 1)

        def results(d, c, lane, size):
            target = pl.ds(pl.multiple_of(j * cols + lane, width), size)
            lane = pl.ds(lane, size)

            def result(to):
                return res.at[d, c, pl.ds(pl.multiple_of(to * outrows, outrows), outrows), lane]

            @pl.when(d > 0)
            def _():
                for to in range(g):
                    remote(result(to), out_ref.at[c, :, target], res_send, out_recv.at[0], to, near(d)).start()

            @pl.when(d == 0)
            def _():
                for mask in range(1, g):
                    to = flip(mask)
                    remote(result(to), out_ref.at[c, :, target], res_send, out_recv.at[0], to, near(d)).start()
                pltpu.make_async_copy(result(j), out_ref.at[c, :, target], out_recv.at[0]).start()

        def product(d, c, lane, i_first, count):
            band = band_of(d)

            @pl.when(d == first)
            def _():
                for e in range(half - 1):
                    for i in range(count):
                        wait_bytes(block_part(0, 0), blk_recv.at[far_slot(e, i_first + i)])
            size = lane.size
            ahead = wide.at[:, pl.ds(0, size)]
            ahead[...] = jnp.dot(ops[band, others], blocks[c, others, lane], preferred_element_type=jnp.float32)

            @pl.when(d == first)
            def _():
                for i in range(count):
                    wait_bytes(block_part(0, 0), blk_recv.at[far_slot(half - 1, i_first + i)])
            total = ahead[...] + jnp.dot(
                ops[band, from_source(final)], blocks[c, from_source(final), lane], preferred_element_type=jnp.float32)
            res[d, c, :, lane] = total.astype(res.dtype)

        def near_half():
            for m in range(half - 1):
                wait_bytes(last_plane(0), blk_recv.at[near_slot(m, raw)])
            near_sum[...] = jnp.dot(ops[:, mine], blocks[planes - 1, mine, :], preferred_element_type=jnp.float32)
            near_out[...] = near_sum[band_of(0), :].astype(near_out.dtype)
            target = terms.at[1, :, pl.ds(pl.multiple_of(j * cols, cols), cols)]

            def term(to):
                return near_out.at[pl.ds(pl.multiple_of(to * outrows, outrows), outrows), :]
            for mask in reversed(range(1, g)):
                remote(term(flip(mask)), target, late_send, terms_recv.at[1], flip(mask), k).start()
            pltpu.make_async_copy(term(j), target, terms_recv.at[1]).start()

        def far_half(at):
            d, chip = pairs[at]
            band = far_rows(d, 2 * chip, 2)
            total = part[band, :]
            for m in range(half - 1):
                wait_bytes(part_in.at[m, band, :], part_recv.at[m, at])
                total = total + part_in[m, band, :].astype(jnp.float32)
            far_out[band, :] = total.astype(far_out.dtype)
            if at < joined:
                remote(far_out.at[band, :], far_in.at[band, :], far_send, far_recv.at[at], j, other).start()
                return
            for to in (2 * chip, 2 * chip + 1):
                remote(far_out.at[far_rows(d, to), :], terms.at[0, :, pl.ds(pl.multiple_of(j * cols, cols), cols)],
                       far_send, terms_recv.at[0], to, other).start()

        def late_result(at):
            d, chip = pairs[at]
            band = near_rows(d, 2 * chip, 2)
            wait_bytes(far_in.at[band, :], far_recv.at[at])
            late[band, :] = (near_sum[band, :] + far_in[band, :].astype(jnp.float32)).astype(late.dtype)
            target = out_ref.at[planes - 1, :, pl.ds(pl.multiple_of(j * cols, cols), cols)]
            for to in (2 * chip, 2 * chip + 1):
                remote(late.at[near_rows(d, to), :], target, late_send, out_recv.at[1], to, near(d)).start()

        early = (planes - 2) * parts

        def one(t, carry):
            i = jnp.where(t < early, t, early + lax.div(t - early, half))
            d = jnp.where(t < early, first, first - lax.rem(t - early, half))
            c, h = lax.div(i, parts), lax.rem(i, parts)
            at = pl.multiple_of(h * width, width)

            @pl.when(t == 1)
            def _():
                for e in range(3, raw):
                    forward(e)
                for e in outer_first[1:]:
                    share(e)

            @pl.when(t == early)
            def _():
                for e in outer_first[1:]:
                    complete(e)
                    for whole in range(planes - 2):
                        product(jnp.int32(e), whole, pl.ds(0, cols), 0, 0)
                        results(jnp.int32(e), whole, 0, cols)

            @pl.when(t == early + 1)
            def _():
                near_half()
                far_half(0)
                far_half(1)

            @pl.when(t == early + 2)
            def _():
                far_half(2)

            @pl.when(t == last_turn)
            def _():
                far_half(3)

            product(d, c, pl.ds(at, width), i, 1)
            results(d, c, at, width)
            return carry

        last_turn = early + half * parts - 1
        lax.fori_loop(0, last_turn + 1, one, 0)
        late_result(0)
        pl.semaphore_wait(ready.at[rounds + 1], 1)
        far_half(4)
        late_result(1)
        for at in range(5, len(pairs)):
            far_half(at)
            if at - 3 < joined:
                late_result(at - 3)
        for at in range(len(pairs) - 3, joined):
            late_result(at)
        wait_bytes(op_bytes(half * half), op_send)
        wait_bytes(blocks.at[pl.ds(0, planes - 1), pl.ds(0, half * rows), :], block_send)
        wait_bytes(blocks.at[pl.ds(0, planes - 1), pl.ds(0, half * rows - outrows), :], res_send)
        for e in range(len(sources)):
            wait_bytes(op_bytes(half * (g - 1)), spread_send.at[e])
        wait_bytes(far_out, far_send)
        wait_bytes(late.at[pl.ds(0, half * rows - outrows), :], late_send)
        for b in (1, 0):
            wait_bytes(terms.at[b], terms_recv.at[b])
        out_ref[planes - 1] = (terms[0].astype(jnp.float32) + terms[1].astype(jnp.float32)).astype(out_ref.dtype)

    @pl.when(jnp.logical_not(is_centre))
    def _():
        m = away - 1

        def op_in(d):
            remote(first_ops.at[1, d], ops.at[near_rows(d, j), from_source(k)],
                   op_send, op_recv.at[m, d], j, centre).start()

        def op_past(d):
            remote(first_ops.at[0, d], passing.at[m, d], op_send, pass_recv.at[m, d], j, centre).start()

        staged_in(1)
        op_in(half - 1)
        staged_in(0)
        for d in outer_first:
            op_past(d)
        for d in outer_first[1:]:
            op_in(d)
        own_start.wait()
        own_rest.wait()
        for i in range(raw):
            at = block_part(k, i)
            remote(at, at, block_send, blk_recv.at[near_slot(m, i)], j, centre).start()
        remote(last_plane(k), last_plane(k), block_send, blk_recv.at[near_slot(m, raw)], j, centre).start()
        operator_in()
        own_part()
        part_out[...] = part[...].astype(part_out.dtype)
        for at, (d, chip) in enumerate(pairs):
            band = far_rows(d, 2 * chip, 2)
            remote(part_out.at[band, :], part_in.at[m, band, :], far_send, part_recv.at[m, at], j, centre).start()
        plane_entered()
        signal(ready.at[rounds], j, centre)
        wait_bytes(op_bytes(2 * half), op_send)
        wait_bytes(blocks.at[:, from_source(0), :], block_send)
        wait_bytes(part_out, far_send)

    wait_bytes(out_ref.at[pl.ds(0, planes - 1)], out_recv.at[0])

    @pl.when(jnp.logical_not(is_centre))
    def _():
        wait_bytes(out_ref.at[planes - 1], out_recv.at[1])


def at_centres(n, g, products, operator):
    rows, planes, cols = products.shape
    parts = 2 if cols % (2 * LANES) == 0 else 1
    half = n // 2
    outer, roles, raw = max(half - 1, 1), 2 * half - 1, (planes - 1) * parts
    out = pl.pallas_call(
        functools.partial(kernel, n, g, parts),
        out_shape=jax.ShapeDtypeStruct((planes, rows // g, cols * g), jnp.bfloat16),
        in_specs=[pl.BlockSpec(memory_space=pl.ANY)] * 2,
        out_specs=pl.BlockSpec(memory_space=pltpu.VMEM),
        scratch_shapes=[
            pltpu.VMEM((planes, n * rows, cols), jnp.bfloat16),
            pltpu.VMEM((half * rows, n * rows), jnp.bfloat16),
            pltpu.VMEM((half * rows, rows), jnp.bfloat16),
            pltpu.VMEM((2, half, rows // g, rows), jnp.bfloat16),
            pltpu.VMEM((outer, half, rows // g, rows), jnp.bfloat16),
            pltpu.VMEM((half, planes - 1, rows, cols), jnp.bfloat16),
            pltpu.VMEM((rows, cols), jnp.float32),
            pltpu.VMEM((half * rows, cols), jnp.float32),
            pltpu.VMEM((half * rows, cols), jnp.bfloat16),
            pltpu.VMEM((outer, half * rows, cols), jnp.bfloat16),
            pltpu.VMEM((half * rows, cols), jnp.bfloat16),
            pltpu.VMEM((half * rows, cols), jnp.bfloat16),
            pltpu.VMEM((half * rows, cols), jnp.float32),
            pltpu.VMEM((rows, cols), jnp.bfloat16),
            pltpu.VMEM((half * rows, cols), jnp.bfloat16),
            pltpu.VMEM((2, rows // g, g * cols), jnp.bfloat16),
            pltpu.SemaphoreType.DMA,
            pltpu.SemaphoreType.DMA,
            pltpu.SemaphoreType.DMA((roles,)),
            pltpu.SemaphoreType.DMA,
            pltpu.SemaphoreType.DMA,
            pltpu.SemaphoreType.DMA,
            pltpu.SemaphoreType.DMA((outer * (raw + 1) + half * raw,)),
            pltpu.SemaphoreType.DMA((roles, half)),
            pltpu.SemaphoreType.DMA((outer, half)),
            pltpu.SemaphoreType.DMA((roles, half)),
            pltpu.SemaphoreType.DMA((half,)),
            pltpu.SemaphoreType.DMA((2,)),
            pltpu.SemaphoreType.DMA((outer, half * g // 2)),
            pltpu.SemaphoreType.DMA((outer * g // 2,)),
            pltpu.SemaphoreType.DMA((2,)),
            pltpu.SemaphoreType.DMA((5,)),
            pltpu.SemaphoreType.REGULAR((g.bit_length() + 1,)),
        ],
        compiler_params=pltpu.CompilerParams(
            collective_id=0, has_side_effects=True, vmem_limit_bytes=GRANT),
    )(products.transpose(1, 0, 2), operator)
    return out.transpose(1, 0, 2)


def by_collectives(products, operator):
    y_local, three, m_local = products.shape
    flat = products.reshape(y_local, three * m_local)
    summed = lax.psum_scatter(
        jnp.dot(operator, flat, preferred_element_type=jnp.float32), "gy", scatter_dimension=0, tiled=True)
    result = summed.astype(jnp.bfloat16).reshape(y_local, three, m_local)
    return lax.all_to_all(result, "gx", split_axis=0, concat_axis=2, tiled=True)


def solution(mesh):
    n, g = mesh.shape["gy"], mesh.shape["gx"]

    def body(products, operator):
        rows, planes, cols = products.shape
        aligned = (n // 2 == 2 and n % 2 == 0 and planes > 2 and g & (g - 1) == 0 and g > 4 and rows % (g * SUBLANES) == 0
                   and rows % LANES == 0 and cols % (2 * LANES) == 0)
        held = 2 * (products.size * (n + n // 2 + 2) + operator.size * (2 + n // 2)) + 20 * n * rows * cols
        if aligned and held < VMEM_BYTES // 2:
            return at_centres(n, g, products, operator)
        return by_collectives(products, operator)

    return jax.shard_map(
        body,
        mesh=mesh,
        in_specs=(P("gy", None, "gx"), P(None, "gy")),
        out_specs=P(("gy", "gx"), None, None),
        check_vma=False,
    )
```

```python
import functools

import jax
import jax.numpy as jnp
from jax import lax
from jax.experimental import pallas as pl
from jax.experimental.pallas import tpu as pltpu
from jax.sharding import PartitionSpec as P

MESH = pl.DeviceIdType.MESH
LANES = 128
SUBLANES = 16
VMEM_BYTES = 60 * 1024 * 1024
GRANT = 54500 * 1024


def kernel(n, g, parts, p_ref, op_ref, out_ref, blocks, ops, far_ops, first_ops, passing, res, wide, part, part_out,
           part_in, far_out, far_in, near_sum, near_out, late, terms, block_send, op_send, spread_send, res_send,
           far_send, late_send, blk_recv, op_recv, pass_recv, plane_recv, sibling_recv, out_recv, part_recv, far_recv,
           terms_recv, own_copy, ready):
    j, k = lax.axis_index("gx"), lax.axis_index("gy")
    half = n // 2
    side = lax.div(k, half)
    step = 1 - 2 * side
    centre = jnp.where(side == 0, half - 1, half)
    other = n - 1 - centre
    is_centre = k == centre
    away = step * (centre - k)
    planes, rows, cols = p_ref.shape
    width = cols // parts
    raw = (planes - 1) * parts
    outrows = rows // g
    mine = pl.ds(pl.multiple_of(side * (half * rows), half * rows), half * rows)
    theirs = pl.ds(pl.multiple_of((1 - side) * (half * rows), half * rows), half * rows)

    def flip(mask):
        to = j
        for bit in (1 << b for b in range(mask.bit_length())):
            if mask & bit:
                to = to + bit * (1 - 2 * lax.rem(lax.div(j, bit), 2))
        return to

    def near(d):
        return centre - step * d

    def far(d):
        return other + step * d

    def from_source(s):
        return pl.ds(pl.multiple_of(s * rows, rows), rows)

    def near_rows(d, to, count=1):
        at = (near(d) - side * half) * rows + to * outrows
        return pl.ds(pl.multiple_of(at, outrows), count * outrows)

    def far_rows(d, to, count=1):
        at = (far(d) - (1 - side) * half) * rows + to * outrows
        return pl.ds(pl.multiple_of(at, outrows), count * outrows)

    def wait_bytes(ref, sem):
        pltpu.make_async_copy(ref, ref, sem).wait()

    def op_bytes(pieces):
        return ops.at[pl.ds(0, pieces * outrows), pl.ds(0, rows)]

    rounds = g.bit_length() - 1
    barrier = pltpu.get_barrier_semaphore()

    def signal(sem, gx, gy):
        pl.semaphore_signal(sem, inc=1, device_id=(gx, gy), device_id_type=MESH)

    @pl.when(is_centre)
    def _():
        signal(barrier, j, other)
        for d in range(1, half):
            signal(barrier, j, near(d))

    for b in range(rounds):
        signal(barrier, flip(1 << b), k)

    def staged(slot, d):
        at = far_rows(d, j) if slot == 0 else near_rows(d, j)
        start = (theirs if slot == 0 else mine).start
        return pltpu.make_async_copy(
            op_ref.at[pl.ds(pl.multiple_of(start + at.start, outrows), outrows), :], first_ops.at[slot, d],
            own_copy.at[slot])

    own_start = pltpu.make_async_copy(p_ref.at[0], blocks.at[0, from_source(k), :], own_copy.at[2])
    own_rest = pltpu.make_async_copy(
        p_ref.at[pl.ds(1, planes - 1)], blocks.at[pl.ds(1, planes - 1), from_source(k), :], own_copy.at[3])
    own_far = pltpu.make_async_copy(op_ref.at[theirs, :], far_ops, own_copy.at[4])
    own_ops = pltpu.make_async_copy(op_ref.at[mine, :], ops.at[:, from_source(k)], own_copy.at[4])
    for d in reversed(range(half)):
        for slot in (1, 0):
            staged(slot, d).start()
    own_start.start()
    for copy in (own_rest, own_far, own_ops):
        copy.start()

    def staged_in(slot):
        wait_bytes(first_ops.at[slot], own_copy.at[slot])

    def operator_in():
        wait_bytes(ops.at[:, pl.ds(0, 2 * rows)], own_copy.at[4])

    pl.semaphore_wait(barrier, rounds + 1)

    def plane_entered():
        for b in range(rounds):
            signal(ready.at[b], flip(1 << b), k)
            pl.semaphore_wait(ready.at[b], 1)

    def remote(src, dst, send, recv, gx, gy):
        return pltpu.make_async_remote_copy(
            src_ref=src, dst_ref=dst, send_sem=send, recv_sem=recv,
            device_id=(gx, gy), device_id_type=MESH)

    def lanes(i):
        return pl.ds(pl.multiple_of(lax.rem(i, parts) * width, width), width)

    def block_part(s, i):
        return blocks.at[lax.div(i, parts), from_source(s), lanes(i)]

    def near_slot(m, i):
        return m * (raw + 1) + i

    def far_slot(m, i):
        return (half - 1) * (raw + 1) + m * raw + i

    def last_plane(s):
        return blocks.at[planes - 1, from_source(s), :]

    sources = [near(d) for d in range(1, half)] + [far(d) for d in range(half)]

    chips = g // 2
    column = lax.div(j, 2)

    def bits(x):
        return bin(x).count("1")

    def pick(at):
        chip = jnp.int32(0)
        for c in range(chips):
            order = sorted(range(1, chips), key=lambda x: (bits(x) - bits(x ^ c), x == c, x))
            chip = jnp.where(column == c, order[at], chip)
        return chip

    turns = [pick(at) for at in range(chips - 1)]
    outer_first = list(reversed(range(half)))
    pairs = [(d, 0) for d in outer_first[:-1]] + [(d, chip) for d in outer_first[:-1] for chip in turns]
    joined = len(pairs)
    pairs += [(0, chip) for chip in turns[:1] + [0] + turns[1:]]

    def own_part():
        part[...] = jnp.dot(far_ops[...], last_plane(k)[...], preferred_element_type=jnp.float32)

    @pl.when(is_centre)
    def _():
        def block_out(i):
            at = block_part(k, i)
            remote(at, at, block_send, blk_recv.at[far_slot(0, i)], j, other).start()

        staged_in(0)
        for d in outer_first:
            remote(first_ops.at[0, d], ops.at[far_rows(d, j), from_source(k)],
                   op_send, op_recv.at[half - 1, d], j, other).start()
        own_start.wait()
        block_out(0)
        block_out(1)
        staged_in(1)
        own_rest.wait()
        operator_in()
        own_part()

        def spread(e, d, at, mask):
            part_of = ops.at[near_rows(d, at), from_source(sources[e])]
            sem = sibling_recv.at[d] if mask == 1 else plane_recv.at[e, d]
            remote(part_of, part_of, spread_send.at[e], sem, flip(mask), k).start()

        adjacent = [1 << b for b in reversed(range(rounds))]
        distant = [2 * m for m in range(1, g // 2) if 2 * m not in adjacent]

        def enter(e, d, everywhere):
            wait_bytes(op_bytes(1), op_recv.at[e, d])
            for mask in [1] + (distant if everywhere else []) + adjacent[:-1]:
                spread(e, d, j, mask)

        def share(d):
            for e in range(len(sources)):
                wait_bytes(op_bytes(g // 2 - 1), plane_recv.at[e, d])
                for mask in range(1, g // 2):
                    spread(e, d, flip(2 * mask), 1)

        def complete(d):
            wait_bytes(op_bytes(len(sources) * (g // 2)), sibling_recv.at[d])

        def pass_on(d):
            for m in range(half - 1):
                wait_bytes(op_bytes(1), pass_recv.at[m, d])
                remote(passing.at[m, d], ops.at[far_rows(d, j), from_source(near(m + 1))],
                       op_send, op_recv.at[half + m, d], j, other).start()

        def forward(i):
            for m in range(half - 1):
                at = block_part(near(m + 1), i)
                wait_bytes(at, blk_recv.at[near_slot(m, i)])
                remote(at, at, block_send, blk_recv.at[far_slot(m + 1, i)], j, other).start()

        closest, rest = range(half), range(half, 2 * half - 1)
        first = half - 1
        enter(0, first, False)
        plane_entered()
        signal(ready.at[rounds + 1], j, other)
        for mask in distant:
            spread(0, first, j, mask)
        for e in closest[1:]:
            enter(e, first, True)
        for d in outer_first:
            pass_on(d)
        block_out(2)
        forward(0)
        for e in rest:
            enter(e, first, True)
        for d in outer_first[1:]:
            for e in range(len(sources)):
                enter(e, d, True)
        forward(1)
        forward(2)
        for i in range(3, raw):
            block_out(i)
        share(first)
        complete(first)
        if half > 1:
            pl.semaphore_wait(ready.at[rounds], half - 1)

        band_of = lambda d: from_source(near(d) - side * half)
        others = pl.ds(pl.multiple_of(side * rows, rows), (n - 1) * rows)
        final = far(half - 1)

        def results(d, c, lane, size):
            target = pl.ds(pl.multiple_of(j * cols + lane, width), size)
            lane = pl.ds(lane, size)

            def result(to):
                return res.at[d, c, pl.ds(pl.multiple_of(to * outrows, outrows), outrows), lane]

            @pl.when(d > 0)
            def _():
                for to in range(g):
                    remote(result(to), out_ref.at[c, :, target], res_send, out_recv.at[0], to, near(d)).start()

            @pl.when(d == 0)
            def _():
                for mask in range(1, g):
                    to = flip(mask)
                    remote(result(to), out_ref.at[c, :, target], res_send, out_recv.at[0], to, near(d)).start()
                pltpu.make_async_copy(result(j), out_ref.at[c, :, target], out_recv.at[0]).start()

        def product(d, c, lane, i_first, count):
            band = band_of(d)

            @pl.when(d == first)
            def _():
                for e in range(half - 1):
                    for i in range(count):
                        wait_bytes(block_part(0, 0), blk_recv.at[far_slot(e, i_first + i)])
            size = lane.size
            ahead = wide.at[:, pl.ds(0, size)]
            ahead[...] = jnp.dot(ops[band, others], blocks[c, others, lane], preferred_element_type=jnp.float32)

            @pl.when(d == first)
            def _():
                for i in range(count):
                    wait_bytes(block_part(0, 0), blk_recv.at[far_slot(half - 1, i_first + i)])
            total = ahead[...] + jnp.dot(
                ops[band, from_source(final)], blocks[c, from_source(final), lane], preferred_element_type=jnp.float32)
            res[d, c, :, lane] = total.astype(res.dtype)

        def near_half():
            for m in range(half - 1):
                wait_bytes(last_plane(0), blk_recv.at[near_slot(m, raw)])
            near_sum[...] = jnp.dot(ops[:, mine], blocks[planes - 1, mine, :], preferred_element_type=jnp.float32)
            near_out[...] = near_sum[band_of(0), :].astype(near_out.dtype)
            target = terms.at[1, :, pl.ds(pl.multiple_of(j * cols, cols), cols)]

            def term(to):
                return near_out.at[pl.ds(pl.multiple_of(to * outrows, outrows), outrows), :]
            for mask in reversed(range(1, g)):
                remote(term(flip(mask)), target, late_send, terms_recv.at[1], flip(mask), k).start()
            pltpu.make_async_copy(term(j), target, terms_recv.at[1]).start()

        def far_half(at):
            d, chip = pairs[at]
            band = far_rows(d, 2 * chip, 2)
            total = part[band, :]
            for m in range(half - 1):
                wait_bytes(part_in.at[m, band, :], part_recv.at[m, at])
                total = total + part_in[m, band, :].astype(jnp.float32)
            far_out[band, :] = total.astype(far_out.dtype)
            if at < joined:
                remote(far_out.at[band, :], far_in.at[band, :], far_send, far_recv.at[at], j, other).start()
                return
            for to in (2 * chip, 2 * chip + 1):
                remote(far_out.at[far_rows(d, to), :], terms.at[0, :, pl.ds(pl.multiple_of(j * cols, cols), cols)],
                       far_send, terms_recv.at[0], to, other).start()

        def late_result(at):
            d, chip = pairs[at]
            band = near_rows(d, 2 * chip, 2)
            wait_bytes(far_in.at[band, :], far_recv.at[at])
            late[band, :] = (near_sum[band, :] + far_in[band, :].astype(jnp.float32)).astype(late.dtype)
            target = out_ref.at[planes - 1, :, pl.ds(pl.multiple_of(j * cols, cols), cols)]
            for to in (2 * chip, 2 * chip + 1):
                remote(late.at[near_rows(d, to), :], target, late_send, out_recv.at[1], to, near(d)).start()

        early = (planes - 2) * parts

        def one(t, carry):
            i = jnp.where(t < early, t, early + lax.div(t - early, half))
            d = jnp.where(t < early, first, first - lax.rem(t - early, half))
            c, h = lax.div(i, parts), lax.rem(i, parts)
            at = pl.multiple_of(h * width, width)

            @pl.when(t == 1)
            def _():
                for e in range(3, raw):
                    forward(e)
                for e in outer_first[1:]:
                    share(e)

            @pl.when(t == early)
            def _():
                for e in outer_first[1:]:
                    complete(e)
                    for whole in range(planes - 2):
                        product(jnp.int32(e), whole, pl.ds(0, cols), 0, 0)
                        results(jnp.int32(e), whole, 0, cols)

            @pl.when(t == early + 1)
            def _():
                near_half()
                far_half(0)
                far_half(1)

            @pl.when(t == early + 2)
            def _():
                far_half(2)

            @pl.when(t == last_turn)
            def _():
                far_half(3)

            product(d, c, pl.ds(at, width), i, 1)
            results(d, c, at, width)
            return carry

        last_turn = early + half * parts - 1
        lax.fori_loop(0, last_turn + 1, one, 0)
        late_result(0)
        pl.semaphore_wait(ready.at[rounds + 1], 1)
        far_half(4)
        late_result(1)
        for at in range(5, len(pairs)):
            far_half(at)
            if at - 3 < joined:
                late_result(at - 3)
        for at in range(len(pairs) - 3, joined):
            late_result(at)
        wait_bytes(op_bytes(half * half), op_send)
        wait_bytes(blocks.at[pl.ds(0, planes - 1), pl.ds(0, half * rows), :], block_send)
        wait_bytes(blocks.at[pl.ds(0, planes - 1), pl.ds(0, half * rows - outrows), :], res_send)
        for e in range(len(sources)):
            wait_bytes(op_bytes(half * (g - 1)), spread_send.at[e])
        wait_bytes(far_out, far_send)
        wait_bytes(late.at[pl.ds(0, half * rows - outrows), :], late_send)
        for b in (1, 0):
            wait_bytes(terms.at[b], terms_recv.at[b])
        out_ref[planes - 1] = (terms[0].astype(jnp.float32) + terms[1].astype(jnp.float32)).astype(out_ref.dtype)

    @pl.when(jnp.logical_not(is_centre))
    def _():
        m = away - 1

        def op_in(d):
            remote(first_ops.at[1, d], ops.at[near_rows(d, j), from_source(k)],
                   op_send, op_recv.at[m, d], j, centre).start()

        def op_past(d):
            remote(first_ops.at[0, d], passing.at[m, d], op_send, pass_recv.at[m, d], j, centre).start()

        staged_in(1)
        op_in(half - 1)
        staged_in(0)
        for d in outer_first:
            op_past(d)
        for d in outer_first[1:]:
            op_in(d)
        own_start.wait()
        own_rest.wait()
        for i in range(raw):
            at = block_part(k, i)
            remote(at, at, block_send, blk_recv.at[near_slot(m, i)], j, centre).start()
        remote(last_plane(k), last_plane(k), block_send, blk_recv.at[near_slot(m, raw)], j, centre).start()
        operator_in()
        own_part()
        part_out[...] = part[...].astype(part_out.dtype)
        for at, (d, chip) in enumerate(pairs):
            band = far_rows(d, 2 * chip, 2)
            remote(part_out.at[band, :], part_in.at[m, band, :], far_send, part_recv.at[m, at], j, centre).start()
        plane_entered()
        signal(ready.at[rounds], j, centre)
        wait_bytes(op_bytes(2 * half), op_send)
        wait_bytes(blocks.at[:, from_source(0), :], block_send)
        wait_bytes(part_out, far_send)

    wait_bytes(out_ref.at[pl.ds(0, planes - 1)], out_recv.at[0])

    @pl.when(jnp.logical_not(is_centre))
    def _():
        wait_bytes(out_ref.at[planes - 1], out_recv.at[1])


def at_centres(n, g, products, operator):
    rows, planes, cols = products.shape
    parts = 2 if cols % (2 * LANES) == 0 else 1
    half = n // 2
    outer, roles, raw = max(half - 1, 1), 2 * half - 1, (planes - 1) * parts
    out = pl.pallas_call(
        functools.partial(kernel, n, g, parts),
        out_shape=jax.ShapeDtypeStruct((planes, rows // g, cols * g), jnp.bfloat16),
        in_specs=[pl.BlockSpec(memory_space=pl.ANY)] * 2,
        out_specs=pl.BlockSpec(memory_space=pltpu.VMEM),
        scratch_shapes=[
            pltpu.VMEM((planes, n * rows, cols), jnp.bfloat16),
            pltpu.VMEM((half * rows, n * rows), jnp.bfloat16),
            pltpu.VMEM((half * rows, rows), jnp.bfloat16),
            pltpu.VMEM((2, half, rows // g, rows), jnp.bfloat16),
            pltpu.VMEM((outer, half, rows // g, rows), jnp.bfloat16),
            pltpu.VMEM((half, planes - 1, rows, cols), jnp.bfloat16),
            pltpu.VMEM((rows, cols), jnp.float32),
            pltpu.VMEM((half * rows, cols), jnp.float32),
            pltpu.VMEM((half * rows, cols), jnp.bfloat16),
            pltpu.VMEM((outer, half * rows, cols), jnp.bfloat16),
            pltpu.VMEM((half * rows, cols), jnp.bfloat16),
            pltpu.VMEM((half * rows, cols), jnp.bfloat16),
            pltpu.VMEM((half * rows, cols), jnp.float32),
            pltpu.VMEM((rows, cols), jnp.bfloat16),
            pltpu.VMEM((half * rows, cols), jnp.bfloat16),
            pltpu.VMEM((2, rows // g, g * cols), jnp.bfloat16),
            pltpu.SemaphoreType.DMA,
            pltpu.SemaphoreType.DMA,
            pltpu.SemaphoreType.DMA((roles,)),
            pltpu.SemaphoreType.DMA,
            pltpu.SemaphoreType.DMA,
            pltpu.SemaphoreType.DMA,
            pltpu.SemaphoreType.DMA((outer * (raw + 1) + half * raw,)),
            pltpu.SemaphoreType.DMA((roles, half)),
            pltpu.SemaphoreType.DMA((outer, half)),
            pltpu.SemaphoreType.DMA((roles, half)),
            pltpu.SemaphoreType.DMA((half,)),
            pltpu.SemaphoreType.DMA((2,)),
            pltpu.SemaphoreType.DMA((outer, half * g // 2)),
            pltpu.SemaphoreType.DMA((outer * g // 2,)),
            pltpu.SemaphoreType.DMA((2,)),
            pltpu.SemaphoreType.DMA((5,)),
            pltpu.SemaphoreType.REGULAR((g.bit_length() + 1,)),
        ],
        compiler_params=pltpu.CompilerParams(
            collective_id=0, has_side_effects=True, vmem_limit_bytes=GRANT),
    )(products.transpose(1, 0, 2), operator)
    return out.transpose(1, 0, 2)


def by_collectives(products, operator):
    y_local, three, m_local = products.shape
    flat = products.reshape(y_local, three * m_local)
    summed = lax.psum_scatter(
        jnp.dot(operator, flat, preferred_element_type=jnp.float32), "gy", scatter_dimension=0, tiled=True)
    result = summed.astype(jnp.bfloat16).reshape(y_local, three, m_local)
    return lax.all_to_all(result, "gx", split_axis=0, concat_axis=2, tiled=True)


def solution(mesh):
    n, g = mesh.shape["gy"], mesh.shape["gx"]

    def body(products, operator):
        rows, planes, cols = products.shape
        aligned = (n // 2 == 2 and n % 2 == 0 and planes > 2 and g & (g - 1) == 0 and g > 4 and rows % (g * SUBLANES) == 0
                   and rows % LANES == 0 and cols % (2 * LANES) == 0)
        held = 2 * (products.size * (n + n // 2 + 2) + operator.size * (2 + n // 2)) + 20 * n * rows * cols
        if aligned and held < VMEM_BYTES // 2:
            return at_centres(n, g, products, operator)
        return by_collectives(products, operator)

    return jax.shard_map(
        body,
        mesh=mesh,
        in_specs=(P("gy", None, "gx"), P(None, "gy")),
        out_specs=P(("gy", "gx"), None, None),
        check_vma=False,
    )
```
